128 devices in a mesh: dp: 1, tx: 16 (over z, y), tyz: 8 (over x, core).
Axes of the slice: x: 4, y: 4, z: 4, core: 2. Of those that a mesh axis runs over, the one named last changes fastest.
Arguments:
- residual: bfloat16 [8192, 5120], P('dp', ('tx', 'tyz'))
- ln_scale: bfloat16 [5120], P(('tx', 'tyz'))
- w_query: bfloat16 [5120, 5120], P('tx', 'tyz')
- w_key: bfloat16 [5120, 128], P('tx')
- w_value: bfloat16 [5120, 128], P('tx')
- w_gate: bfloat16 [5120, 20480], P('tx', 'tyz')
- w_up: bfloat16 [5120, 20480], P('tx', 'tyz')
- w_out: bfloat16 [5120, 5120], P('tyz', 'tx')
- w_down: bfloat16 [20480, 5120], P('tyz', 'tx')
- k_cache: bfloat16 [8192, 64, 128], P(('dp', 'tx', 'tyz'))
- v_cache: bfloat16 [8192, 64, 128], P(('dp', 'tx', 'tyz'))
- lengths: int32 [8192], P(('dp', 'tx', 'tyz'))
Outputs:
- output 1: bfloat16 [8192, 5120], P('dp', ('tx', 'tyz'))
- output 2: bfloat16 [8192, 64, 128], P(('dp', 'tx', 'tyz'))
- output 3: bfloat16 [8192, 64, 128], P(('dp', 'tx', 'tyz'))
All inputs are finite; a program needn't handle non-finite values.
Results may differ from the reference program's by a relative error of at most 0.02.
Values are sent between devices in bfloat16 or wider.
A program may use at most 1 GiB of HBM per device.

```python
import jax
import jax.numpy as jnp
from jax import lax

MODEL_DIM = 5120
FF_DIM = 20480
NUM_HEADS = 40
HEAD_DIM = 128
SEQ_LEN = 64
BATCH_ROWS = 8192
ROW_BLOCK = 64
LN_EPS = 1e-5
ROPE_BASE = 10000.0


def draw_lengths(len_key):
    low_key, pick_key = jax.random.split(len_key)
    drawn_lens = jax.random.randint(low_key, (BATCH_ROWS,), SEQ_LEN // 8, SEQ_LEN, dtype=jnp.int32)
    row_order = jax.random.permutation(pick_key, BATCH_ROWS)
    row_ids = jnp.arange(BATCH_ROWS)
    drawn_lens = jnp.where(row_ids == row_order[0], SEQ_LEN - 1, drawn_lens)
    drawn_lens = jnp.where(row_ids == row_order[1], SEQ_LEN // 8, drawn_lens)
    return drawn_lens.astype(jnp.int32)


def setup_inputs(seed: int = 0, part: int = 0) -> dict:
    part_keys = jax.random.split(jax.random.fold_in(jax.random.key(seed), part), 4)
    shared_keys = jax.random.split(jax.random.key(seed + 1), 8)
    q_width = NUM_HEADS * HEAD_DIM
    in_scale = MODEL_DIM ** -0.5
    out_scale = 0.3 * (SEQ_LEN / q_width) ** 0.5
    down_scale = FF_DIM ** -0.5
    return {
        'residual': jax.random.normal(part_keys[0], (BATCH_ROWS, MODEL_DIM), jnp.float32).astype(jnp.bfloat16),
        'ln_scale': (1.0 + 0.4 * jax.random.normal(shared_keys[0], (MODEL_DIM,), jnp.float32)).astype(jnp.bfloat16),
        'w_query': (jax.random.normal(shared_keys[1], (MODEL_DIM, q_width), jnp.float32) * in_scale).astype(jnp.bfloat16),
        'w_key': (jax.random.normal(shared_keys[2], (MODEL_DIM, HEAD_DIM), jnp.float32) * in_scale).astype(jnp.bfloat16),
        'w_value': (jax.random.normal(shared_keys[3], (MODEL_DIM, HEAD_DIM), jnp.float32) * in_scale).astype(jnp.bfloat16),
        'w_gate': (jax.random.normal(shared_keys[4], (MODEL_DIM, FF_DIM), jnp.float32) * in_scale).astype(jnp.bfloat16),
        'w_up': (jax.random.normal(shared_keys[5], (MODEL_DIM, FF_DIM), jnp.float32) * in_scale).astype(jnp.bfloat16),
        'w_out': (jax.random.normal(shared_keys[6], (q_width, MODEL_DIM), jnp.float32) * out_scale).astype(jnp.bfloat16),
        'w_down': (jax.random.normal(shared_keys[7], (FF_DIM, MODEL_DIM), jnp.float32) * down_scale).astype(jnp.bfloat16),
        'k_cache': jax.random.normal(part_keys[1], (BATCH_ROWS, SEQ_LEN, HEAD_DIM), jnp.float32).astype(jnp.bfloat16),
        'v_cache': jax.random.normal(part_keys[2], (BATCH_ROWS, SEQ_LEN, HEAD_DIM), jnp.float32).astype(jnp.bfloat16),
        'lengths': draw_lengths(part_keys[3]),
    }


def rope_rotate(vectors, positions):
    head_dim = vectors.shape[-1]
    half_dim = head_dim // 2
    inv_freq = ROPE_BASE ** (-2.0 * jnp.arange(half_dim, dtype=jnp.float32) / head_dim)
    angles = positions.astype(jnp.float32)[:, None] * inv_freq[None, :]
    bcast_shape = (angles.shape[0],) + (1,) * (vectors.ndim - 2) + (half_dim,)
    cos_part = jnp.cos(angles).reshape(bcast_shape)
    sin_part = jnp.sin(angles).reshape(bcast_shape)
    vec_f32 = vectors.astype(jnp.float32)
    first_half = vec_f32[..., :half_dim]
    second_half = vec_f32[..., half_dim:]
    rotated = jnp.concatenate([first_half * cos_part - second_half * sin_part, second_half * cos_part + first_half * sin_part], axis=-1)
    return rotated.astype(jnp.bfloat16)


def attend_rows(query_rot, key_rot, value_new, k_cache, v_cache, lengths):
    positions = jnp.arange(k_cache.shape[1], dtype=jnp.int32)
    write_mask = (positions[None, :] == lengths[:, None])[:, :, None]
    k_updated = jnp.where(write_mask, key_rot[:, None, :], k_cache)
    v_updated = jnp.where(write_mask, value_new[:, None, :], v_cache)
    scores = jnp.einsum('rhd,rtd->rht', query_rot.astype(jnp.float32), k_updated.astype(jnp.float32)) * (query_rot.shape[-1] ** -0.5)
    valid_mask = (positions[None, :] <= lengths[:, None])[:, None, :]
    scores = jnp.where(valid_mask, scores, -1e30)
    attn_probs = jax.nn.softmax(scores, axis=-1).astype(jnp.bfloat16)
    attended = jnp.einsum('rht,rtd->rhd', attn_probs.astype(jnp.float32), v_updated.astype(jnp.float32)).astype(jnp.bfloat16)
    return attended, k_updated, v_updated


def reference(residual, ln_scale, w_query, w_key, w_value, w_gate, w_up, w_out, w_down, k_cache, v_cache, lengths):
    res_f32 = residual.astype(jnp.float32)
    row_mean = jnp.mean(res_f32, axis=-1, keepdims=True)
    row_var = jnp.mean(jnp.square(res_f32 - row_mean), axis=-1, keepdims=True)
    normed = ((res_f32 - row_mean) * lax.rsqrt(row_var + LN_EPS) * ln_scale.astype(jnp.float32)).astype(jnp.bfloat16)
    query_vec = jnp.dot(normed, w_query, preferred_element_type=jnp.float32).astype(jnp.bfloat16)
    key_new = jnp.dot(normed, w_key, preferred_element_type=jnp.float32).astype(jnp.bfloat16)
    value_new = jnp.dot(normed, w_value, preferred_element_type=jnp.float32).astype(jnp.bfloat16)
    gate_val = jnp.dot(normed, w_gate, preferred_element_type=jnp.float32).astype(jnp.bfloat16)
    up_val = jnp.dot(normed, w_up, preferred_element_type=jnp.float32).astype(jnp.bfloat16)
    mlp_act = (jax.nn.silu(gate_val.astype(jnp.float32)) * up_val.astype(jnp.float32)).astype(jnp.bfloat16)
    query_rot = rope_rotate(query_vec.reshape(BATCH_ROWS, NUM_HEADS, HEAD_DIM), lengths)
    key_rot = rope_rotate(key_new, lengths)
    num_blocks = BATCH_ROWS // ROW_BLOCK

    def attend_block(block_args):
        return attend_rows(block_args[0], block_args[1], block_args[2], block_args[3], block_args[4], block_args[5])

    attended, k_blocks, v_blocks = lax.map(attend_block, (
        query_rot.reshape(num_blocks, ROW_BLOCK, NUM_HEADS, HEAD_DIM),
        key_rot.reshape(num_blocks, ROW_BLOCK, HEAD_DIM),
        value_new.reshape(num_blocks, ROW_BLOCK, HEAD_DIM),
        k_cache.reshape(num_blocks, ROW_BLOCK, SEQ_LEN, HEAD_DIM),
        v_cache.reshape(num_blocks, ROW_BLOCK, SEQ_LEN, HEAD_DIM),
        lengths.reshape(num_blocks, ROW_BLOCK)))
    attn_flat = attended.reshape(BATCH_ROWS, NUM_HEADS * HEAD_DIM)
    block_out = jnp.dot(attn_flat, w_out, preferred_element_type=jnp.float32) + jnp.dot(mlp_act, w_down, preferred_element_type=jnp.float32)
    new_resid = (res_f32 + block_out).astype(jnp.bfloat16)
    return (new_resid, k_blocks.reshape(BATCH_ROWS, SEQ_LEN, HEAD_DIM), v_blocks.reshape(BATCH_ROWS, SEQ_LEN, HEAD_DIM))
```

```python
import jax
import jax.numpy as jnp
from jax import lax
from jax.sharding import Mesh, PartitionSpec as P

LN_EPS = 1e-5
ROPE_BASE = 10000.0


def rope_rotate(vectors, positions):
    head_dim = vectors.shape[-1]
    half_dim = head_dim // 2
    inv_freq = ROPE_BASE ** (-2.0 * jnp.arange(half_dim, dtype=jnp.float32) / head_dim)
    angles = positions.astype(jnp.float32)[:, None] * inv_freq[None, :]
    bcast_shape = (angles.shape[0],) + (1,) * (vectors.ndim - 2) + (half_dim,)
    cos_part = jnp.cos(angles).reshape(bcast_shape)
    sin_part = jnp.sin(angles).reshape(bcast_shape)
    vec_f32 = vectors.astype(jnp.float32)
    first_half = vec_f32[..., :half_dim]
    second_half = vec_f32[..., half_dim:]
    rotated = jnp.concatenate([first_half * cos_part - second_half * sin_part, second_half * cos_part + first_half * sin_part], axis=-1)
    return rotated.astype(jnp.bfloat16)


def attend_rows(query_rot, key_rot, value_new, k_cache, v_cache, lengths):
    positions = jnp.arange(k_cache.shape[1], dtype=jnp.int32)
    write_mask = (positions[None, :] == lengths[:, None])[:, :, None]
    k_updated = jnp.where(write_mask, key_rot[:, None, :], k_cache)
    v_updated = jnp.where(write_mask, value_new[:, None, :], v_cache)
    scores = jnp.einsum('rhd,rtd->rht', query_rot, k_updated, preferred_element_type=jnp.float32) * (query_rot.shape[-1] ** -0.5)
    valid_mask = (positions[None, :] <= lengths[:, None])[:, None, :]
    scores = jnp.where(valid_mask, scores, -1e30)
    attn_probs = jax.nn.softmax(scores, axis=-1).astype(jnp.bfloat16)
    attended = jnp.einsum('rht,rtd->rhd', attn_probs, v_updated, preferred_element_type=jnp.float32).astype(jnp.bfloat16)
    return attended, k_updated, v_updated


def solution(mesh):
    inner = Mesh(mesh.devices.reshape(4, 4, 4, 2), ('z', 'y', 'x', 'c'))
    f32, bf16 = jnp.float32, jnp.bfloat16

    def decode_layer(residual, ln_scale, w_query, w_key, w_value, w_gate, w_up, w_out, w_down, k_cache, v_cache, lengths):
        feats = residual.shape[1]
        model_dim = feats * 128
        def cols_by_y(w):
            parts = w.reshape(w.shape[0], 4, -1).transpose(1, 0, 2)
            parts = lax.all_to_all(parts, 'y', 0, 0, tiled=True)
            return lax.all_gather(parts, ('z', 'c'), axis=0, tiled=False).reshape((4, 2) + parts.shape)
        wq = lax.all_gather(w_query, ('z', 'c'), axis=0, tiled=False).reshape(4, 2, *w_query.shape)
        wkv = lax.all_gather(jnp.concatenate([w_key, w_value], axis=1), 'z', axis=0, tiled=False)
        wg = cols_by_y(w_gate)
        wu = cols_by_y(w_up)
        wo = lax.all_gather(w_out, ('z', 'c'), axis=0, tiled=False).reshape(4, 2, *w_out.shape)
        wd = lax.all_to_all(w_down.reshape(4, -1, w_down.shape[1]), 'y', 0, 0, tiled=True)
        wd = lax.all_gather(wd, ('z', 'c'), axis=0, tiled=False).reshape((4, 2) + wd.shape)

        rows = residual.reshape(4, 16, 2, 64, feats).transpose(0, 2, 4, 1, 3).reshape(8, feats, 1024)
        scale8 = lax.all_gather(ln_scale, ('z', 'c'), axis=0, tiled=False)
        mine = lax.all_to_all(rows, ('z', 'c'), 0, 0, tiled=True)
        x = mine.astype(f32)
        stats = jnp.stack([jnp.sum(x, axis=(0, 1)), jnp.sum(jnp.square(x), axis=(0, 1))])
        stats = lax.psum(stats, ('y', 'x'))
        mean = stats[0] / model_dim
        var = stats[1] / model_dim - jnp.square(mean)
        hn = ((x - mean) * lax.rsqrt(var + LN_EPS) * scale8.astype(f32)[:, :, None]).astype(bf16)
        hn = lax.all_gather(hn.reshape(8 * feats, 1024), ('y', 'x'), axis=0, tiled=False)
        hn = hn.reshape(4, 4, 4, 2, feats, 1024)
        hn = hn.transpose(2, 0, 1, 3, 4, 5).reshape(4, 4, 8 * feats, 1024)
        hn_y = lax.dynamic_index_in_dim(hn, lax.axis_index('y'), 1, keepdims=False)

        q_part = jnp.einsum('zkr,zckn->rcn', hn_y, wq, preferred_element_type=f32).astype(bf16).reshape(1024, -1)
        kv_part = jnp.einsum('zkr,zkn->rn', hn_y, wkv, preferred_element_type=f32).astype(bf16)
        q_rows = lax.psum_scatter(jnp.concatenate([q_part, kv_part], axis=1), 'y', scatter_dimension=0, tiled=True)
        kv_rows = lax.dynamic_slice_in_dim(q_rows[:, 1280:], lax.axis_index('x') * 64, 64, axis=0)
        q = lax.all_to_all(q_rows[:, :1280].reshape(4, 64, 1280), 'x', 0, 0, tiled=True)
        q = q.transpose(1, 0, 2).reshape(64, 40, 128)
        q_rot = rope_rotate(q, lengths)
        k_rot = rope_rotate(kv_rows[:, :128], lengths)
        o, k_new, v_new = attend_rows(q_rot, k_rot, kv_rows[:, 128:], k_cache, v_cache, lengths)
        o = o.reshape(64, 4, 1280).transpose(1, 0, 2)
        o = lax.all_to_all(o, 'x', 0, 0, tiled=True).reshape(256, 1280)
        o = lax.all_gather(o, 'y', axis=0, tiled=True)

        gate = jnp.einsum('zykr,zcykn->rcn', hn, wg, preferred_element_type=f32).astype(bf16)
        up = jnp.einsum('zykr,zcykn->rcn', hn, wu, preferred_element_type=f32).astype(bf16)
        act = (jax.nn.silu(gate.astype(f32)) * up.astype(f32)).astype(bf16)
        out = jnp.einsum('zcynf,rcn->zyfr', wd, act, preferred_element_type=f32)
        out_o = jnp.einsum('zcnf,rcn->zfr', wo, o.reshape(1024, 2, 640), preferred_element_type=f32)
        here = (jnp.arange(4) == lax.axis_index('y')).astype(f32)[None, :, None, None]
        out = (out + here * out_o[:, None]).astype(bf16)
        out = out.reshape(4, 4, 4, 2 * feats, 1024).transpose(1, 2, 0, 3, 4).reshape(16 * 8 * feats, 1024)
        out = lax.psum_scatter(out, ('y', 'x'), scatter_dimension=0, tiled=True)
        new = (x.reshape(8 * feats, 1024) + out.astype(f32)).astype(bf16).reshape(8, feats, 1024)
        new = lax.all_to_all(new, ('z', 'c'), 0, 0, tiled=True)
        new = new.reshape(4, 2, feats, 16, 64).transpose(0, 3, 1, 4, 2).reshape(8192, feats)
        return new, k_new, v_new

    rc = ('z', 'y', 'x', 'c')
    tx, tyz = ('z', 'y'), ('x', 'c')
    in_specs = (P(None, rc), P(rc), P(tx, tyz), P(tx, None), P(tx, None), P(tx, tyz), P(tx, tyz), P(tyz, tx), P(tyz, tx), P(rc, None, None), P(rc, None, None), P(rc))
    out_specs = (P(None, rc), P(rc, None, None), P(rc, None, None))
    return jax.shard_map(decode_layer, mesh=inner, in_specs=in_specs, out_specs=out_specs, check_vma=False)
```

```python
import jax
import jax.numpy as jnp
from jax import lax
from jax.experimental import pallas as pl
from jax.experimental.pallas import tpu as pltpu
from jax.sharding import Mesh, PartitionSpec as P

LN_EPS = 1e-5
ROPE_BASE = 10000.0
MESH = pl.DeviceIdType.MESH
DMA = pltpu.SemaphoreType.DMA
F32, BF16 = jnp.float32, jnp.bfloat16
ROWS, MODEL, FEATS, BATCH = 1024, 5120, 40, 8192
KB, NB, HB, QB, HD, SUB = 1280, 640, 320, 896, 128, 80
MINE, SEQ, HEADS, LANE = 64, 64, 40, 128
NR, NC, NJ, NG = 4, 2, 16, 8
SPLIT = 384
CUT = 512
TILE = 256
RING = range(4)
AWAY = (1, 3, 2)
GROUPS = ((0, 1), (1, 2), (2, 4))
ORDER = (0, 1, 3, 2)
PAIRS = tuple(sorted(((dy, dx) for dy in RING for dx in RING if dy or dx), key=lambda p: (p.count(2), sum(p))))
NT = (((1,), (1,)), ((), ()))


def flip(i, d):
    return (i, i + 1 - 2 * lax.rem(i, 2), lax.rem(i + 2, 4), 3 - i)[d]


def put(src, dst, ssem, rsem, dev):
    pltpu.make_async_remote_copy(src_ref=src, dst_ref=dst, send_sem=ssem, recv_sem=rsem, device_id=dev, device_id_type=MESH).start()


def three(ref):
    return sum(ref[k].astype(F32) for k in range(3))


def get(src, dst, sem):
    pltpu.make_async_copy(src, dst, sem).start()


def first(n):
    return pl.ds(0, n)


def drain(ref, sem):
    pltpu.make_async_copy(ref, ref, sem).wait()


class Wide:
    def __init__(self, land, src, sems, pos):
        self.land, self.src = land, src
        self.send, self.yr, self.zr, self.fr, self.dr, self.loc = sems
        self.z, self.y, self.x, self.c = pos
        self.base = self.c * 16

    def piece(self, yy):
        return self.src.at[:, pl.ds(pl.multiple_of(yy * NB, LANE), NB)]

    def at(self, dz, g, base=None):
        lo, hi = GROUPS[g]
        return self.land.at[pl.ds((self.base if base is None else base) + dz * 4 + lo, hi - lo)]

    def start_local(self):
        get(self.piece(self.y), self.land.at[self.base], self.loc)

    def y_send(self):
        for dy in AWAY:
            yy = flip(self.y, dy)
            put(self.piece(yy), self.land.at[self.base + dy], self.send, self.yr.at[dy - 1], dict(y=yy))

    def z_send(self, g):
        if g:
            for dy in range(*GROUPS[g]):
                drain(self.land.at[self.base + dy], self.yr.at[dy - 1])
        for k, dz in enumerate(AWAY[:2]):
            to = dict(z=flip(self.z, dz))
            if g:
                put(self.at(0, g), self.at(dz, g), self.send, self.zr.at[k * 3 + g], to)
            else:
                put(self.piece(self.y), self.land.at[self.base + dz * 4], self.send, self.zr.at[k * 3], to)
        self.d2d(0, g)

    def forward(self, g):
        for k, dz in enumerate(AWAY[:2]):
            drain(self.at(dz, g), self.zr.at[k * 3 + g])
        src, to = (1, 3) if g < 2 else (3, 1)
        put(self.at(src, g), self.at(2, g), self.send, self.fr.at[g], dict(z=flip(self.z, to)))
        self.d2d(1, g)
        self.d2d(3, g)

    def last(self, g):
        drain(self.at(2, g), self.fr.at[g])
        self.d2d(2, g)

    def d2d(self, dz, g):
        to = dict(c=1 - self.c)
        if dz or g:
            put(self.at(dz, g), self.at(dz, g), self.send, self.dr.at[dz * 3 + g], to)
        else:
            put(self.piece(self.y), self.land.at[self.base], self.send, self.dr.at[0], to)

    def load(self, dz, tile, sem):
        if dz == 0:
            drain(self.land.at[self.base], self.loc)
        for g in range(3):
            drain(self.at(dz, g, 16 - self.base), self.dr.at[dz * 3 + g])
        for cc in range(NC):
            get(self.land.at[pl.ds(cc * 16 + dz * 4, 4)], tile.at[:, :, pl.ds(cc * NB, NB)], sem)

    def finish(self):
        drain(self.land.at[first(31)], self.send)


class Narrow:
    def __init__(self, land, parts, sems, pos):
        self.land, self.parts = land, parts
        self.send, self.yr, self.zr, self.fr, self.dr, self.loc = sems
        self.z, self.y, self.x, self.c = pos
        self.s = lax.rem(self.c + self.y, 2)

    def own(self, slot):
        lo = 0
        for ref in self.parts:
            hi = lo + ref.shape[1]
            yield ref, self.land.at[slot, :, pl.ds(lo, hi - lo)]
            lo = hi

    def start(self):
        @pl.when(self.s == 0)
        def _():
            for src, dst in self.own(0):
                get(src, dst, self.loc)

        @pl.when(self.s == 1)
        def _():
            for src, dst in self.own(1):
                put(src, dst, self.send, self.yr, dict(y=flip(self.y, 1), c=1 - self.c))

    def z_first(self):
        @pl.when(self.s == 0)
        def _():
            for k, dz in enumerate(AWAY[:2]):
                for (src, _), (_, dst) in zip(self.own(0), self.own(dz * 2)):
                    put(src, dst, self.send, self.zr.at[k], dict(z=flip(self.z, dz)))
            for src, dst in self.own(0):
                put(src, dst, self.send, self.dr.at[0], dict(c=1 - self.c))

    def z_second(self):
        @pl.when(self.s == 1)
        def _():
            src = self.land.at[1]
            drain(src, self.yr)
            for k, dz in enumerate(AWAY[:2]):
                put(src, self.land.at[dz * 2 + 1], self.send, self.zr.at[k], dict(z=flip(self.z, dz)))
            put(src, src, self.send, self.dr.at[0], dict(c=1 - self.c))

    def half(self, slot, k):
        return self.land.at[slot, pl.ds(k * HB // 2, HB // 2)]

    def forward(self):
        for k, dz in enumerate(AWAY[:2]):
            slot = dz * 2 + self.s
            piece = self.land.at[slot]
            drain(piece, self.zr.at[k])
            put(self.half(slot, k), self.half(4 + self.s, k), self.send, self.fr.at[k], dict(z=flip(self.z, AWAY[1 - k])))
            put(piece, piece, self.send, self.dr.at[1 + k], dict(c=1 - self.c))

    def last(self):
        for k in range(NC):
            piece = self.half(4 + self.s, k)
            drain(piece, self.fr.at[k])
            put(piece, piece, self.send, self.dr.at[3 + k], dict(c=1 - self.c))

    def load(self, dz, tile, sem):
        o = 1 - self.s
        if dz == 0:
            @pl.when(self.s == 0)
            def _():
                drain(self.land.at[0], self.loc)
        if dz == 2:
            for k in range(NC):
                drain(self.half(4 + o, k), self.dr.at[3 + k])
        else:
            drain(self.land.at[dz * 2 + o], self.dr.at[(dz + 1) // 2])
        get(self.land.at[pl.ds(dz * 2, 2)], tile, sem)

    def finish(self):
        for s in range(NC):
            @pl.when(self.s == s)
            def _():
                drain(self.land.at[first(7 + s)], self.send)


WIDE_SEMS = [DMA, DMA((3,)), DMA((6,)), DMA((3,)), DMA((12,)), DMA]
NARROW_SEMS = [DMA, DMA, DMA((2,)), DMA((2,)), DMA((5,)), DMA]
HBM_BUFS = dict(
    Q=((NG, HB, QB), BF16), G=((NG * NR, HB, NB), BF16), U=((NG * NR, HB, NB), BF16), D=((NG * NR, HB, NB), BF16), O=((NG, HB, NB), BF16),
    hnT=((NR, NR, HB, ROWS), BF16), a1=((NR, NR - 1, HB, CUT), BF16), b1=((NR, NR - 1, NR, SUB, ROWS - CUT), BF16))
VMEM_BUFS = dict(
    rT=((FEATS, BATCH), BF16), xs=((NG, FEATS, ROWS + LANE), BF16), F=((NG, FEATS, ROWS + LANE), BF16), S=((NJ, 2, ROWS), F32),
    hs=((NR, SUB, ROWS), BF16), hn=((NR, ROWS, KB), BF16), wt=((NC, NR, HB, KB), BF16), wo_t=((NC, NC, HB, NB), BF16),
    gacc=((ROWS, KB), F32), uacc=((ROWS, KB), F32), qout=((NJ, MINE, QB), BF16), q_in=((NJ, MINE, NB), BF16), kv_in=((NC, MINE, 2 * HD), BF16),
    q3=((MINE * HEADS, HD), F32), lenb=((MINE, HD), F32), kc=((MINE, SEQ, HD), BF16), vc=((MINE, SEQ, HD), BF16), kn=((MINE, 2 * HD), F32),
    o_v=((MINE, MODEL), BF16), o_in=((NJ, MINE, NB), BF16), act=((ROWS, KB), BF16), sb=((NC, NR, HB, ROWS), BF16),
    va=((NR - 1, HB, CUT), BF16), vb=((NR - 1, NR, SUB, ROWS - CUT), BF16), s2a=((NR, HB, CUT), BF16), s2b=((NR, NR, SUB, ROWS - CUT), BF16),
    a2=((NR, NR - 1, SUB, CUT), BF16), b2=((NR, NR - 1, SUB, ROWS - CUT), BF16), fs=((NR, NC, FEATS, ROWS), BF16), fin=((NG, FEATS, ROWS), BF16), ov=((FEATS, BATCH), BF16))
ONE, EACH, BY_GROUP = (), (NR,), (NG,)
SEMS = dict(f_s=ONE, s_s=ONE, s_r=ONE, own_l=ONE, q_s=ONE, q_r=ONE, kv_s=ONE, kv_r=ONE, o_s=ONE, o_r=ONE, fin_s=ONE, out_l=ONE,
            a1s=EACH, a1r=EACH, b1s=EACH, b1r=EACH, a2s=EACH, a2r=EACH, b2s=EACH, b2r=EACH, ag_s=EACH, ag_r=EACH, ld=EACH, wsem=EACH, osem=EACH, vsem=EACH,
            f_r=BY_GROUP, fin_r=BY_GROUP)


def kernel(res, ls, lens, wq, wk, wv, wg, wu, wdT, woT, kc_h, vc_h, outT, kc_o, vc_o, *rest):
    rest = list(rest)

    class b:
        pass
    for name in list(HBM_BUFS) + list(VMEM_BUFS) + list(SEMS):
        setattr(b, name, rest.pop(0))
    pos = z, y, x, c = tuple(lax.axis_index(a) for a in 'zyxc')
    flow = lambda kind, land, src: kind(land, src, [rest.pop(0) for _ in WIDE_SEMS], pos)
    fq = flow(Narrow, b.Q, (wq, wk, wv))
    fg, fu, fd = flow(Wide, b.G, wg), flow(Wide, b.U, wu), flow(Wide, b.D, wdT)
    fo = flow(Narrow, b.O, (woT,))
    me = y * 4 + x
    row_low = lax.broadcasted_iota(jnp.int32, (FEATS, LANE), 1) < LANE // 2

    bar = pltpu.get_barrier_semaphore()
    peers = [dict(z=flip(z, dz), c=cc) for dz in AWAY for cc in (c, 1 - c)] + [dict(c=1 - c), dict(y=flip(y, 1), c=1 - c)]
    peers += [dict(y=flip(y, dy), x=flip(x, dx)) for dy, dx in PAIRS]
    for p in peers:
        pl.semaphore_signal(bar, inc=1, device_id=p, device_id_type=MESH)
    get(res, b.rT, b.ld.at[0])
    get(kc_h, b.kc, b.ld.at[1])
    get(vc_h, b.vc, b.ld.at[2])
    for f in (fg, fu, fd):
        f.start_local()
    pl.semaphore_wait(bar, len(peers))
    fq.start()
    fo_start = fo.start

    drain(b.rT, b.ld.at[0])
    scale = jnp.broadcast_to(ls[...].astype(F32), (LANE, FEATS)).T.astype(BF16)
    for dz in AWAY + (0,):
        zz = flip(z, dz)
        for p in range(NG):
            pair = b.rT[:, pl.ds(pl.multiple_of(zz * 2 * ROWS + p * 2 * LANE, LANE), 2 * LANE)].astype(F32)
            t0, t1 = pair[:, :LANE], pair[:, LANE:]
            at = pl.ds(p * LANE, LANE)
            b.xs[dz * 2, :, at] = jnp.where(row_low, t0, pltpu.roll(t1, LANE // 2, 1)).astype(BF16)
            b.xs[dz * 2 + 1, :, at] = jnp.where(row_low, pltpu.roll(t0, LANE // 2, 1), t1).astype(BF16)
        for cc in range(NC):
            b.xs[dz * 2 + cc, :, ROWS:] = scale
        for cc in (c, 1 - c)[dz == 0:]:
            put(b.xs.at[dz * 2 + cc], b.F.at[dz * 2 + c], b.f_s, b.f_r.at[dz * 2 + c], dict(z=flip(z, dz), c=cc))
    b.F[c] = b.xs[c]
    fq.z_first()
    fg.z_send(0)
    fu.z_send(0)

    for dz in RING:
        for cc in (c, 1 - c)[dz == 0:]:
            drain(b.F.at[dz * 2 + cc], b.f_r.at[dz * 2 + cc])
    tot = sq = jnp.zeros((FEATS, ROWS), F32)
    for i in range(NG):
        v = b.F[i, :, :ROWS].astype(F32)
        tot, sq = tot + v, sq + v * v
    b.S[me] = jnp.concatenate([jnp.sum(v, axis=0, keepdims=True) for v in (tot, sq)], axis=0)
    for dy, dx in PAIRS:
        put(b.S.at[me], b.S.at[me], b.s_s, b.s_r, dict(y=flip(y, dy), x=flip(x, dx)))
    drain(b.S.at[first(NJ - 1)], b.s_r)
    stats = sum(b.S[i] for i in range(NJ)) / MODEL
    mean = stats[0:1]
    inv = lax.rsqrt(stats[1:2] - mean * mean + LN_EPS)
    for dz in RING:
        both = []
        for cc in range(NC):
            i = dz * 2 + cc
            both.append((b.F[i, :, :ROWS].astype(F32) - mean) * inv * b.F[i, :, ROWS:].astype(F32)[:, 0:1])
        b.hs[dz] = jnp.concatenate(both, axis=0).astype(BF16)

    mine = lambda d: pl.ds(pl.multiple_of(flip(x, d) * SUB, 16), SUB)
    A, B = first(SPLIT), pl.ds(SPLIT, ROWS - SPLIT)
    get(b.hs, b.hnT.at[:, 0, mine(0)], b.own_l)
    for d in AWAY:
        put(b.hs.at[:, :, A], b.hnT.at[:, 0, mine(0), A], b.ag_s.at[0], b.ag_r.at[0], dict(x=flip(x, d)))
        put(b.hs.at[:, :, B], b.hnT.at[:, d, mine(0), B], b.ag_s.at[1], b.ag_r.at[1], dict(y=flip(y, d)))
    fg.y_send()
    fq.z_second()
    part_a = lambda n: b.hnT.at[:, 0, first(n * SUB), A]
    part_b = lambda n: b.hnT.at[:, first(n), first(SUB), B]
    drain(b.hnT.at[:, 0, mine(0)], b.own_l)
    drain(part_a(3), b.ag_r.at[0])
    for d in AWAY:
        put(b.hnT.at[:, 0, :, A], b.hnT.at[:, d, :, A], b.ag_s.at[2], b.ag_r.at[2], dict(y=flip(y, d)))
    drain(part_b(3), b.ag_r.at[1])
    for d in AWAY:
        put(b.hnT.at[:, :, mine(0), B], b.hnT.at[:, :, mine(0), B], b.ag_s.at[3], b.ag_r.at[3], dict(x=flip(x, d)))
    all_a = b.hnT.at[:, first(3), :, A]
    all_b = b.hnT.at[:, :, first((NR - 1) * SUB), B]
    fu.y_send()
    fo_start()
    fd.y_send()
    fq.forward()
    fg.forward(0)
    fu.forward(0)
    fg.z_send(1)
    fg.z_send(2)
    fq.last()
    fd.z_send(0)
    fg.forward(1)
    fg.forward(2)
    fg.last(0)
    fu.last(0)

    drain(all_a, b.ag_r.at[2])
    drain(all_b, b.ag_r.at[3])

    def load_hn(dz, slot):
        get(b.hnT.at[dz], b.wt.at[slot, :, :, first(ROWS)], b.wsem.at[slot])

    def turn_hn(dz, slot):
        drain(b.wt.at[slot, :, :, first(ROWS)], b.wsem.at[slot])

        @pl.loop(0, ROWS // LANE)
        def _(r):
            at = pl.ds(pl.multiple_of(r * LANE, LANE), LANE)
            b.hn[dz, at, :] = b.wt[slot, :, :, at].reshape(KB, LANE).T

    load_hn(0, 0)
    for dz in RING:
        if dz < 3:
            load_hn(dz + 1, (dz + 1) % 2)
        turn_hn(dz, dz % 2)

    def load_q(i):
        fq.load(ORDER[i], b.wt.at[i % 2, first(2), :, first(QB)], b.wsem.at[i % 2])

    load_q(0)
    for i, dz in enumerate(ORDER):
        if i < 3:
            load_q(i + 1)
        w_at = (i % 2, first(2), slice(None), first(QB))
        drain(b.wt.at[w_at], b.wsem.at[i % 2])

        @pl.loop(0, ROWS // TILE)
        def _(r):
            at = pl.ds(pl.multiple_of(r * TILE, TILE), TILE)
            new = jnp.dot(b.hn[dz, at, :NB], b.wt[w_at].reshape(NB, QB), preferred_element_type=F32)
            if i:
                new += b.gacc[at, :QB]
            if i < 3:
                b.gacc[at, :QB] = new
            else:
                b.qout[pl.ds(r * 4, 4)] = new.astype(BF16).reshape(4, MINE, QB)
    for dy, dx in PAIRS:
        yy, xx = flip(y, dy), flip(x, dx)
        put(b.qout.at[yy * 4 + xx, :, first(NB)], b.q_in.at[me], b.q_s, b.q_r, dict(y=yy, x=xx))
    put(b.qout.at[flip(y, 2) * 4 + x, :, pl.ds(NB, 2 * HD)], b.kv_in.at[1], b.kv_s, b.kv_r, dict(y=flip(y, 2)))
    b.q_in[me] = b.qout[me, :, :NB]
    b.kv_in[0] = b.qout[me, :, NB:]

    def project(acc, i, slot):
        drain(b.wt.at[slot], b.wsem.at[slot])

        @pl.loop(0, ROWS // TILE)
        def _(r):
            at = pl.ds(pl.multiple_of(r * TILE, TILE), TILE)
            new = jnp.dot(b.hn[ORDER[i], at, :], b.wt[slot].reshape(KB, KB), preferred_element_type=F32)
            acc[at, :] = new + acc[at, :] if i else new

    fetch = lambda f, i, slot: f.load(ORDER[i], b.wt.at[slot], b.wsem.at[slot])
    fetch(fg, 0, 0)
    fu.z_send(1)
    fetch(fg, 1, 1)
    project(b.gacc, 0, 0)
    fu.z_send(2)
    fetch(fg, 2, 0)
    project(b.gacc, 1, 1)
    fo.z_first()
    fo.z_second()
    fg.last(1)
    fg.last(2)
    project(b.gacc, 2, 0)
    fetch(fg, 3, 1)
    fd.forward(0)
    fetch(fu, 0, 0)
    project(b.gacc, 3, 1)
    fd.z_send(1)
    fd.z_send(2)
    project(b.uacc, 0, 0)

    drain(b.kc, b.ld.at[1])
    drain(b.vc, b.ld.at[2])
    drain(b.q_in.at[first(NJ - 1)], b.q_r)
    drain(b.kv_in.at[1], b.kv_r)

    @pl.loop(0, MINE)
    def _(r):
        b.lenb[pl.ds(r, 1), :] = jnp.broadcast_to(lens[r], (1, HD)).astype(F32)
    i_half = lax.rem(lax.broadcasted_iota(jnp.int32, (MINE, HD), 1), HD // 2).astype(F32)
    angle = b.lenb[...] * jnp.power(ROPE_BASE, i_half * (-2.0 / HD))
    low = lax.broadcasted_iota(jnp.int32, (MINE, HD), 1) < HD // 2
    cos = jnp.cos(angle)
    sin = jnp.where(low, -jnp.sin(angle), jnp.sin(angle))
    rope = lambda v: v * cos + pltpu.roll(v, HD // 2, 1) * sin
    kv = (b.kv_in[0].astype(F32) + b.kv_in[1].astype(F32)).astype(BF16).astype(F32)
    b.kn[:, :HD] = rope(kv[:, :HD])
    b.kn[:, HD:] = kv[:, HD:]
    for xs in RING:
        for yh in range(NC):
            q = (b.q_in[yh * 4 + xs].astype(F32) + b.q_in[(yh + 2) * 4 + xs].astype(F32)).astype(BF16).astype(F32)
            for h in range(5):
                b.q3[pl.ds(xs * 10 + yh * 5 + h, MINE, stride=HEADS), :] = rope(q[:, h * HD:(h + 1) * HD])
    t_row = lax.broadcasted_iota(jnp.int32, (SEQ, HD), 0)
    t_col = lax.broadcasted_iota(jnp.int32, (HEADS, SEQ), 1)

    @pl.loop(0, MINE // 4)
    def _(step):
        for k in RING:
            r = step * 4 + k
            here = t_row == lens[r]
            new = b.kn[pl.ds(r, 1), :]
            keys = jnp.where(here, new[:, :HD].astype(BF16).astype(F32), b.kc[r].astype(F32)).astype(BF16)
            vals = jnp.where(here, new[:, HD:], b.vc[r].astype(F32)).astype(BF16)
            b.kc[r] = keys
            b.vc[r] = vals
            at = pl.ds(pl.multiple_of(r * HEADS, 8), HEADS)
            s = lax.dot_general(b.q3[at, :].astype(BF16), keys, NT, preferred_element_type=F32) * (HD ** -0.5)
            s = jnp.where(t_col <= lens[r], s, -1e30)
            e = jnp.exp(s - jnp.max(s, axis=1, keepdims=True))
            p = (e / jnp.sum(e, axis=1, keepdims=True)).astype(BF16)
            b.q3[at, :] = jnp.dot(p, vals, preferred_element_type=F32)
    get(b.kc, kc_o, b.out_l)
    get(b.vc, vc_o, b.out_l)
    for h in range(HEADS):
        b.o_v[:, h * HD:(h + 1) * HD] = b.q3[pl.ds(h, MINE, stride=HEADS), :].astype(BF16)
    block = lambda yy, xx: b.o_v.at[:, pl.ds(pl.multiple_of((xx * 2 + lax.rem(yy, 2)) * NB, LANE), NB)]
    for dy, dx in PAIRS:
        yy, xx = flip(y, dy), flip(x, dx)
        put(block(yy, xx), b.o_in.at[me], b.o_s, b.o_r, dict(y=yy, x=xx))
    b.o_in[me] = block(y, x)[...]

    fu.forward(1)
    fu.forward(2)
    fo.forward()
    fetch(fu, 1, 1)
    fetch(fu, 2, 0)
    project(b.uacc, 1, 1)
    fu.last(1)
    fu.last(2)
    project(b.uacc, 2, 0)
    fetch(fu, 3, 1)
    fetch(fd, 0, 0)
    load_o = lambda i: fo.load(ORDER[i], b.wo_t.at[i % 2], b.osem.at[i % 2])
    load_o(0)
    project(b.uacc, 3, 1)

    @pl.loop(0, ROWS // LANE)
    def _(r):
        at = pl.ds(pl.multiple_of(r * LANE, LANE), LANE)
        g = b.gacc[at, :].astype(BF16).astype(F32)
        b.act[at, :] = (g / (1.0 + jnp.exp(-g)) * b.uacc[at, :].astype(BF16).astype(F32)).astype(BF16)
    fd.forward(1)
    fd.forward(2)
    fo.last()

    drain(b.o_in.at[first(NJ - 1)], b.o_r)
    HA, HBk = first(CUT), pl.ds(CUT, ROWS - CUT)

    def multiply(i):
        dz, slot = ORDER[i], i % 2
        drain(b.wt.at[slot], b.wsem.at[slot])
        drain(b.wo_t.at[slot], b.osem.at[slot])
        if i > 1:
            old = ORDER[i - 2]
            drain(b.a1.at[old], b.a1s.at[old])
            drain(b.b1.at[old], b.b1s.at[old])

        def some(lo, hi):
            @pl.loop(lo // TILE, hi // TILE)
            def _(r):
                at = pl.ds(pl.multiple_of(r * TILE, TILE), TILE)
                out = lax.dot_general(b.wt[slot].reshape(KB, KB), b.act[at, :], NT, preferred_element_type=F32)
                rows = b.o_in[pl.ds(r * 4, 4)].reshape(TILE, NB)
                att = lax.dot_general(b.wo_t[slot].reshape(NB, NB), rows, NT, preferred_element_type=F32)
                b.sb[slot, first(2), :, at] = (out[:NB] + att).astype(BF16).reshape(2, HB, TILE)
                b.sb[slot, pl.ds(2, 2), :, at] = out[NB:].astype(BF16).reshape(2, HB, TILE)

        some(0, CUT)
        for d in AWAY:
            put(b.sb.at[slot, d, :, HA], b.a1.at[dz, d - 1], b.a1s.at[dz], b.a1r.at[dz], dict(y=flip(y, d)))
        some(CUT, ROWS)
        for d in AWAY:
            put(b.sb.at[slot, :, mine(d), HBk], b.b1.at[dz, d - 1], b.b1s.at[dz], b.b1r.at[dz], dict(x=flip(x, d)))

    def second(i):
        dz, slot = ORDER[i], i % 2
        drain(b.a1.at[dz], b.a1r.at[dz])
        get(b.a1.at[dz], b.va, b.vsem.at[0])
        drain(b.b1.at[dz], b.b1r.at[dz])
        get(b.b1.at[dz], b.vb, b.vsem.at[1])
        drain(b.va, b.vsem.at[0])
        b.s2a[dz] = (b.sb[slot, 0, :, HA].astype(F32) + three(b.va)).astype(BF16)
        for d in AWAY:
            put(b.s2a.at[dz, mine(d)], b.a2.at[dz, d - 1], b.a2s.at[dz], b.a2r.at[dz], dict(x=flip(x, d)))
        drain(b.vb, b.vsem.at[1])
        b.s2b[dz] = (b.sb[slot, :, mine(0), HBk].astype(F32) + three(b.vb)).astype(BF16)
        for d in AWAY:
            put(b.s2b.at[dz, d], b.b2.at[dz, d - 1], b.b2s.at[dz], b.b2r.at[dz], dict(y=flip(y, d)))

    def third(i):
        dz = ORDER[i]
        drain(b.a2.at[dz], b.a2r.at[dz])
        drain(b.b2.at[dz], b.b2r.at[dz])
        for src, own, lanes in ((b.a2, b.s2a[dz, mine(0)], HA), (b.b2, b.s2b[dz, 0], HBk)):
            total = own.astype(F32) + three(src.at[dz])
            for cc in range(NC):
                b.fs[dz, cc, :, lanes] = (b.F[dz * 2 + cc, :, lanes].astype(F32) + total[cc * FEATS:(cc + 1) * FEATS]).astype(BF16)
        at = z * 2 + c
        for cc in (c, 1 - c)[dz == 0:]:
            put(b.fs.at[dz, cc], b.fin.at[at], b.fin_s, b.fin_r.at[at], dict(z=flip(z, dz), c=cc))
        if dz == 0:
            b.fin[at] = b.fs[0, c]

    multiply(0)
    fetch(fd, 1, 1)
    load_o(1)
    fetch(fd, 2, 0)
    load_o(2)
    multiply(1)
    second(0)
    for g in range(3):
        fd.last(g)
    multiply(2)
    fetch(fd, 3, 1)
    load_o(3)
    second(1)
    third(0)
    multiply(3)
    second(2)
    third(1)
    second(3)
    third(2)
    third(3)

    for dz in AWAY + (0,):
        zz = flip(z, dz)
        for cc in (c, 1 - c)[dz == 0:]:
            drain(b.fin.at[zz * 2 + cc], b.fin_r.at[zz * 2 + cc])
        for p in range(NG):
            at = pl.ds(p * LANE, LANE)
            lo, hi = b.fin[zz * 2, :, at].astype(F32), b.fin[zz * 2 + 1, :, at].astype(F32)
            pair = [jnp.where(row_low, lo, pltpu.roll(hi, LANE // 2, 1)), jnp.where(row_low, pltpu.roll(lo, LANE // 2, 1), hi)]
            b.ov[:, pl.ds(pl.multiple_of(zz * 2 * ROWS + p * 2 * LANE, LANE), 2 * LANE)] = jnp.concatenate(pair, axis=1).astype(BF16)
    get(b.ov, outT, b.ld.at[0])

    drain(part_a(3), b.ag_s.at[0])
    drain(part_b(3), b.ag_s.at[1])
    drain(all_a, b.ag_s.at[2])
    drain(all_b, b.ag_s.at[3])
    drain(b.S.at[first(NJ - 1)], b.s_s)
    drain(b.F.at[first(7)], b.f_s)
    drain(b.q_in.at[first(NJ - 1)], b.q_s)
    drain(b.kv_in.at[1], b.kv_s)
    drain(b.o_in.at[first(NJ - 1)], b.o_s)
    for dz in ORDER:
        if dz in ORDER[2:]:
            drain(b.a1.at[dz], b.a1s.at[dz])
            drain(b.b1.at[dz], b.b1s.at[dz])
        drain(b.a2.at[dz], b.a2s.at[dz])
        drain(b.b2.at[dz], b.b2s.at[dz])
    drain(b.fin.at[first(7)], b.fin_s)
    for f in (fq, fg, fu, fd, fo):
        f.finish()
    for ref in (b.kc, b.vc):
        drain(ref, b.out_l)
    drain(b.ov, b.ld.at[0])


def solution(mesh):
    inner = Mesh(mesh.devices.reshape(4, 4, 4, 2), tuple('zyxc'))

    def layer(residual, ln_scale, w_query, w_key, w_value, w_gate, w_up, w_out, w_down, k_cache, v_cache, lengths):
        hbm = pl.BlockSpec(memory_space=pltpu.HBM)
        vmem = pl.BlockSpec(memory_space=pltpu.VMEM)
        smem = pl.BlockSpec(memory_space=pltpu.SMEM)
        shape = lambda a: jax.ShapeDtypeStruct(*a)
        outs = [((FEATS, BATCH), BF16), (k_cache.shape, BF16), (v_cache.shape, BF16)] + list(HBM_BUFS.values())
        res = pl.pallas_call(
            kernel,
            out_shape=[shape(a) for a in outs],
            in_specs=[hbm, vmem, smem] + [hbm] * 9,
            out_specs=[hbm] * len(outs),
            scratch_shapes=[pltpu.VMEM(*a) for a in VMEM_BUFS.values()] + [DMA(s) if s else DMA for s in SEMS.values()] + NARROW_SEMS + WIDE_SEMS * 3 + NARROW_SEMS,
            name='decode_layer',
            compiler_params=pltpu.CompilerParams(collective_id=0, has_side_effects=True, vmem_limit_bytes=67043328),
        )(residual.T, ln_scale.reshape(1, FEATS), lengths, w_query, w_key, w_value, w_gate, w_up, w_down.T, w_out.T, k_cache, v_cache)
        return res[0].T, res[1], res[2]

    rc, tx, tyz = tuple('zyxc'), tuple('zy'), tuple('xc')
    cache = P(rc, None, None)
    in_specs = (P(None, rc), P(rc), P(tx, tyz), P(tx, None), P(tx, None), P(tx, tyz), P(tx, tyz), P(tyz, tx), P(tyz, tx), cache, cache, P(rc))
    return jax.shard_map(layer, mesh=inner, in_specs=in_specs, out_specs=(P(None, rc), cache, cache), check_vma=False)
```

```python
import jax
import jax.numpy as jnp
from jax import lax
from jax.experimental import pallas as pl
from jax.experimental.pallas import tpu as pltpu
from jax.sharding import Mesh, PartitionSpec as P

LN_EPS = 1e-5
ROPE_BASE = 10000.0
MESH = pl.DeviceIdType.MESH
DMA = pltpu.SemaphoreType.DMA
F32, BF16 = jnp.float32, jnp.bfloat16
ROWS, MODEL, FEATS, BATCH = 1024, 5120, 40, 8192
KB, NB, HB, QB, HD, SUB = 1280, 640, 320, 896, 128, 80
MINE, SEQ, HEADS, LANE, HALF = 64, 64, 40, 128, 64
NR, NC, NJ, NG = 4, 2, 16, 8
X_FIRST = (1,)
CUT = 512
TILE = 256
RING = range(4)
AWAY = (1, 3, 2)
SIDES = AWAY[:2]
FORTH, BACK = ((1, 0), (3, 1)), ((3, 0), (1, 1))
GROUPS = ((0, 1), (1, 2), (2, 4))
ORDER = (0, 1, 3, 2)
PAIRS = tuple(sorted(((dy, dx) for dy in RING for dx in RING if dy or dx), key=lambda p: (p.count(2), 0 not in p, abs(p[0] - p[1]))))
NT = (((1,), (1,)), ((), ()))


def flip(i, d):
    return (i, i + 1 - 2 * lax.rem(i, 2), lax.rem(i + 2, 4), 3 - i)[d]


def put(src, dst, ssem, rsem, dev):
    pltpu.make_async_remote_copy(src_ref=src, dst_ref=dst, send_sem=ssem, recv_sem=rsem, device_id=dev, device_id_type=MESH).start()


def added(ref):
    return sum(ref[k].astype(F32) for k in range(NR - 1))


def get(src, dst, sem):
    pltpu.make_async_copy(src, dst, sem).start()


def first(n):
    return pl.ds(0, n)


def drain(ref, sem):
    pltpu.make_async_copy(ref, ref, sem).wait()


class Wide:
    def __init__(self, land, src, sems, pos):
        self.land, self.src = land, src
        self.send, self.yr, self.zr, self.fr, self.dr, self.loc = sems
        self.z, self.y, self.x, self.c = pos
        self.base = self.c * 16
        self.here = set()

    def piece(self, yy):
        return self.src.at[:, pl.ds(pl.multiple_of(yy * NB, LANE), NB)]

    def at(self, dz, g, base=None):
        lo, hi = GROUPS[g]
        return self.land.at[pl.ds((self.base if base is None else base) + dz * 4 + lo, hi - lo)]

    def start_local(self):
        get(self.piece(self.y), self.land.at[self.base], self.loc)

    def y_send(self):
        for dy in AWAY:
            yy = flip(self.y, dy)
            put(self.piece(yy), self.land.at[self.base + dy], self.send, self.yr.at[dy - 1], dict(y=yy))

    def z_send(self, g):
        if g:
            for dy in range(*GROUPS[g]):
                drain(self.land.at[self.base + dy], self.yr.at[dy - 1])
        for k, dz in enumerate(SIDES):
            to = dict(z=flip(self.z, dz))
            if g:
                put(self.at(0, g), self.at(dz, g), self.send, self.zr.at[k * 3 + g], to)
            else:
                put(self.piece(self.y), self.land.at[self.base + dz * 4], self.send, self.zr.at[k * 3], to)
        self.d2d(0, g)

    def forward(self, g):
        for k, dz in enumerate(SIDES):
            drain(self.at(dz, g), self.zr.at[k * 3 + g])
        for k, dz in enumerate(SIDES):
            put(self.half(dz, g, k), self.half(2, g, k), self.send, self.fr.at[g], dict(z=flip(self.z, AWAY[1 - k])))
            self.d2d(dz, g)

    def half(self, dz, g, k):
        lo, hi = GROUPS[g]
        return self.land.at[pl.ds(self.base + dz * 4 + lo, hi - lo), pl.ds(k * HB // 2, HB // 2)]

    def last(self, g):
        drain(self.at(2, g), self.fr.at[g])
        self.d2d(2, g)

    def d2d(self, dz, g):
        to = dict(c=1 - self.c)
        if dz or g:
            put(self.at(dz, g), self.at(dz, g), self.send, self.dr.at[dz * 3 + g], to)
        else:
            put(self.piece(self.y), self.land.at[self.base], self.send, self.dr.at[0], to)

    def load(self, dz, tile, sem):
        if dz not in self.here:
            if dz == 0:
                drain(self.land.at[self.base], self.loc)
            for g in range(len(GROUPS)):
                drain(self.at(dz, g, 16 - self.base), self.dr.at[dz * 3 + g])
        self.here.add(dz)
        for cc in range(NC):
            get(self.land.at[pl.ds(cc * 16 + dz * 4, 4)], tile.at[:, :, pl.ds(cc * NB, NB)], sem)

    def finish(self):
        drain(self.land.at[first(31)], self.send)


class Narrow:
    def __init__(self, land, parts, sems, pos):
        self.land, self.parts = land, parts
        self.send, self.yr, self.zr, self.fr, self.dr, self.loc = sems
        self.z, self.y, self.x, self.c = pos
        self.s = lax.rem(self.c + self.y, 2)

    def own(self, slot):
        lo = 0
        for ref in self.parts:
            hi = lo + ref.shape[1]
            yield ref, self.land.at[slot, :, pl.ds(lo, hi - lo)]
            lo = hi

    def start(self):
        @pl.when(self.s == 0)
        def _():
            for src, dst in self.own(0):
                get(src, dst, self.loc)

        @pl.when(self.s == 1)
        def _():
            for src, dst in self.own(1):
                put(src, dst, self.send, self.yr, dict(y=flip(self.y, 1), c=1 - self.c))

    def z_first(self):
        @pl.when(self.s == 0)
        def _():
            for k, dz in enumerate(SIDES):
                for (src, _), (_, dst) in zip(self.own(0), self.own(dz * 2)):
                    put(src, dst, self.send, self.zr.at[k], dict(z=flip(self.z, dz)))
            for src, dst in self.own(0):
                put(src, dst, self.send, self.dr.at[0], dict(c=1 - self.c))

    def z_second(self):
        @pl.when(self.s == 1)
        def _():
            src = self.land.at[1]
            drain(src, self.yr)
            for k, dz in enumerate(SIDES):
                put(src, self.land.at[dz * 2 + 1], self.send, self.zr.at[k], dict(z=flip(self.z, dz)))
            put(src, src, self.send, self.dr.at[0], dict(c=1 - self.c))

    def half(self, slot, k):
        return self.land.at[slot, pl.ds(k * HB // 2, HB // 2)]

    def forward(self):
        for k, dz in enumerate(SIDES):
            slot = dz * 2 + self.s
            piece = self.land.at[slot]
            drain(piece, self.zr.at[k])
            put(self.half(slot, k), self.half(4 + self.s, k), self.send, self.fr.at[k], dict(z=flip(self.z, AWAY[1 - k])))
            put(piece, piece, self.send, self.dr.at[1 + k], dict(c=1 - self.c))

    def last(self):
        for k in range(NC):
            piece = self.half(4 + self.s, k)
            drain(piece, self.fr.at[k])
            put(piece, piece, self.send, self.dr.at[3 + k], dict(c=1 - self.c))

    def load(self, dz, tile, sem):
        o = 1 - self.s
        if dz == 0:
            @pl.when(self.s == 0)
            def _():
                drain(self.land.at[0], self.loc)
        if dz == 2:
            for k in range(NC):
                drain(self.half(4 + o, k), self.dr.at[3 + k])
        else:
            drain(self.land.at[dz * 2 + o], self.dr.at[(dz + 1) // 2])
        get(self.land.at[pl.ds(dz * 2, 2)], tile, sem)

    def finish(self):
        for s in range(NC):
            @pl.when(self.s == s)
            def _():
                drain(self.land.at[first(7 + s)], self.send)


class Ring:
    def __init__(self, axis, at, own, land, moved, sems):
        self.axis, self.at, self.own, self.land, self.moved = axis, at, own, land, moved
        self.send, self.recv = sems

    def to(self, d):
        return {self.axis: flip(self.at, d)}

    def start(self):
        for k in range(NC):
            for d, h in ((1, k), (3, 1 - k)):
                put(self.own(h), self.land(d, h), self.send, self.recv.at[d - 1 + h], self.to(d))

    def forward(self):
        for d, h in FORTH:
            drain(self.moved(d, h), self.recv.at[d - 1 + h])
            put(self.moved(d, h), self.moved(2, h) if self.axis == 'y' else self.moved(d, h), self.send, self.recv.at[4 + h], self.to(4 - d))

    def finish(self):
        for d, h in BACK:
            drain(self.moved(d, h), self.recv.at[d - 1 + h])
        for h in range(NC):
            drain(self.moved(2, h), self.recv.at[4 + h])


WIDE_SEMS = [DMA, DMA((3,)), DMA((6,)), DMA((3,)), DMA((12,)), DMA]
NARROW_SEMS = [DMA, DMA, DMA((2,)), DMA((2,)), DMA((5,)), DMA]
HBM_BUFS = dict(
    Q=((NG, HB, QB), BF16), G=((NG * NR, HB, NB), BF16), U=((NG * NR, HB, NB), BF16), D=((NG * NR, HB, NB), BF16), O=((NG, HB, NB), BF16),
    hnT=((NR, NR, HB, ROWS), BF16), a1=((NR, NC, HB, CUT), BF16), b1=((NR, NC, NR, SUB, ROWS - CUT), BF16))
VMEM_BUFS = dict(
    rT=((FEATS, BATCH), BF16), xs=((NG, FEATS, ROWS + LANE), BF16), F=((NG, FEATS, ROWS + LANE), BF16), S=((NC, NJ, 2, CUT), F32),
    hs=((NR, SUB, ROWS), BF16), hn=((NR, ROWS, KB), BF16), wt=((NC, NR, HB, KB), BF16), wo_t=((NC, NC, HB, NB), BF16),
    gacc=((ROWS, KB), F32), uacc=((ROWS, KB), F32), qout=((NJ, MINE, QB), BF16), q_in=((NJ, MINE, NB), BF16), kv_in=((NC, MINE, 2 * HD), BF16),
    q3=((MINE * HEADS, HD), F32), lenb=((MINE, HD), F32), kc=((MINE, SEQ, HD), BF16), vc=((MINE, SEQ, HD), BF16), kn=((MINE, 2 * HD), F32),
    o_v=((MINE, MODEL), BF16), o_in=((NJ, MINE, NB), BF16), act=((ROWS, KB), BF16), sb=((NR - 1, NR, HB, ROWS), BF16),
    va=((NC, HB, CUT), BF16), vb=((NC, NR, SUB, ROWS - CUT), BF16),
    ta=((NR, NC, HB // 2, CUT), BF16), tb=((NR, NC, NR // 2, SUB, ROWS - CUT), BF16), s2a=((NR, HB, CUT), BF16), s2b=((NR, NR, SUB, ROWS - CUT), BF16),
    a2=((NR, NR - 1, SUB, CUT), BF16), b2=((NR, NR - 1, SUB, ROWS - CUT), BF16), fs=((NR, NC, FEATS, ROWS), BF16))
ONE, EACH, BY_GROUP = (), (NR,), (NG,)
SEMS = dict(f_s=ONE, fin_l=ONE, s_s=EACH, s_r=EACH, own_l=EACH, q_s=ONE, q_r=ONE, kv_s=ONE, kv_r=ONE, o_s=ONE, o_r=ONE, fin_s=ONE, out_l=ONE,
            a1s=EACH, a1r=EACH, b1s=EACH, b1r=EACH, a2s=EACH, a2r=EACH, b2s=EACH, b2r=EACH, ag_s=BY_GROUP, ag_r=(NG, NG), tas=EACH, tbs=EACH, tar=BY_GROUP, tbr=BY_GROUP, ld=EACH, wsem=EACH, osem=EACH, vsem=EACH,
            f_r=(NC, NG), fin_r=BY_GROUP)


def kernel(res, ls, lens, wq, wk, wv, wg, wu, wdT, woT, kc_h, vc_h, fin, kc_o, vc_o, *rest):
    rest = list(rest)

    class b:
        pass
    for name in list(HBM_BUFS) + list(VMEM_BUFS) + list(SEMS):
        setattr(b, name, rest.pop(0))
    pos = z, y, x, c = tuple(lax.axis_index(a) for a in 'zyxc')
    flow = lambda kind, land, src: kind(land, src, [rest.pop(0) for _ in WIDE_SEMS], pos)
    fq = flow(Narrow, b.Q, (wq, wk, wv))
    fg, fu, fd = flow(Wide, b.G, wg), flow(Wide, b.U, wu), flow(Wide, b.D, wdT)
    fo = flow(Narrow, b.O, (woT,))
    me = y * 4 + x
    row_low = lax.broadcasted_iota(jnp.int32, (FEATS, LANE), 1) < HALF
    sides = lambda dz: (c, 1 - c)[not dz:]

    bar = pltpu.get_barrier_semaphore()
    peers = [dict(z=flip(z, dz), c=cc) for dz in AWAY for cc in (c, 1 - c)] + [dict(c=1 - c), dict(y=flip(y, 1), c=1 - c)]
    peers += [dict(y=flip(y, dy), x=flip(x, dx)) for dy, dx in PAIRS]
    for p in peers:
        pl.semaphore_signal(bar, inc=1, device_id=p, device_id_type=MESH)
    get(res, b.rT, b.ld.at[0])
    get(kc_h, b.kc, b.ld.at[1])
    get(vc_h, b.vc, b.ld.at[2])
    for f in (fg, fu, fd):
        f.start_local()
    pl.semaphore_wait(bar, len(peers))
    fq.start()

    drain(b.rT, b.ld.at[0])
    scale = jnp.broadcast_to(ls[...].astype(F32), (LANE, FEATS)).T.astype(BF16)
    wide = lambda h: pl.ds(LANE * h + CUT * h, CUT + LANE * (1 - h))
    for i in range(NG):
        b.xs[i, :, :LANE] = scale
    for h in range(NC):
        for dz in AWAY + (0,):
            zz = flip(z, dz)
            for p in range(NR * h, NR * h + NR):
                pair = b.rT[:, pl.ds(pl.multiple_of(zz * NC * ROWS + p * TILE, LANE), TILE)].astype(F32)
                t0, t1 = pair[:, :LANE], pair[:, LANE:]
                at = pl.ds(LANE + p * LANE, LANE)
                b.xs[dz * NC, :, at] = jnp.where(row_low, t0, pltpu.roll(t1, HALF, 1)).astype(BF16)
                b.xs[dz * NC + 1, :, at] = jnp.where(row_low, pltpu.roll(t0, HALF, 1), t1).astype(BF16)
            for cc in sides(dz):
                put(b.xs.at[dz * NC + cc, :, wide(h)], b.F.at[dz * NC + c, :, wide(h)], b.f_s, b.f_r.at[h, dz * NC + c], dict(z=flip(z, dz), c=cc))
    b.F[c] = b.xs[c]
    fq.z_first()
    fg.z_send(0)

    for h in range(NC):
        for dz in RING:
            for cc in sides(dz):
                drain(b.F.at[dz * NC + cc, :, wide(h)], b.f_r.at[h, dz * NC + cc])
        tot = sq = jnp.zeros((FEATS, CUT), F32)
        for i in range(NG):
            v = b.F[i, :, pl.ds(LANE + CUT * h, CUT)].astype(F32)
            tot, sq = tot + v, sq + v * v
        b.S[h, me] = jnp.concatenate([jnp.sum(v, axis=0, keepdims=True) for v in (tot, sq)], axis=0)
        for dy, dx in PAIRS:
            put(b.S.at[h, me], b.S.at[h, me], b.s_s.at[h], b.s_r.at[h], dict(y=flip(y, dy), x=flip(x, dx)))
    fq.z_second()

    mine = lambda d: pl.ds(pl.multiple_of(flip(x, d) * SUB, 16), SUB)

    def normalize(h):
        drain(b.S.at[h, first(NJ - 1)], b.s_r.at[h])
        stats = sum(b.S[h, i] for i in range(NJ)) / MODEL
        mean = stats[0:1]
        inv = lax.rsqrt(stats[1:] - mean * mean + LN_EPS)
        lanes = pl.ds(CUT * h, CUT)
        for dz in RING:
            both = []
            for i in (dz * NC, dz * NC + 1):
                both.append((b.F[i, :, pl.ds(LANE + CUT * h, CUT)].astype(F32) - mean) * inv * b.F[i, :, :LANE].astype(F32)[:, :1])
            b.hs[dz, :, lanes] = jnp.concatenate(both, axis=0).astype(BF16)
        get(b.hs.at[:, :, lanes], b.hnT.at[:, 0, mine(0), lanes], b.own_l.at[h])

    part = lambda h: pl.ds(2 * h, 2)

    def rings(k):
        lanes = pl.ds(k * TILE, TILE)
        far = lambda d, h: b.hnT.at[part(h), :, mine(d), lanes]
        near = lambda d, h: b.hnT.at[part(h), d, mine(0), lanes]
        own = lambda h: b.hs.at[part(h), :, lanes]
        sems = [(b.ag_s.at[NC * k + j], b.ag_r.at[NC * k + j]) for j in range(NC)]
        if k in X_FIRST:
            spot = lambda d, h: b.hnT.at[part(h), 0, mine(d), lanes]
            row = lambda d, h: b.hnT.at[part(h), d, :, lanes]
            return Ring('x', x, own, lambda d, h: spot(0, h), spot, sems[0]), Ring('y', y, lambda h: row(0, h), row, row, sems[1])
        return Ring('y', y, own, near, near, sems[0]), Ring('x', x, lambda h: far(0, h), lambda d, h: far(0, h), far, sems[1])

    one, two = zip(*(rings(k) for k in RING))
    normalize(0)
    one[0].start()
    one[1].start()
    one[0].forward()
    one[1].forward()
    normalize(1)
    one[2].start()
    one[3].start()
    for h in range(NC):
        drain(b.hs.at[:, :, pl.ds(CUT * h, CUT)], b.own_l.at[h])
    one[0].finish()
    two[0].start()
    one[2].forward()
    one[3].forward()
    fg.y_send()
    one[1].finish()
    two[1].start()
    two[0].forward()
    fq.forward()
    fg.forward(0)
    one[2].finish()
    two[2].start()
    one[3].finish()
    fg.z_send(1)
    fq.last()

    def load_q(pair):
        for i in range(NC):
            fq.load(NC * pair + i, b.sb.at[pair, part(i), :, first(QB)], b.osem.at[pair])

    def stage(k):
        two[k].finish()
        for dz in RING:
            get(b.hnT.at[dz, :, :, pl.ds(k * TILE, TILE)], b.wt.at[1, :, :, pl.ds(dz * TILE, TILE)], b.wsem.at[1])

    def turn(k):
        drain(b.wt.at[1, :, :, first(ROWS)], b.wsem.at[1])
        for dz in RING:
            for h in range(NC):
                b.hn[dz, pl.ds(k * TILE + h * LANE, LANE), :] = b.wt[1, :, :, pl.ds(dz * TILE + h * LANE, LANE)].reshape(KB, LANE).T

    def query(k):
        at = pl.ds(k * TILE, TILE)
        new = sum(jnp.dot(b.hn[dz, at, :NB], b.sb[dz // 2, part(dz % 2), :, :QB].reshape(NB, QB), preferred_element_type=F32) for dz in RING)
        b.qout[pl.ds(k * NR, NR)] = new.astype(BF16).reshape(NR, MINE, QB)

    def project(acc, i, slot, lo=0, hi=ROWS, fresh=False, wait=True):
        if wait:
            drain(b.wt.at[slot], b.wsem.at[slot])

        @pl.loop(lo // TILE, hi // TILE)
        def _(r):
            at = pl.ds(pl.multiple_of(r * TILE, TILE), TILE)
            new = jnp.dot(b.hn[ORDER[i], at, :], b.wt[slot].reshape(KB, KB), preferred_element_type=F32)
            acc[at, :] = new if fresh else new + acc[at, :]

    fetch = lambda f, i, slot: f.load(ORDER[i], b.wt.at[slot], b.wsem.at[slot])
    fg.z_send(2)
    fu.z_send(0)
    load_q(0)
    load_q(1)
    stage(0)
    two[2].forward()
    two[3].start()
    turn(0)
    for pair in range(NC):
        drain(b.sb.at[pair, :, :, first(QB)], b.osem.at[pair])
    query(0)
    two[1].forward()
    fu.y_send()
    fg.forward(1)
    stage(2)
    turn(2)
    query(2)
    fetch(fg, 0, 0)
    two[3].forward()
    stage(1)
    turn(1)
    query(1)
    fg.forward(2)
    fg.last(0)
    project(b.gacc, 0, 0, 0, 3 * TILE, fresh=True)
    fu.z_send(1)
    fu.forward(0)
    fetch(fg, 1, 0)
    project(b.gacc, 1, 0, 0, 3 * TILE)
    fu.z_send(2)
    stage(3)
    turn(3)
    fetch(fg, 0, 1)
    query(3)
    for dy, dx in PAIRS:
        yy, xx = flip(y, dy), flip(x, dx)
        put(b.qout.at[yy * NR + xx, :, first(NB)], b.q_in.at[me], b.q_s, b.q_r, dict(y=yy, x=xx))
    put(b.qout.at[flip(y, 2) * NR + x, :, pl.ds(NB, 2 * HD)], b.kv_in.at[1], b.kv_s, b.kv_r, dict(y=flip(y, 2)))
    b.q_in[me] = b.qout[me, :, :NB]
    b.kv_in[0] = b.qout[me, :, NB:]
    fo.start()
    fd.y_send()

    project(b.gacc, 1, 0, 3 * TILE, ROWS, fresh=True, wait=False)
    fetch(fg, 2, 0)
    project(b.gacc, 0, 1, 3 * TILE, ROWS)
    fg.last(1)
    fg.last(2)
    fetch(fg, 3, 1)
    project(b.gacc, 2, 0)
    fu.forward(1)
    fetch(fu, 0, 0)
    project(b.gacc, 3, 1)
    project(b.uacc, 0, 0, fresh=True)
    drain(b.kc, b.ld.at[1])
    drain(b.vc, b.ld.at[2])
    drain(b.q_in.at[first(NJ - 1)], b.q_r)
    drain(b.kv_in.at[1], b.kv_r)

    @pl.loop(0, MINE)
    def _(r):
        b.lenb[pl.ds(r, 1), :] = jnp.broadcast_to(lens[r], (1, HD)).astype(F32)
    i_half = lax.rem(lax.broadcasted_iota(jnp.int32, (MINE, HD), 1), HALF).astype(F32)
    angle = b.lenb[...] * jnp.power(ROPE_BASE, i_half * (-2.0 / HD))
    low = lax.broadcasted_iota(jnp.int32, (MINE, HD), 1) < HALF
    cos = jnp.cos(angle)
    sin = jnp.where(low, -jnp.sin(angle), jnp.sin(angle))
    rope = lambda v: v * cos + pltpu.roll(v, HALF, 1) * sin
    kv = (b.kv_in[0].astype(F32) + b.kv_in[1].astype(F32)).astype(BF16).astype(F32)
    b.kn[:, :HD] = rope(kv[:, :HD])
    b.kn[:, HD:] = kv[:, HD:]
    for xs in RING:
        for yh in range(NC):
            q = (b.q_in[yh * 4 + xs].astype(F32) + b.q_in[(yh + 2) * 4 + xs].astype(F32)).astype(BF16).astype(F32)
            for h in range(5):
                b.q3[pl.ds(xs * 10 + yh * 5 + h, MINE, stride=HEADS), :] = rope(q[:, h * HD:(h + 1) * HD])
    t_row = lax.broadcasted_iota(jnp.int32, (SEQ, HD), 0)
    t_col = lax.broadcasted_iota(jnp.int32, (HEADS, SEQ), 1)

    def attend(r):
        here = t_row == lens[r]
        new = b.kn[pl.ds(r, 1), :]
        keys = jnp.where(here, new[:, :HD].astype(BF16).astype(F32), b.kc[r].astype(F32)).astype(BF16)
        vals = jnp.where(here, new[:, HD:], b.vc[r].astype(F32)).astype(BF16)
        b.kc[r] = keys
        b.vc[r] = vals
        at = pl.ds(pl.multiple_of(r * HEADS, 8), HEADS)
        s = lax.dot_general(b.q3[at, :].astype(BF16), keys, NT, preferred_element_type=F32) * (HD ** -0.5)
        s = jnp.where(t_col <= lens[r], s, -1e30)
        e = jnp.exp(s - jnp.max(s, axis=1, keepdims=True))
        p = (e / jnp.sum(e, axis=1, keepdims=True)).astype(BF16)
        b.q3[at, :] = jnp.dot(p, vals, preferred_element_type=F32)

    def attend_some(lo, hi):
        @pl.loop(lo // NR, hi // NR)
        def _(step):
            for k in RING:
                attend(step * NR + k)

    attend_some(0, MINE // 4)
    fu.forward(2)
    fo.z_first()
    fo.z_second()
    fd.z_send(0)
    fd.z_send(1)
    attend_some(MINE // 4, MINE)
    get(b.kc, kc_o, b.out_l)
    get(b.vc, vc_o, b.out_l)
    for h in range(HEADS):
        b.o_v[:, h * HD:(h + 1) * HD] = b.q3[pl.ds(h, MINE, stride=HEADS), :].astype(BF16)
    block = lambda yy, xx: b.o_v.at[:, pl.ds(pl.multiple_of((xx * 2 + lax.rem(yy, 2)) * NB, LANE), NB)]
    for dy, dx in PAIRS:
        yy, xx = flip(y, dy), flip(x, dx)
        put(block(yy, xx), b.o_in.at[me], b.o_s, b.o_r, dict(y=yy, x=xx))
    b.o_in[me] = block(y, x)[...]

    fd.z_send(2)
    fetch(fu, 1, 1)
    fetch(fu, 2, 0)
    project(b.uacc, 1, 1)
    fu.last(0)
    fu.last(1)
    fu.last(2)
    project(b.uacc, 2, 0)
    fetch(fu, 3, 1)
    fetch(fd, 0, 0)
    load_o = lambda i: fo.load(ORDER[i], b.wo_t.at[i % 2], b.osem.at[i % 2])
    load_o(0)
    project(b.uacc, 3, 1)

    @pl.loop(0, ROWS // LANE)
    def _(r):
        at = pl.ds(pl.multiple_of(r * LANE, LANE), LANE)
        g = b.gacc[at, :].astype(BF16).astype(F32)
        b.act[at, :] = (g / (1.0 + jnp.exp(-g)) * b.uacc[at, :].astype(BF16).astype(F32)).astype(BF16)
    fo.forward()

    drain(b.o_in.at[first(NJ - 1)], b.o_r)
    HA, HBk = first(CUT), pl.ds(CUT, ROWS - CUT)

    def sent(dz):
        for land, sem in ((b.a1, b.a1s), (b.b1, b.b1s), (b.ta, b.tas), (b.tb, b.tbs)):
            drain(land.at[dz], sem.at[dz])

    def multiply(i):
        dz, slot = ORDER[i], i % 2
        drain(b.wt.at[slot], b.wsem.at[slot])
        drain(b.wo_t.at[slot], b.osem.at[slot])
        if i == 3:
            sent(ORDER[0])

        def some(lo, hi):
            @pl.loop(lo // TILE, hi // TILE)
            def _(r):
                at = pl.ds(pl.multiple_of(r * TILE, TILE), TILE)
                out = lax.dot_general(b.wt[slot].reshape(KB, KB), b.act[at, :], NT, preferred_element_type=F32)
                rows = b.o_in[pl.ds(r * 4, 4)].reshape(TILE, NB)
                att = lax.dot_general(b.wo_t[slot].reshape(NB, NB), rows, NT, preferred_element_type=F32)
                b.sb[i % 3, first(2), :, at] = (out[:NB] + att).astype(BF16).reshape(2, HB, TILE)
                b.sb[i % 3, pl.ds(2, 2), :, at] = out[NB:].astype(BF16).reshape(2, HB, TILE)

        some(0, CUT)
        half = HB // 2
        for d, h in FORTH:
            rows = pl.ds(h * half, half)
            put(b.sb.at[i % 3, 2, rows, HA], b.ta.at[dz, h], b.tas.at[dz], b.tar.at[2 * dz + h], dict(y=flip(y, d)))
            put(b.sb.at[i % 3, d, rows, HA], b.a1.at[dz, h, rows], b.a1s.at[dz], b.a1r.at[dz], dict(y=flip(y, d)))
        some(CUT, ROWS)
        for d, h in FORTH:
            dys = pl.ds(2 * h, 2)
            put(b.sb.at[i % 3, dys, mine(2), HBk], b.tb.at[dz, h], b.tbs.at[dz], b.tbr.at[2 * dz + h], dict(x=flip(x, d)))
            put(b.sb.at[i % 3, dys, mine(d), HBk], b.b1.at[dz, h, dys], b.b1s.at[dz], b.b1r.at[dz], dict(x=flip(x, d)))

    def passed(i):
        dz, slot = ORDER[i], i % 3
        half = HB // 2
        for d, h in BACK:
            rows = pl.ds(h * half, half)
            drain(b.ta.at[dz, h], b.tar.at[2 * dz + h])
            b.sb[slot, d, rows, HA] = (b.sb[slot, d, rows, HA].astype(F32) + b.ta[dz, h].astype(F32)).astype(BF16)
            put(b.sb.at[slot, d, rows, HA], b.a1.at[dz, 1 - h, rows], b.a1s.at[dz], b.a1r.at[dz], dict(y=flip(y, d)))
        for d, h in BACK:
            dys = pl.ds(2 * h, 2)
            drain(b.tb.at[dz, h], b.tbr.at[2 * dz + h])
            b.sb[slot, dys, mine(d), HBk] = (b.sb[slot, dys, mine(d), HBk].astype(F32) + b.tb[dz, h].astype(F32)).astype(BF16)
            put(b.sb.at[slot, dys, mine(d), HBk], b.b1.at[dz, 1 - h, dys], b.b1s.at[dz], b.b1r.at[dz], dict(x=flip(x, d)))

    def second(i):
        dz, slot = ORDER[i], i % 3
        drain(b.a1.at[dz], b.a1r.at[dz])
        get(b.a1.at[dz], b.va, b.vsem.at[0])
        drain(b.b1.at[dz], b.b1r.at[dz])
        get(b.b1.at[dz], b.vb, b.vsem.at[1])
        drain(b.va, b.vsem.at[0])
        b.s2a[dz] = (b.sb[slot, 0, :, HA].astype(F32) + (b.va[0].astype(F32) + b.va[1].astype(F32))).astype(BF16)
        for d in AWAY:
            put(b.s2a.at[dz, mine(d)], b.a2.at[dz, d - 1], b.a2s.at[dz], b.a2r.at[dz], dict(x=flip(x, d)))
        drain(b.vb, b.vsem.at[1])
        b.s2b[dz] = (b.sb[slot, :, mine(0), HBk].astype(F32) + (b.vb[0].astype(F32) + b.vb[1].astype(F32))).astype(BF16)
        for d in AWAY:
            put(b.s2b.at[dz, d], b.b2.at[dz, d - 1], b.b2s.at[dz], b.b2r.at[dz], dict(y=flip(y, d)))

    def third(i):
        dz = ORDER[i]
        drain(b.a2.at[dz], b.a2r.at[dz])
        drain(b.b2.at[dz], b.b2r.at[dz])
        for src, own, lanes, shifted in ((b.a2, b.s2a[dz, mine(0)], HA, pl.ds(LANE, CUT)), (b.b2, b.s2b[dz, 0], HBk, pl.ds(LANE + CUT, ROWS - CUT))):
            total = own.astype(F32) + added(src.at[dz])
            for cc in range(NC):
                b.fs[dz, cc, :, lanes] = (b.F[dz * 2 + cc, :, shifted].astype(F32) + total[cc * FEATS:(cc + 1) * FEATS]).astype(BF16)
        at = z * 2 + c
        for cc in sides(dz):
            put(b.fs.at[dz, cc], fin.at[at], b.fin_s, b.fin_r.at[at], dict(z=flip(z, dz), c=cc))
        if dz == 0:
            get(b.fs.at[0, c], fin.at[at], b.fin_l)

    multiply(0)
    passed(0)
    fd.forward(0)
    fd.forward(1)
    second(0)
    fd.forward(2)
    fetch(fd, 1, 1)
    load_o(1)
    fetch(fd, 2, 0)
    load_o(2)
    multiply(1)
    multiply(2)
    passed(1)
    for g in range(len(GROUPS)):
        fd.last(g)
    fo.last()
    fetch(fd, 3, 1)
    load_o(3)
    passed(2)
    multiply(3)
    second(1)
    passed(3)
    second(2)
    third(0)
    third(1)
    second(3)
    third(2)
    third(3)

    for dz in AWAY + (0,):
        for cc in sides(dz):
            at = flip(z, dz) * NC + cc
            drain(fin.at[at], b.fin_r.at[at])
    drain(fin.at[0], b.fin_l)

    some, tile = first(NR - 1), first(TILE)
    for k in RING:
        drain(b.hnT.at[some, 0, :, tile], b.ag_s.at[NC * k])
        drain(b.hnT.at[some, :, :, tile], b.ag_s.at[NC * k + 1])
    for h in range(NC):
        drain(b.S.at[h, first(NJ - 1)], b.s_s.at[h])
    drain(b.F.at[first(NG - 1)], b.f_s)
    drain(b.q_in.at[first(NJ - 1)], b.q_s)
    drain(b.kv_in.at[1], b.kv_s)
    drain(b.o_in.at[first(NJ - 1)], b.o_s)
    for dz in ORDER:
        if dz:
            sent(dz)
        drain(b.a2.at[dz], b.a2s.at[dz])
        drain(b.b2.at[dz], b.b2s.at[dz])
    drain(fin.at[first(NG - 1)], b.fin_s)
    for f in (fq, fg, fu, fd, fo):
        f.finish()
    for ref in (b.kc, b.vc):
        drain(ref, b.out_l)


def finish(fin, kc_h, vc_h, out, kc_o, vc_o, fin_v, kc, vc, ov, sem):
    get(fin, fin_v, sem.at[0])
    get(kc_h, kc, sem.at[1])
    get(vc_h, vc, sem.at[2])
    drain(fin_v, sem.at[0])
    row_low = lax.broadcasted_iota(jnp.int32, (FEATS, LANE), 1) < HALF
    for zz in RING:
        for p in range(NG):
            lo, hi = (fin_v[zz * NC + cc, :, pl.ds(p * LANE, LANE)].astype(F32) for cc in range(NC))
            pair = [jnp.where(row_low, lo, pltpu.roll(hi, HALF, 1)), jnp.where(row_low, pltpu.roll(lo, HALF, 1), hi)]
            ov[:, pl.ds(zz * NC * ROWS + p * TILE, TILE)] = jnp.concatenate(pair, axis=1).astype(BF16)
    drain(kc, sem.at[1])
    get(kc, kc_o, sem.at[1])
    drain(vc, sem.at[2])
    get(vc, vc_o, sem.at[2])
    get(ov, out, sem.at[0])
    for i, ref in enumerate((ov, kc, vc)):
        drain(ref, sem.at[i])


def solution(mesh):
    inner = Mesh(mesh.devices.reshape(4, 4, 4, 2), tuple('zyxc'))

    def layer(residual, ln_scale, w_query, w_key, w_value, w_gate, w_up, w_out, w_down, k_cache, v_cache, lengths):
        hbm = pl.BlockSpec(memory_space=pltpu.HBM)
        vmem = pl.BlockSpec(memory_space=pltpu.VMEM)
        smem = pl.BlockSpec(memory_space=pltpu.SMEM)
        shape = lambda a: jax.ShapeDtypeStruct(*a)
        results = [((FEATS, BATCH), BF16), (k_cache.shape, BF16), (v_cache.shape, BF16)]
        fin = ((NG, FEATS, ROWS), BF16)
        outs = [fin] + results[1:] + list(HBM_BUFS.values())
        got = pl.pallas_call(
            kernel,
            out_shape=[shape(a) for a in outs],
            in_specs=[hbm, vmem, smem] + [hbm] * 9,
            out_specs=[hbm] * len(outs),
            scratch_shapes=[pltpu.VMEM(*a) for a in VMEM_BUFS.values()] + [DMA(s) if s else DMA for s in SEMS.values()] + NARROW_SEMS + WIDE_SEMS * 3 + NARROW_SEMS,
            name='decode_layer',
            compiler_params=pltpu.CompilerParams(collective_id=0, has_side_effects=True, vmem_limit_bytes=67043328),
        )(residual.T, ln_scale.reshape(1, FEATS), lengths, w_query, w_key, w_value, w_gate, w_up, w_down.T, w_out.T, k_cache, v_cache)
        out, k_new, v_new = pl.pallas_call(
            finish,
            out_shape=[shape(a) for a in results],
            in_specs=[hbm] * 3,
            out_specs=[hbm] * 3,
            scratch_shapes=[pltpu.VMEM(*a) for a in [fin] + results[1:] + results[:1]] + [DMA((3,))],
            name='finish',
        )(*got[:3])
        return out.T, k_new, v_new

    rc, tx, tyz = tuple('zyxc'), tuple('zy'), tuple('xc')
    cache = P(rc, None, None)
    in_specs = (P(None, rc), P(rc), P(tx, tyz), P(tx, None), P(tx, None), P(tx, tyz), P(tx, tyz), P(tyz, tx), P(tyz, tx), cache, cache, P(rc))
    return jax.shard_map(layer, mesh=inner, in_specs=in_specs, out_specs=(P(None, rc), cache, cache), check_vma=False)
```

```python
import jax
import jax.numpy as jnp
from jax import lax
from jax.experimental import pallas as pl
from jax.experimental.pallas import tpu as pltpu
from jax.sharding import Mesh, PartitionSpec as P

LN_EPS = 1e-5
ROPE_BASE = 10000.0
MESH = pl.DeviceIdType.MESH
DMA = pltpu.SemaphoreType.DMA
F32, BF16 = jnp.float32, jnp.bfloat16
ROWS, MODEL, FEATS, BATCH = 1024, 5120, 40, 8192
KB, NB, HB, HD, SUB = 1280, 640, 320, 128, 80
MINE, SEQ, HEADS, LANE, HALF = 64, 64, 40, 128, 64
NR, NC, NJ, NG = 4, 2, 16, 8
X_FIRST = (1,)
CUT = 512
TILE = 256
RING = range(4)
N0, N1, N2, N3 = RING
AWAY = (1, 3, 2)
SIDES = AWAY[:2]
FORTH, BACK = ((1, 0), (3, 1)), ((3, 0), (1, 1))
GROUPS = ((0, 1), (1, 2), (2, 4))
SINGLE = ((0, 1), (1, 2), (2, 3), (3, 4))
ORDER = (0, 1, 3, 2)
BOTH = NEAR, FAR = (0, 1)
TURNED = 2
PAIRS = tuple(sorted(((dy, dx) for dy in RING for dx in RING if dy or dx), key=lambda p: (p.count(2), 0 not in p, abs(p[0] - p[1]))))
NT = (((1,), (1,)), ((), ()))


def flip(i, d):
    return (i, i + 1 - 2 * lax.rem(i, 2), lax.rem(i + 2, 4), 3 - i)[d]


def put(src, dst, ssem, rsem, dev):
    pltpu.make_async_remote_copy(src_ref=src, dst_ref=dst, send_sem=ssem, recv_sem=rsem, device_id=dev, device_id_type=MESH).start()


def added(ref):
    return sum(ref[k].astype(F32) for k in range(NR - 1))


def get(src, dst, sem):
    pltpu.make_async_copy(src, dst, sem).start()


def first(n):
    return pl.ds(0, n)


def drain(ref, sem):
    pltpu.make_async_copy(ref, ref, sem).wait()


class Wide:
    def __init__(self, land, src, sems, pos, groups=GROUPS):
        self.land, self.src = land, src
        self.send, self.yr, self.zr, self.fr, self.dr, self.loc = sems
        self.z, self.y, self.x, self.c = pos
        self.base = self.c * 16
        self.groups = groups
        self.here = set()

    def piece(self, yy):
        return self.src.at[:, pl.ds(pl.multiple_of(yy * NB, LANE), NB)]

    def at(self, dz, g, base=None):
        lo, hi = self.groups[g]
        return self.land.at[pl.ds((self.base if base is None else base) + dz * 4 + lo, hi - lo)]

    def start_local(self):
        get(self.piece(self.y), self.land.at[self.base], self.loc)

    def y_send(self, order=AWAY):
        for dy in order:
            yy = flip(self.y, dy)
            put(self.piece(yy), self.land.at[self.base + dy], self.send, self.yr.at[dy - 1], dict(y=yy))

    def z_send(self, g):
        self.wait_y(g)
        for dz in SIDES:
            self.z_put(g, dz)

    def wait_y(self, g):
        if g:
            for dy in range(*self.groups[g]):
                drain(self.land.at[self.base + dy], self.yr.at[dy - 1])
        self.d2d(0, g)

    def z_put(self, g, dz):
        src = self.at(0, g) if g else self.piece(self.y)
        dst = self.at(dz, g) if g else self.land.at[self.base + dz * 4]
        put(src, dst, self.send, self.zr.at[dz // 2 * len(self.groups) + g], dict(z=flip(self.z, dz)))

    def arrive(self, dz, g):
        drain(self.at(dz, g), self.zr.at[dz // 2 * len(self.groups) + g])
        self.d2d(dz, g)

    def forward(self, g):
        for dz in SIDES:
            self.arrive(dz, g)
        self.pass_on(g)

    def pass_on(self, g, *sides):
        for k, dz in enumerate(SIDES):
            src, dst = (self.at(dz, g), self.at(2, g)) if sides else (self.half(dz, g, k), self.half(2, g, k))
            if dz in (sides or SIDES):
                put(src, dst, self.send, self.fr.at[g], dict(z=flip(self.z, 4 - dz)))

    def half(self, dz, g, k):
        lo, hi = self.groups[g]
        return self.land.at[pl.ds(self.base + dz * 4 + lo, hi - lo), pl.ds(k * HB // 2, HB // 2)]

    def last(self, g):
        drain(self.at(2, g), self.fr.at[g])
        self.d2d(2, g)

    def d2d(self, dz, g):
        to = dict(c=1 - self.c)
        if dz or g:
            put(self.at(dz, g), self.at(dz, g), self.send, self.dr.at[dz * len(self.groups) + g], to)
        else:
            put(self.piece(self.y), self.land.at[self.base], self.send, self.dr.at[0], to)

    def ready(self, dz, g):
        if (dz, g) not in self.here:
            if dz == g == 0:
                drain(self.land.at[self.base], self.loc)
            drain(self.at(dz, g, 16 - self.base), self.dr.at[dz * len(self.groups) + g])
        self.here.add((dz, g))

    def load(self, dz, tile, sem):
        for g in range(len(self.groups)):
            self.ready(dz, g)
        self.bring(dz, 0, NR, tile, sem)

    def bring(self, dz, lo, n, tile, sem):
        for cc in range(NC):
            get(self.land.at[pl.ds(cc * 16 + dz * NR + lo, n)], tile.at[:, :, pl.ds(cc * NB, NB)], sem)

    def finish(self):
        drain(self.land.at[first(31)], self.send)


class Narrow:
    def __init__(self, land, parts, sems, pos):
        self.land, self.parts = land, parts
        self.send, self.yr, self.zr, self.fr, self.dr, self.loc = sems
        self.z, self.y, self.x, self.c = pos
        self.s = lax.rem(self.c + self.y, 2)

    def own(self, slot):
        lo = 0
        for ref in self.parts:
            hi = lo + ref.shape[1]
            yield ref, self.land.at[slot, :, pl.ds(lo, hi - lo)]
            lo = hi

    def start(self):
        @pl.when(self.s == 0)
        def _():
            for src, dst in self.own(0):
                get(src, dst, self.loc)

        @pl.when(self.s == 1)
        def _():
            for src, dst in self.own(1):
                put(src, dst, self.send, self.yr, dict(y=flip(self.y, 1), c=1 - self.c))

    def z_first(self):
        @pl.when(self.s == 0)
        def _():
            for k, dz in enumerate(SIDES):
                for (src, _), (_, dst) in zip(self.own(0), self.own(dz * 2)):
                    put(src, dst, self.send, self.zr.at[k], dict(z=flip(self.z, dz)))
            for src, dst in self.own(0):
                put(src, dst, self.send, self.dr.at[0], dict(c=1 - self.c))

    def z_second(self):
        @pl.when(self.s == 1)
        def _():
            src = self.land.at[1]
            drain(src, self.yr)
            for k, dz in enumerate(SIDES):
                put(src, self.land.at[dz * 2 + 1], self.send, self.zr.at[k], dict(z=flip(self.z, dz)))
            put(src, src, self.send, self.dr.at[0], dict(c=1 - self.c))

    def half(self, slot, k):
        return self.land.at[slot, pl.ds(k * HB // 2, HB // 2)]

    def forward(self):
        for k, dz in enumerate(SIDES):
            slot = dz * 2 + self.s
            piece = self.land.at[slot]
            drain(piece, self.zr.at[k])
            put(self.half(slot, k), self.half(4 + self.s, k), self.send, self.fr.at[k], dict(z=flip(self.z, AWAY[1 - k])))
            put(piece, piece, self.send, self.dr.at[1 + k], dict(c=1 - self.c))

    def last(self):
        for k in range(NC):
            piece = self.half(4 + self.s, k)
            drain(piece, self.fr.at[k])
            put(piece, piece, self.send, self.dr.at[3 + k], dict(c=1 - self.c))

    def load(self, dz, tile, sem):
        o = 1 - self.s
        if dz == 0:
            @pl.when(self.s == 0)
            def _():
                drain(self.land.at[0], self.loc)
        if dz == 2:
            for k in range(NC):
                drain(self.half(4 + o, k), self.dr.at[3 + k])
        else:
            drain(self.land.at[dz * 2 + o], self.dr.at[(dz + 1) // 2])
        get(self.land.at[pl.ds(dz * 2, 2)], tile, sem)

    def finish(self):
        for s in range(NC):
            @pl.when(self.s == s)
            def _():
                drain(self.land.at[first(7 + s)], self.send)


class Ring:
    def __init__(self, axis, at, own, land, moved, sems):
        self.axis, self.at, self.own, self.land, self.moved = axis, at, own, land, moved
        self.send, self.recv = sems

    def to(self, d):
        return {self.axis: flip(self.at, d)}

    def start(self):
        for k in range(NC):
            for d, h in ((1, k), (3, 1 - k)):
                put(self.own(h), self.land(d, h), self.send, self.recv.at[d - 1 + h], self.to(d))

    def forward(self):
        for d, h in FORTH:
            drain(self.moved(d, h), self.recv.at[d - 1 + h])
            put(self.moved(d, h), self.moved(2, h) if self.axis == 'y' else self.moved(d, h), self.send, self.recv.at[4 + h], self.to(4 - d))

    def finish(self):
        for d, h in BACK:
            drain(self.moved(d, h), self.recv.at[d - 1 + h])
        for h in range(NC):
            drain(self.moved(2, h), self.recv.at[4 + h])


WIDE_SEMS, SINGLE_SEMS = ([DMA, DMA((NR - 1,)), DMA((2 * n,)), DMA((n,)), DMA((NR * n,)), DMA] for n in map(len, (GROUPS, SINGLE)))
NARROW_SEMS = [DMA, DMA, DMA((2,)), DMA((2,)), DMA((5,)), DMA]
HBM_BUFS = dict(
    Q=((NG, HB, NB), BF16), G=((NG * NR, HB, NB), BF16), U=((NG * NR, HB, NB), BF16), D=((NG * NR, HB, NB), BF16), O=((NG, HB, NB), BF16),
    hnT=((NR, NR, HB, ROWS), BF16), a1=((NR, NC, HB, CUT), BF16), b1=((NR, NC, NR, SUB, ROWS - CUT), BF16))
VMEM_BUFS = dict(
    rT=((FEATS, BATCH), BF16), xs=((NG, FEATS, ROWS + LANE), BF16), F=((NG, FEATS, ROWS + LANE), BF16), S=((NC, NJ, 2, CUT), F32),
    hs=((NR, SUB, ROWS), BF16), hn=((NR, ROWS, KB), BF16), wt=((NC, NR, HB, KB), BF16), wo_t=((NC, NC, HB, NB), BF16),
    gacc=((ROWS, KB), F32), uacc=((ROWS, KB), F32), qout=((NJ, MINE, NB), BF16), kvout=((NJ, MINE, 2 * HD), BF16), kvw=((NC, NC, HB, HD), BF16), q_in=((NJ, MINE, NB), BF16), kv_in=((NG, MINE, 2 * HD), BF16),
    q3=((MINE * HEADS, HD), F32), lenb=((MINE, HD), F32), kc=((MINE, SEQ, HD), BF16), vc=((MINE, SEQ, HD), BF16), kn=((MINE, 2 * HD), F32),
    o_v=((MINE, MODEL), BF16), o_in=((NJ, MINE, NB), BF16), act=((ROWS, KB), BF16), sb=((NR - 1, NR, HB, ROWS), BF16),
    va=((NC, NC, HB, CUT), BF16), vb=((NC, NC, NR, SUB, ROWS - CUT), BF16),
    ta=((NR, NC, HB // 2, CUT), BF16), tb=((NR, NC, NR // 2, SUB, ROWS - CUT), BF16), s2a=((NR, HB, CUT), BF16), s2b=((NR, NR, SUB, ROWS - CUT), BF16),
    a2=((NR, NR - 1, SUB, CUT), BF16), b2=((NR, NR - 1, SUB, ROWS - CUT), BF16), fs=((NR, NC, FEATS, ROWS), BF16))
ONE, EACH, BY_GROUP = (), (NR,), (NG,)
SEMS = dict(f_s=ONE, fin_l=ONE, s_s=EACH, s_r=EACH, own_l=EACH, q_s=ONE, kw_s=ONE, kw_z=ONE, kw_y=ONE, kw_c=EACH, q_r=ONE, kv_s=ONE, kv_r=ONE, o_s=ONE, o_r=ONE, fin_s=ONE, out_l=ONE,
            a1s=EACH, b1s=EACH, a2s=EACH, a2r=EACH, b2s=EACH, b2r=EACH, ag_s=BY_GROUP, ag_r=(NG, NG), tas=EACH, tbs=EACH, tar=(NR, NC), tbr=(NR, NC), b1r=(NR, NC), a1r=(NR, NC), ld=EACH, wsem=EACH, osem=EACH, vsem=BY_GROUP,
            f_r=(NC, NG), fin_r=BY_GROUP)


def kernel(res, ls, lens, wq, wk, wv, wg, wu, wdT, woT, kc_h, vc_h, fin, kc_o, vc_o, *rest):
    rest = list(rest)

    class b:
        pass
    for name in list(HBM_BUFS) + list(VMEM_BUFS) + list(SEMS):
        setattr(b, name, rest.pop(0))
    pos = z, y, x, c = tuple(lax.axis_index(a) for a in 'zyxc')
    flow = lambda kind, land, src, *more: kind(land, src, [rest.pop(0) for _ in WIDE_SEMS], pos, *more)
    fq = flow(Narrow, b.Q, (wq,))
    fg, fu, fd = flow(Wide, b.G, wg), flow(Wide, b.U, wu), flow(Wide, b.D, wdT, SINGLE)
    fo = flow(Narrow, b.O, (woT,))
    me = y * 4 + x
    row_low = lax.broadcasted_iota(jnp.int32, (FEATS, LANE), 1) < HALF
    sides = lambda dz: (c, 1 - c)[not dz:]

    bar = pltpu.get_barrier_semaphore()
    peers = [dict(z=flip(z, dz), c=cc) for dz in AWAY for cc in (c, 1 - c)] + [dict(c=1 - c), dict(y=flip(y, 1), c=1 - c)]
    peers += [dict(y=flip(y, dy), x=flip(x, dx)) for dy, dx in PAIRS]
    for p in peers:
        pl.semaphore_signal(bar, inc=1, device_id=p, device_id_type=MESH)
    get(res, b.rT, b.ld.at[0])
    get(kc_h, b.kc, b.ld.at[1])
    get(vc_h, b.vc, b.ld.at[2])
    for f in (fg, fu, fd):
        f.start_local()
    pl.semaphore_wait(bar, len(peers))
    fq.start()

    drain(b.rT, b.ld.at[0])
    scale = jnp.broadcast_to(ls[...].astype(F32), (LANE, FEATS)).T.astype(BF16)
    wide = lambda h: pl.ds(LANE * h + CUT * h, CUT + LANE * (1 - h))
    for i in range(NG):
        b.xs[i, :, :LANE] = scale
    for h in range(NC):
        for dz in AWAY + (0,):
            zz = flip(z, dz)
            for p in range(NR * h, NR * h + NR):
                pair = b.rT[:, pl.ds(pl.multiple_of(zz * NC * ROWS + p * TILE, LANE), TILE)].astype(F32)
                t0, t1 = pair[:, :LANE], pair[:, LANE:]
                at = pl.ds(LANE + p * LANE, LANE)
                b.xs[dz * NC, :, at] = jnp.where(row_low, t0, pltpu.roll(t1, HALF, 1)).astype(BF16)
                b.xs[dz * NC + 1, :, at] = jnp.where(row_low, pltpu.roll(t0, HALF, 1), t1).astype(BF16)
            for cc in sides(dz):
                put(b.xs.at[dz * NC + cc, :, wide(h)], b.F.at[dz * NC + c, :, wide(h)], b.f_s, b.f_r.at[h, dz * NC + c], dict(z=flip(z, dz), c=cc))
    b.F[c] = b.xs[c]
    def kv_half(slot, side):
        return b.kvw.at[slot, side]

    for side, w in enumerate((wk, wv)):
        @pl.when((c == side) & (x == 0))
        def _():
            get(w, kv_half(0, side), b.kw_z)

        @pl.when((c == side) & (x > 0))
        def _():
            zx = lax.rem(z // 2 + x // 2, 2) * 2 + lax.rem(z + x, 2)
            put(w, kv_half(0, side), b.kw_s, b.kw_z, dict(z=zx))
    fq.z_first()
    fg.z_send(0)

    for h in range(NC):
        for dz in RING:
            for cc in sides(dz):
                drain(b.F.at[dz * NC + cc, :, wide(h)], b.f_r.at[h, dz * NC + cc])
        tot = sq = jnp.zeros((FEATS, CUT), F32)
        for i in range(NG):
            v = b.F[i, :, pl.ds(LANE + CUT * h, CUT)].astype(F32)
            tot, sq = tot + v, sq + v * v
        b.S[h, me] = jnp.concatenate([jnp.sum(v, axis=0, keepdims=True) for v in (tot, sq)], axis=0)
        for dy, dx in PAIRS:
            put(b.S.at[h, me], b.S.at[h, me], b.s_s.at[h], b.s_r.at[h], dict(y=flip(y, dy), x=flip(x, dx)))
    fq.z_second()
    fo.z_first()

    mine = lambda d: pl.ds(pl.multiple_of(flip(x, d) * SUB, 16), SUB)

    def normalize(h):
        drain(b.S.at[h, first(NJ - 1)], b.s_r.at[h])
        stats = sum(b.S[h, i] for i in range(NJ)) / MODEL
        mean = stats[0:1]
        inv = lax.rsqrt(stats[1:] - mean * mean + LN_EPS)
        lanes = pl.ds(CUT * h, CUT)
        for dz in RING:
            both = []
            for i in (dz * NC, dz * NC + 1):
                both.append((b.F[i, :, pl.ds(LANE + CUT * h, CUT)].astype(F32) - mean) * inv * b.F[i, :, :LANE].astype(F32)[:, :1])
            b.hs[dz, :, lanes] = jnp.concatenate(both, axis=0).astype(BF16)
        get(b.hs.at[:, :, lanes], b.hnT.at[:, 0, mine(0), lanes], b.own_l.at[h])

    part = lambda h: pl.ds(2 * h, 2)

    def rings(k):
        lanes = pl.ds(k * TILE, TILE)
        far = lambda d, h: b.hnT.at[part(h), :, mine(d), lanes]
        near = lambda d, h: b.hnT.at[part(h), d, mine(0), lanes]
        own = lambda h: b.hs.at[part(h), :, lanes]
        sems = [(b.ag_s.at[NC * k + j], b.ag_r.at[NC * k + j]) for j in range(NC)]
        if k in X_FIRST:
            spot = lambda d, h: b.hnT.at[part(h), 0, mine(d), lanes]
            row = lambda d, h: b.hnT.at[part(h), d, :, lanes]
            return Ring('x', x, own, lambda d, h: spot(0, h), spot, sems[0]), Ring('y', y, lambda h: row(0, h), row, row, sems[1])
        return Ring('y', y, own, near, near, sems[0]), Ring('x', x, lambda h: far(0, h), lambda d, h: far(0, h), far, sems[1])

    one, two = zip(*(rings(k) for k in RING))
    normalize(0)
    one[0].start()
    one[1].start()
    one[0].forward()
    one[1].forward()
    normalize(1)
    one[2].start()
    one[3].start()
    for h in range(NC):
        drain(b.hs.at[:, :, pl.ds(CUT * h, CUT)], b.own_l.at[h])
    one[0].finish()
    two[0].start()
    one[2].forward()
    one[3].forward()
    drain(kv_half(0, c), b.kw_z)
    put(kv_half(0, c), kv_half(1, c), b.kw_s, b.kw_y, dict(y=flip(y, 1)))
    put(kv_half(0, c), kv_half(0, c), b.kw_s, b.kw_c.at[0], dict(c=1 - c))
    fg.y_send()
    one[1].finish()
    two[1].start()
    two[0].forward()
    fq.forward()
    fg.forward(0)
    one[2].finish()
    two[2].start()
    one[3].finish()
    fg.z_send(1)
    fq.last()
    drain(kv_half(1, c), b.kw_y)
    put(kv_half(1, c), kv_half(1, c), b.kw_s, b.kw_c.at[1], dict(c=1 - c))

    def load_q(pair):
        for i in range(NC):
            fq.load(NC * pair + i, b.sb.at[pair, part(i), :, first(NB)], b.osem.at[pair])

    def stage(k):
        two[k].finish()
        for dz in RING:
            get(b.hnT.at[dz, :, :, pl.ds(k * TILE, TILE)], b.wt.at[1, :, :, pl.ds(dz * TILE, TILE)], b.wsem.at[1])

    def turn(k):
        drain(b.wt.at[1, :, :, first(ROWS)], b.wsem.at[1])
        for dz in RING:
            for h in range(NC):
                b.hn[dz, pl.ds(k * TILE + h * LANE, LANE), :] = b.wt[1, :, :, pl.ds(dz * TILE + h * LANE, LANE)].reshape(KB, LANE).T

    def query(k):
        at = pl.ds(k * TILE, TILE)
        new = sum(jnp.dot(b.hn[dz, at, :NB], b.sb[dz // 2, part(dz % 2), :, :NB].reshape(NB, NB), preferred_element_type=F32) for dz in RING)
        b.qout[pl.ds(k * NR, NR)] = new.astype(BF16).reshape(NR, MINE, NB)
        kv = jnp.concatenate([b.kvw[:, side].reshape(NB, HD) for side in range(NC)], axis=1)
        new = jnp.dot(b.hn[x, at, :NB], kv, preferred_element_type=F32)
        b.kvout[pl.ds(k * NR, NR)] = new.astype(BF16).reshape(NR, MINE, 2 * HD)

    def project(acc, i, slot, lo=0, hi=ROWS, fresh=False, wait=True):
        if wait:
            drain(b.wt.at[slot], b.wsem.at[slot])

        @pl.loop(lo // TILE, hi // TILE)
        def _(r):
            at = pl.ds(pl.multiple_of(r * TILE, TILE), TILE)
            new = jnp.dot(b.hn[ORDER[i], at, :], b.wt[slot].reshape(KB, KB), preferred_element_type=F32)
            acc[at, :] = new if fresh else new + acc[at, :]

    fetch = lambda f, i, slot: f.load(ORDER[i], b.wt.at[slot], b.wsem.at[slot])

    def roles(i):
        return (0, 3, 2, 1) if i == TURNED else tuple(RING)

    def fetch_d(i, *parts):
        for h in parts:
            for t in (2 * h, 2 * h + 1):
                g = roles(i)[t]
                fd.ready(ORDER[i], g)
                fd.bring(ORDER[i], g, 1, b.wt.at[i % 2, pl.ds(t, 1)], b.wsem.at[2 * h + i % 2])


    fg.z_send(2)
    fu.z_send(0)
    load_q(0)
    load_q(1)
    stage(0)
    two[2].forward()
    two[3].start()
    turn(0)
    for pair in range(NC):
        drain(b.sb.at[pair, :, :, first(NB)], b.osem.at[pair])
    for slot in range(NC):
        drain(kv_half(slot, 1 - c), b.kw_c.at[slot])
    query(0)
    two[1].forward()
    fu.y_send()
    fg.forward(1)
    stage(2)
    turn(2)
    query(2)
    fetch(fg, 0, 0)
    two[3].forward()
    stage(1)
    turn(1)
    query(1)
    fg.forward(2)
    fg.last(0)
    project(b.gacc, 0, 0, 0, 3 * TILE, fresh=True)
    fu.z_send(1)
    fu.forward(0)
    fetch(fg, 1, 0)
    project(b.gacc, 1, 0, 0, 3 * TILE)
    fu.z_send(2)
    stage(3)
    turn(3)
    fetch(fg, 0, 1)
    query(3)
    for dy in (0, 2):
        for dx in AWAY + (0,)[:dy]:
            yy, xx = flip(y, dy), flip(x, dx)
            put(b.kvout.at[yy * NR + xx], b.kv_in.at[2 * dy + x], b.kv_s, b.kv_r, dict(y=yy, x=xx))
    for dy, dx in PAIRS:
        yy, xx = flip(y, dy), flip(x, dx)
        put(b.qout.at[yy * NR + xx], b.q_in.at[me], b.q_s, b.q_r, dict(y=yy, x=xx))
    b.q_in[me] = b.qout[me]
    b.kv_in[x] = b.kvout[me]
    fo.start()
    fd.y_send((2, 1, 3))

    project(b.gacc, 1, 0, 3 * TILE, ROWS, fresh=True, wait=False)
    fetch(fg, 2, 0)
    project(b.gacc, 0, 1, 3 * TILE, ROWS)
    fg.last(1)
    fg.last(2)
    fetch(fg, 3, 1)
    project(b.gacc, 2, 0)
    fu.forward(1)
    fetch(fu, 0, 0)
    project(b.gacc, 3, 1)
    project(b.uacc, 0, 0, fresh=True)
    drain(b.kc, b.ld.at[1])
    drain(b.vc, b.ld.at[2])
    drain(b.q_in.at[first(NJ - 1)], b.q_r)
    drain(b.kv_in.at[first(NG - 1)], b.kv_r)

    @pl.loop(0, MINE)
    def _(r):
        b.lenb[pl.ds(r, 1), :] = jnp.broadcast_to(lens[r], (1, HD)).astype(F32)
    i_half = lax.rem(lax.broadcasted_iota(jnp.int32, (MINE, HD), 1), HALF).astype(F32)
    angle = b.lenb[...] * jnp.power(ROPE_BASE, i_half * (-2.0 / HD))
    low = lax.broadcasted_iota(jnp.int32, (MINE, HD), 1) < HALF
    cos = jnp.cos(angle)
    sin = jnp.where(low, -jnp.sin(angle), jnp.sin(angle))
    rope = lambda v: v * cos + pltpu.roll(v, HALF, 1) * sin
    kv = sum(b.kv_in[i].astype(F32) for i in range(NG)).astype(BF16).astype(F32)
    b.kn[:, :HD] = rope(kv[:, :HD])
    b.kn[:, HD:] = kv[:, HD:]
    for xs in RING:
        for yh in range(NC):
            q = (b.q_in[yh * 4 + xs].astype(F32) + b.q_in[(yh + 2) * 4 + xs].astype(F32)).astype(BF16).astype(F32)
            for h in range(5):
                b.q3[pl.ds(xs * 10 + yh * 5 + h, MINE, stride=HEADS), :] = rope(q[:, h * HD:(h + 1) * HD])
    t_row = lax.broadcasted_iota(jnp.int32, (SEQ, HD), 0)
    t_col = lax.broadcasted_iota(jnp.int32, (HEADS, SEQ), 1)

    def attend(rows):
        ats = [pl.ds(pl.multiple_of(r * HEADS, 8), HEADS) for r in rows]
        here = [t_row == lens[r] for r in rows]
        new = [b.kn[pl.ds(r, 1), :] for r in rows]
        keys = [jnp.where(h, n[:, :HD].astype(BF16).astype(F32), b.kc[r].astype(F32)).astype(BF16) for r, h, n in zip(rows, here, new)]
        vals = [jnp.where(h, n[:, HD:], b.vc[r].astype(F32)).astype(BF16) for r, h, n in zip(rows, here, new)]
        s = [lax.dot_general(b.q3[at, :].astype(BF16), k, NT, preferred_element_type=F32) for at, k in zip(ats, keys)]
        s = [jnp.where(t_col <= lens[r], v * (HD ** -0.5), -1e30) for r, v in zip(rows, s)]
        top = [jnp.max(v, axis=1, keepdims=True) for v in s]
        e = [jnp.exp(v - t) for v, t in zip(s, top)]
        total = [jnp.sum(v, axis=1, keepdims=True) for v in e]
        p = [(v / t).astype(BF16) for v, t in zip(e, total)]
        o = [jnp.dot(v, w, preferred_element_type=F32) for v, w in zip(p, vals)]
        for r, at, k, v, w in zip(rows, ats, keys, vals, o):
            b.kc[r], b.vc[r], b.q3[at, :] = k, v, w

    def attend_some(lo, hi):
        @pl.loop(lo // NG, hi // NG)
        def _(step):
            attend([step * NG + k for k in range(NG)])

    attend_some(0, MINE)
    get(b.kc, kc_o, b.out_l)
    get(b.vc, vc_o, b.out_l)
    for h in range(HEADS):
        b.o_v[:, h * HD:(h + 1) * HD] = b.q3[pl.ds(h, MINE, stride=HEADS), :].astype(BF16)
    block = lambda yy, xx: b.o_v.at[:, pl.ds(pl.multiple_of((xx * 2 + lax.rem(yy, 2)) * NB, LANE), NB)]
    for dy, dx in PAIRS:
        yy, xx = flip(y, dy), flip(x, dx)
        put(block(yy, xx), b.o_in.at[me], b.o_s, b.o_r, dict(y=yy, x=xx))
    b.o_in[me] = block(y, x)[...]

    def start_d(*plan):
        for g, planes in plan:
            fd.wait_y(g)
            for dz in planes:
                fd.z_put(g, dz)

    fu.forward(2)
    fo.z_second()
    fetch(fu, 1, 1)
    fetch(fu, 2, 0)
    project(b.uacc, 1, 1)
    project(b.uacc, 2, 0)
    start_d((2, SIDES))
    fu.last(0)
    fu.last(1)
    fu.last(2)
    fetch(fu, 3, 1)
    load_o = lambda i: fo.load(ORDER[i], b.wo_t.at[i % 2], b.osem.at[i % 2])
    start_d((1, SIDES[1:]), (3, SIDES[:1]), (0, SIDES))
    project(b.uacc, 3, 1)
    fetch_d(0, *BOTH)
    load_o(0)

    @pl.loop(0, ROWS // LANE)
    def _(r):
        at = pl.ds(pl.multiple_of(r * LANE, LANE), LANE)
        g = b.gacc[at, :].astype(BF16).astype(F32)
        b.act[at, :] = (g / (1.0 + jnp.exp(-g)) * b.uacc[at, :].astype(BF16).astype(F32)).astype(BF16)
    drain(b.o_in.at[first(NJ - N1)], b.o_r)
    HA, HBk = first(CUT), pl.ds(CUT, ROWS - CUT)

    rows_of = lambda h: pl.ds(h * HB // N2, HB // N2)

    def sent(i):
        for land, sem in ((b.a1, b.a1s), (b.b1, b.b1s), (b.ta, b.tas), (b.tb, b.tbs)):
            drain(land.at[i], sem.at[i])

    def multiply(i, h):
        slot, k, tall = i % N2, i % N3, part(h)
        drain(b.wt.at[slot, tall], b.wsem.at[N2 * h + slot])
        heads = [t for t in (N2 * h, N2 * h + N1) if roles(i)[t] < N2]
        if heads and i not in loaded_o:
            drain(b.wo_t.at[slot], b.osem.at[slot])
            loaded_o.add(i)

        def some(lo, hi):
            @pl.loop(lo // TILE, hi // TILE)
            def _(r):
                at = pl.ds(pl.multiple_of(r * TILE, TILE), TILE)
                out = lax.dot_general(b.wt[slot, tall].reshape(NB, KB), b.act[at, :], NT, preferred_element_type=F32)
                rows = b.o_in[pl.ds(r * NR, NR)].reshape(TILE, NB)
                if len(heads) == N2:
                    out += lax.dot_general(b.wo_t[slot].reshape(NB, NB), rows, NT, preferred_element_type=F32)
                elif heads:
                    more = lax.dot_general(b.wo_t[slot, roles(i)[heads[N0]]], rows, NT, preferred_element_type=F32)
                    halves = [out[:HB], out[HB:]]
                    halves[heads[N0] - N2 * h] += more
                    out = jnp.concatenate(halves, axis=N0)
                b.sb[k, tall, :, at] = out.astype(BF16).reshape(N2, HB, TILE)

        def first_rows():
            some(N0, CUT)
            if h == FAR:
                for j, d in enumerate(ends(i)):
                    put(b.sb.at[k, N2, rows_of(j), HA], b.ta.at[i, j], b.tas.at[i], b.tar.at[i, j], dict(y=flip(y, d)))
            put(b.sb.at[k, SIDES[h], rows_of(h), HA], b.a1.at[i, h, rows_of(h)], b.a1s.at[i], b.a1r.at[i, h], dict(y=flip(y, ends(i)[h])))
            if h == NEAR and i:
                pass_a(i, h)

        def last_rows():
            some(CUT, ROWS)
            d = ends(i)[h]
            put(b.sb.at[k, tall, mine(N2), HBk], b.tb.at[i, h], b.tbs.at[i], b.tbr.at[i, h], dict(x=flip(x, d)))
            put(b.sb.at[k, tall, mine(d), HBk], b.b1.at[i, h, tall], b.b1s.at[i], b.b1r.at[i, h], dict(x=flip(x, d)))

        for step in (first_rows, last_rows)[::N1 if h else -N1]:
            step()

    loaded_o = set()
    ends = lambda i: SIDES[::-N1] if i == TURNED else SIDES

    def pass_a(i, h):
        k, t, rows = i % N3, SIDES[h], rows_of(N1 - h)
        drain(b.ta.at[i, N1 - h], b.tar.at[i, N1 - h])
        b.sb[k, t, rows, HA] = (b.sb[k, t, rows, HA].astype(F32) + b.ta[i, N1 - h].astype(F32)).astype(BF16)
        put(b.sb.at[k, t, rows, HA], b.a1.at[i, h, rows], b.a1s.at[i], b.a1r.at[i, h], dict(y=flip(y, ends(i)[h])))

    def passed(i, h):
        k, tall = i % N3, part(h)
        if h == FAR or i == N0:
            pass_a(i, h)
        d = ends(i)[N1 - h]
        drain(b.tb.at[i, h], b.tbr.at[i, h])
        b.sb[k, tall, mine(d), HBk] = (b.sb[k, tall, mine(d), HBk].astype(F32) + b.tb[i, h].astype(F32)).astype(BF16)
        put(b.sb.at[k, tall, mine(d), HBk], b.b1.at[i, N1 - h, tall], b.b1s.at[i], b.b1r.at[i, h], dict(x=flip(x, d)))

    def load_a(i):
        for k in range(NC):
            drain(b.a1.at[i, k], b.a1r.at[i, k])
        get(b.a1.at[i], b.va.at[i % N2], b.vsem.at[i % N2])

    def second_a(i):
        dz, va = ORDER[i], b.va.at[i % N2]
        drain(va, b.vsem.at[i % N2])
        b.s2a[dz] = (b.sb[i % N3, N0, :, HA].astype(F32) + (va[N0].astype(F32) + va[N1].astype(F32))).astype(BF16)
        for d in AWAY:
            put(b.s2a.at[dz, mine(d)], b.a2.at[dz, d - N1], b.a2s.at[dz], b.a2r.at[dz], dict(x=flip(x, d)))

    def load_b(i, h):
        drain(b.b1.at[i, :, part(h)], b.b1r.at[i, h])
        get(b.b1.at[i, :, part(h)], b.vb.at[i % N2, :, part(h)], b.vsem.at[N2 + N2 * h + i % N2])

    def second_b(i, h):
        k, tall = i % N3, part(h)
        vb = b.vb.at[i % N2, :, tall]
        drain(vb, b.vsem.at[N2 + N2 * h + i % N2])
        b.s2b[i, tall] = (b.sb[k, tall, mine(N0), HBk].astype(F32) + (vb[N0].astype(F32) + vb[N1].astype(F32))).astype(BF16)
        for t in ((N1,), (N3, N2))[h]:
            put(b.s2b.at[i, t], b.b2.at[i, t - N1], b.b2s.at[i], b.b2r.at[i], dict(y=flip(y, roles(i)[t])))

    def third(i):
        dz = ORDER[i]
        drain(b.a2.at[dz], b.a2r.at[dz])
        drain(b.b2.at[i], b.b2r.at[i])
        for src, own, lanes, at in ((b.a2.at[dz], b.s2a[dz, mine(N0)], HA, LANE), (b.b2.at[i], b.s2b[i, N0], HBk, LANE + CUT)):
            total = own.astype(F32) + sum(src[d].astype(F32) for d in range(NR - N1))
            for cc in range(NC):
                b.fs[dz, cc, :, lanes] = (b.F[dz * NC + cc, :, pl.ds(at, CUT)].astype(F32) + total[cc * FEATS:(cc + N1) * FEATS]).astype(BF16)
        at = z * NC + c
        for cc in sides(dz):
            put(b.fs.at[dz, cc], fin.at[at], b.fin_s, b.fin_r.at[at], dict(z=flip(z, dz), c=cc))
        if dz == N0:
            get(b.fs.at[N0, c], fin.at[at], b.fin_l)

    multiply(N0, FAR)
    multiply(N0, NEAR)
    for dz, g in ((N1, N2), (N3, N2), (N1, N3), (N3, N1)):
        fd.arrive(dz, g)
    fd.pass_on(N2)
    fd.pass_on(N3, N1)
    fd.pass_on(N1, N3)
    fd.z_put(N1, N1)
    fd.z_put(N3, N3)
    fo.forward()
    fetch_d(N1, FAR)
    load_o(N2)
    fetch_d(N2, FAR)
    passed(N0, FAR)
    passed(N0, NEAR)
    multiply(N1, FAR)
    multiply(N2, FAR)
    load_b(N0, FAR)
    load_a(N0)
    load_b(N0, NEAR)
    second_b(N0, FAR)
    second_a(N0)
    second_b(N0, NEAR)
    passed(N1, FAR)
    passed(N2, FAR)
    load_o(N1)
    fd.last(N2)
    fd.last(N3)
    fd.last(N1)
    sent(N0)
    fetch_d(N3, FAR)
    multiply(N3, FAR)
    load_b(N1, FAR)
    load_b(N2, FAR)
    second_b(N1, FAR)
    second_b(N2, FAR)
    fd.arrive(N1, N0)
    fd.arrive(N3, N0)
    fd.pass_on(N0)
    fd.arrive(N1, N1)
    fd.arrive(N3, N3)
    fetch_d(N1, NEAR)
    fetch_d(N2, NEAR)
    multiply(N1, NEAR)
    multiply(N2, NEAR)
    passed(N3, FAR)
    fo.last()
    fd.last(N0)
    fetch_d(N3, NEAR)
    load_o(N3)
    multiply(N3, NEAR)
    passed(N1, NEAR)
    passed(N2, NEAR)
    load_b(N3, FAR)
    load_a(N1)
    load_a(N2)
    second_b(N3, FAR)
    second_a(N1)
    second_a(N2)
    passed(N3, NEAR)
    load_b(N1, NEAR)
    load_b(N2, NEAR)
    second_b(N1, NEAR)
    second_b(N2, NEAR)
    third(N0)
    load_a(N3)
    load_b(N3, NEAR)
    second_a(N3)
    second_b(N3, NEAR)
    third(N1)
    third(N2)
    third(N3)

    for dz in AWAY + (0,):
        for cc in sides(dz):
            at = flip(z, dz) * NC + cc
            drain(fin.at[at], b.fin_r.at[at])
    drain(fin.at[0], b.fin_l)

    some, tile = first(NR - 1), first(TILE)
    for k in RING:
        drain(b.hnT.at[some, 0, :, tile], b.ag_s.at[NC * k])
        drain(b.hnT.at[some, :, :, tile], b.ag_s.at[NC * k + 1])
    for h in range(NC):
        drain(b.S.at[h, first(NJ - 1)], b.s_s.at[h])
    drain(b.F.at[first(NG - 1)], b.f_s)
    drain(b.q_in.at[first(NJ - 1)], b.q_s)
    drain(b.kv_in.at[first(NG - 1)], b.kv_s)
    drain(b.kvw.at[0], b.kw_s)
    drain(kv_half(1, c), b.kw_s)

    @pl.when(x > 0)
    def _():
        drain(kv_half(0, c), b.kw_s)
    drain(b.o_in.at[first(NJ - 1)], b.o_s)
    for dz in ORDER:
        if dz:
            sent(dz)
        drain(b.a2.at[dz], b.a2s.at[dz])
        drain(b.b2.at[dz], b.b2s.at[dz])
    drain(fin.at[first(NG - 1)], b.fin_s)
    for f in (fq, fg, fu, fd, fo):
        f.finish()
    for ref in (b.kc, b.vc):
        drain(ref, b.out_l)


def finish(fin, kc_h, vc_h, out, kc_o, vc_o, fin_v, kc, vc, ov, sem):
    get(fin, fin_v, sem.at[0])
    get(kc_h, kc, sem.at[1])
    get(vc_h, vc, sem.at[2])
    drain(fin_v, sem.at[0])
    row_low = lax.broadcasted_iota(jnp.int32, (FEATS, LANE), 1) < HALF
    for zz in RING:
        for p in range(NG):
            lo, hi = (fin_v[zz * NC + cc, :, pl.ds(p * LANE, LANE)].astype(F32) for cc in range(NC))
            pair = [jnp.where(row_low, lo, pltpu.roll(hi, HALF, 1)), jnp.where(row_low, pltpu.roll(lo, HALF, 1), hi)]
            ov[:, pl.ds(zz * NC * ROWS + p * TILE, TILE)] = jnp.concatenate(pair, axis=1).astype(BF16)
    drain(kc, sem.at[1])
    get(kc, kc_o, sem.at[1])
    drain(vc, sem.at[2])
    get(vc, vc_o, sem.at[2])
    get(ov, out, sem.at[0])
    for i, ref in enumerate((ov, kc, vc)):
        drain(ref, sem.at[i])


def solution(mesh):
    inner = Mesh(mesh.devices.reshape(4, 4, 4, 2), tuple('zyxc'))

    def layer(residual, ln_scale, w_query, w_key, w_value, w_gate, w_up, w_out, w_down, k_cache, v_cache, lengths):
        hbm = pl.BlockSpec(memory_space=pltpu.HBM)
        vmem = pl.BlockSpec(memory_space=pltpu.VMEM)
        smem = pl.BlockSpec(memory_space=pltpu.SMEM)
        shape = lambda a: jax.ShapeDtypeStruct(*a)
        results = [((FEATS, BATCH), BF16), (k_cache.shape, BF16), (v_cache.shape, BF16)]
        fin = ((NG, FEATS, ROWS), BF16)
        outs = [fin] + results[1:] + list(HBM_BUFS.values())
        got = pl.pallas_call(
            kernel,
            out_shape=[shape(a) for a in outs],
            in_specs=[hbm, vmem, smem] + [hbm] * 9,
            out_specs=[hbm] * len(outs),
            scratch_shapes=[pltpu.VMEM(*a) for a in VMEM_BUFS.values()] + [DMA(s) if s else DMA for s in SEMS.values()] + NARROW_SEMS + WIDE_SEMS * 2 + SINGLE_SEMS + NARROW_SEMS,
            name='decode_layer',
            compiler_params=pltpu.CompilerParams(collective_id=0, has_side_effects=True, vmem_limit_bytes=67043328),
        )(residual.T, ln_scale.reshape(1, FEATS), lengths, w_query, w_key, w_value, w_gate, w_up, w_down.T, w_out.T, k_cache, v_cache)
        out, k_new, v_new = pl.pallas_call(
            finish,
            out_shape=[shape(a) for a in results],
            in_specs=[hbm] * 3,
            out_specs=[hbm] * 3,
            scratch_shapes=[pltpu.VMEM(*a) for a in [fin] + results[1:] + results[:1]] + [DMA((3,))],
            name='finish',
        )(*got[:3])
        return out.T, k_new, v_new

    rc, tx, tyz = tuple('zyxc'), tuple('zy'), tuple('xc')
    cache = P(rc, None, None)
    in_specs = (P(None, rc), P(rc), P(tx, tyz), P(tx, None), P(tx, None), P(tx, tyz), P(tx, tyz), P(tyz, tx), P(tyz, tx), cache, cache, P(rc))
    return jax.shard_map(layer, mesh=inner, in_specs=in_specs, out_specs=(P(None, rc), cache, cache), check_vma=False)
```

```python
import jax
import jax.numpy as jnp
from jax import lax
from jax.experimental import pallas as pl
from jax.experimental.pallas import tpu as pltpu
from jax.sharding import Mesh, PartitionSpec as P

LN_EPS = 1e-5
ROPE_BASE = 10000.0
MESH = pl.DeviceIdType.MESH
DMA = pltpu.SemaphoreType.DMA
F32, BF16 = jnp.float32, jnp.bfloat16
ROWS, MODEL, FEATS, BATCH = 1024, 5120, 40, 8192
KB, NB, HB, HD, SUB = 1280, 640, 320, 128, 80
MINE, SEQ, HEADS, LANE, HALF = 64, 64, 40, 128, 64
NR, NC, NJ, NG = 4, 2, 16, 8
X_FIRST = (1,)
CUT = 512
TILE = 256
RING = range(4)
N0, N1, N2, N3 = RING
AWAY = (1, 3, 2)
SIDES = AWAY[:2]
FORTH, BACK = ((1, 0), (3, 1)), ((3, 0), (1, 1))
GROUPS = ((0, 1), (1, 2), (2, 4))
SINGLE = ((0, 1), (1, 2), (2, 3), (3, 4))
ORDER = (0, 1, 3, 2)
BOTH = NEAR, FAR = (0, 1)
TURNED = 2
PAIRS = tuple(sorted(((dy, dx) for dy in RING for dx in RING if dy or dx), key=lambda p: (p.count(2), 0 not in p, abs(p[0] - p[1]))))
NT = (((1,), (1,)), ((), ()))


def flip(i, d):
    return (i, i + 1 - 2 * lax.rem(i, 2), lax.rem(i + 2, 4), 3 - i)[d]


def put(src, dst, ssem, rsem, dev):
    pltpu.make_async_remote_copy(src_ref=src, dst_ref=dst, send_sem=ssem, recv_sem=rsem, device_id=dev, device_id_type=MESH).start()


def added(ref):
    return sum(ref[k].astype(F32) for k in range(NR - 1))


def get(src, dst, sem):
    pltpu.make_async_copy(src, dst, sem).start()


def first(n):
    return pl.ds(0, n)


def drain(ref, sem):
    pltpu.make_async_copy(ref, ref, sem).wait()


class Wide:
    def __init__(self, land, src, sems, pos, groups=GROUPS):
        self.land, self.src = land, src
        self.send, self.yr, self.zr, self.fr, self.dr, self.loc = sems
        self.z, self.y, self.x, self.c = pos
        self.base = self.c * 16
        self.groups = groups
        self.here = set()

    def piece(self, yy):
        return self.src.at[:, pl.ds(pl.multiple_of(yy * NB, LANE), NB)]

    def at(self, dz, g, base=None):
        lo, hi = self.groups[g]
        return self.land.at[pl.ds((self.base if base is None else base) + dz * 4 + lo, hi - lo)]

    def start_local(self):
        get(self.piece(self.y), self.land.at[self.base], self.loc)

    def y_send(self, order=AWAY):
        for dy in order:
            yy = flip(self.y, dy)
            put(self.piece(yy), self.land.at[self.base + dy], self.send, self.yr.at[dy - 1], dict(y=yy))

    def z_send(self, g):
        self.wait_y(g)
        for dz in SIDES:
            self.z_put(g, dz)

    def wait_y(self, g):
        if g:
            for dy in range(*self.groups[g]):
                drain(self.land.at[self.base + dy], self.yr.at[dy - 1])
        self.d2d(0, g)

    def z_put(self, g, dz):
        src = self.at(0, g) if g else self.piece(self.y)
        dst = self.at(dz, g) if g else self.land.at[self.base + dz * 4]
        put(src, dst, self.send, self.zr.at[dz // 2 * len(self.groups) + g], dict(z=flip(self.z, dz)))

    def arrive(self, dz, g):
        drain(self.at(dz, g), self.zr.at[dz // 2 * len(self.groups) + g])
        self.d2d(dz, g)

    def forward(self, g):
        for dz in SIDES:
            self.arrive(dz, g)
        self.pass_on(g)

    def pass_on(self, g, *sides):
        for k, dz in enumerate(SIDES):
            src, dst = (self.at(dz, g), self.at(2, g)) if sides else (self.half(dz, g, k), self.half(2, g, k))
            if dz in (sides or SIDES):
                put(src, dst, self.send, self.fr.at[g], dict(z=flip(self.z, 4 - dz)))

    def half(self, dz, g, k):
        lo, hi = self.groups[g]
        return self.land.at[pl.ds(self.base + dz * 4 + lo, hi - lo), pl.ds(k * HB // 2, HB // 2)]

    def last(self, g):
        drain(self.at(2, g), self.fr.at[g])
        self.d2d(2, g)

    def d2d(self, dz, g):
        to = dict(c=1 - self.c)
        if dz or g:
            put(self.at(dz, g), self.at(dz, g), self.send, self.dr.at[dz * len(self.groups) + g], to)
        else:
            put(self.piece(self.y), self.land.at[self.base], self.send, self.dr.at[0], to)

    def ready(self, dz, g):
        if (dz, g) not in self.here:
            if dz == g == 0:
                drain(self.land.at[self.base], self.loc)
            drain(self.at(dz, g, 16 - self.base), self.dr.at[dz * len(self.groups) + g])
        self.here.add((dz, g))

    def load(self, dz, tile, sem):
        for g in range(len(self.groups)):
            self.ready(dz, g)
        self.bring(dz, 0, NR, tile, sem)

    def bring(self, dz, lo, n, tile, sem):
        for cc in range(NC):
            get(self.land.at[pl.ds(cc * 16 + dz * NR + lo, n)], tile.at[:, :, pl.ds(cc * NB, NB)], sem)

    def finish(self):
        drain(self.land.at[first(31)], self.send)


class Narrow:
    def __init__(self, land, parts, sems, pos):
        self.land, self.parts = land, parts
        self.send, self.yr, self.zr, self.fr, self.dr, self.loc = sems
        self.z, self.y, self.x, self.c = pos
        self.s = lax.rem(self.c + self.y, 2)

    def own(self, slot):
        lo = 0
        for ref in self.parts:
            hi = lo + ref.shape[1]
            yield ref, self.land.at[slot, :, pl.ds(lo, hi - lo)]
            lo = hi

    def start(self):
        @pl.when(self.s == 0)
        def _():
            for src, dst in self.own(0):
                get(src, dst, self.loc)

        @pl.when(self.s == 1)
        def _():
            for src, dst in self.own(1):
                put(src, dst, self.send, self.yr, dict(y=flip(self.y, 1), c=1 - self.c))

    def z_first(self):
        @pl.when(self.s == 0)
        def _():
            for k, dz in enumerate(SIDES):
                for (src, _), (_, dst) in zip(self.own(0), self.own(dz * 2)):
                    put(src, dst, self.send, self.zr.at[k], dict(z=flip(self.z, dz)))
            for src, dst in self.own(0):
                put(src, dst, self.send, self.dr.at[0], dict(c=1 - self.c))

    def z_second(self):
        @pl.when(self.s == 1)
        def _():
            src = self.land.at[1]
            drain(src, self.yr)
            for k, dz in enumerate(SIDES):
                put(src, self.land.at[dz * 2 + 1], self.send, self.zr.at[k], dict(z=flip(self.z, dz)))
            put(src, src, self.send, self.dr.at[0], dict(c=1 - self.c))

    def half(self, slot, k):
        return self.land.at[slot, pl.ds(k * HB // 2, HB // 2)]

    def forward(self):
        for k, dz in enumerate(SIDES):
            slot = dz * 2 + self.s
            piece = self.land.at[slot]
            drain(piece, self.zr.at[k])
            put(self.half(slot, k), self.half(4 + self.s, k), self.send, self.fr.at[k], dict(z=flip(self.z, AWAY[1 - k])))
            put(piece, piece, self.send, self.dr.at[1 + k], dict(c=1 - self.c))

    def last(self):
        for k in range(NC):
            piece = self.half(4 + self.s, k)
            drain(piece, self.fr.at[k])
            put(piece, piece, self.send, self.dr.at[3 + k], dict(c=1 - self.c))

    def load(self, dz, tile, sem):
        o = 1 - self.s
        if dz == 0:
            @pl.when(self.s == 0)
            def _():
                drain(self.land.at[0], self.loc)
        if dz == 2:
            for k in range(NC):
                drain(self.half(4 + o, k), self.dr.at[3 + k])
        else:
            drain(self.land.at[dz * 2 + o], self.dr.at[(dz + 1) // 2])
        get(self.land.at[pl.ds(dz * 2, 2)], tile, sem)

    def finish(self):
        for s in range(NC):
            @pl.when(self.s == s)
            def _():
                drain(self.land.at[first(7 + s)], self.send)


class Ring:
    def __init__(self, axis, at, own, land, moved, sems):
        self.axis, self.at, self.own, self.land, self.moved = axis, at, own, land, moved
        self.send, self.recv = sems

    def to(self, d):
        return {self.axis: flip(self.at, d)}

    def start(self):
        for k in range(NC):
            for d, h in ((1, k), (3, 1 - k)):
                put(self.own(h), self.land(d, h), self.send, self.recv.at[d - 1 + h], self.to(d))

    def forward(self):
        for d, h in FORTH:
            drain(self.moved(d, h), self.recv.at[d - 1 + h])
            put(self.moved(d, h), self.moved(2, h) if self.axis == 'y' else self.moved(d, h), self.send, self.recv.at[4 + h], self.to(4 - d))

    def finish(self):
        for d, h in BACK:
            drain(self.moved(d, h), self.recv.at[d - 1 + h])
        for h in range(NC):
            drain(self.moved(2, h), self.recv.at[4 + h])


WIDE_SEMS, SINGLE_SEMS = ([DMA, DMA((NR - 1,)), DMA((2 * n,)), DMA((n,)), DMA((NR * n,)), DMA] for n in map(len, (GROUPS, SINGLE)))
NARROW_SEMS = [DMA, DMA, DMA((2,)), DMA((2,)), DMA((5,)), DMA]
HBM_BUFS = dict(
    Q=((NG, HB, NB), BF16), G=((NG * NR, HB, NB), BF16), U=((NG * NR, HB, NB), BF16), D=((NG * NR, HB, NB), BF16), O=((NG, HB, NB), BF16),
    hnT=((NR, NR, HB, ROWS), BF16), a1=((NR, NC, HB, CUT), BF16), b1=((NR, NC, NR, SUB, ROWS - CUT), BF16))
VMEM_BUFS = dict(
    rT=((FEATS, BATCH), BF16), xs=((NG, FEATS, ROWS + LANE), BF16), F=((NG, FEATS, ROWS + LANE), BF16), S=((NC, NJ, 2, CUT), F32),
    hs=((NR, SUB, ROWS), BF16), hn=((NR, ROWS, KB), BF16), wt=((NC, NR, HB, KB), BF16), wo_t=((NC, NC, HB, NB), BF16),
    gacc=((ROWS, KB), F32), uacc=((ROWS, KB), F32), qout=((NJ, MINE, NB), BF16), kvout=((NJ, MINE, 2 * HD), BF16), kvw=((NC, NC, HB, HD), BF16), q_in=((NJ, MINE, NB), BF16), kv_in=((NG, MINE, 2 * HD), BF16),
    q3=((MINE * HEADS, HD), F32), lenb=((MINE, HD), F32), kc=((MINE, SEQ, HD), BF16), vc=((MINE, SEQ, HD), BF16), kn=((MINE, 2 * HD), F32),
    o_v=((MINE, MODEL), BF16), o_in=((NJ, MINE, NB), BF16), act=((ROWS, KB), BF16), sb=((NR - 1, NR, HB, ROWS), BF16),
    va=((NC, NC, HB, CUT), BF16), vb=((NC, NC, NR, SUB, ROWS - CUT), BF16),
    ta=((NR, NC, HB // 2, CUT), BF16), tb=((NR, NC, NR // 2, SUB, ROWS - CUT), BF16), s2a=((NR, HB, CUT), BF16), s2b=((NR, NR, SUB, ROWS - CUT), BF16),
    a2=((NR, NR - 1, SUB, CUT), BF16), b2=((NR, NR - 1, SUB, ROWS - CUT), BF16), fs=((NR, NC, FEATS, ROWS), BF16))
ONE, EACH, BY_GROUP = (), (NR,), (NG,)
SEMS = dict(f_s=ONE, fin_l=ONE, s_s=EACH, s_r=EACH, own_l=EACH, q_s=ONE, kw_s=ONE, kw_z=ONE, kw_y=ONE, kw_c=EACH, q_r=ONE, kv_s=ONE, kv_r=ONE, o_s=ONE, o_r=ONE, fin_s=ONE, out_l=ONE,
            a1s=EACH, b1s=EACH, a2s=EACH, a2r=EACH, b2s=EACH, b2r=EACH, ag_s=BY_GROUP, ag_r=(NG, NG), tas=EACH, tbs=EACH, tar=(NR, NC), tbr=(NR, NC), b1r=(NR, NC), a1r=(NR, NC), ld=EACH, wsem=EACH, osem=EACH, vsem=BY_GROUP,
            f_r=(NC, NG), fin_r=BY_GROUP)


def kernel(res, ls, lens, wq, wk, wv, wg, wu, wdT, woT, kc_h, vc_h, fin, kc_o, vc_o, *rest):
    rest = list(rest)

    class b:
        pass
    for name in list(HBM_BUFS) + list(VMEM_BUFS) + list(SEMS):
        setattr(b, name, rest.pop(0))
    pos = z, y, x, c = tuple(lax.axis_index(a) for a in 'zyxc')
    flow = lambda kind, land, src, *more: kind(land, src, [rest.pop(0) for _ in WIDE_SEMS], pos, *more)
    fq = flow(Narrow, b.Q, (wq,))
    fg, fu, fd = flow(Wide, b.G, wg), flow(Wide, b.U, wu), flow(Wide, b.D, wdT, SINGLE)
    fo = flow(Narrow, b.O, (woT,))
    me = y * 4 + x
    row_low = lax.broadcasted_iota(jnp.int32, (FEATS, LANE), 1) < HALF
    sides = lambda dz: (c, 1 - c)[not dz:]

    bar = pltpu.get_barrier_semaphore()
    peers = [dict(z=flip(z, dz), c=cc) for dz in AWAY for cc in (c, 1 - c)] + [dict(c=1 - c), dict(y=flip(y, 1), c=1 - c)]
    peers += [dict(y=flip(y, dy), x=flip(x, dx)) for dy, dx in PAIRS]
    for p in peers:
        pl.semaphore_signal(bar, inc=1, device_id=p, device_id_type=MESH)
    get(res, b.rT, b.ld.at[0])
    get(kc_h, b.kc, b.ld.at[1])
    get(vc_h, b.vc, b.ld.at[2])
    for f in (fg, fu, fd):
        f.start_local()
    pl.semaphore_wait(bar, len(peers))
    fq.start()

    drain(b.rT, b.ld.at[0])
    scale = jnp.broadcast_to(ls[...].astype(F32), (LANE, FEATS)).T.astype(BF16)
    wide = lambda h: pl.ds(LANE * h + CUT * h, CUT + LANE * (1 - h))
    for i in range(NG):
        b.xs[i, :, :LANE] = scale
    for h in range(NC):
        for dz in AWAY + (0,):
            zz = flip(z, dz)
            for p in range(NR * h, NR * h + NR):
                pair = b.rT[:, pl.ds(pl.multiple_of(zz * NC * ROWS + p * TILE, LANE), TILE)].astype(F32)
                t0, t1 = pair[:, :LANE], pair[:, LANE:]
                at = pl.ds(LANE + p * LANE, LANE)
                b.xs[dz * NC, :, at] = jnp.where(row_low, t0, pltpu.roll(t1, HALF, 1)).astype(BF16)
                b.xs[dz * NC + 1, :, at] = jnp.where(row_low, pltpu.roll(t0, HALF, 1), t1).astype(BF16)
            for cc in sides(dz):
                put(b.xs.at[dz * NC + cc, :, wide(h)], b.F.at[dz * NC + c, :, wide(h)], b.f_s, b.f_r.at[h, dz * NC + c], dict(z=flip(z, dz), c=cc))
    b.F[c] = b.xs[c]
    def kv_half(slot, side):
        return b.kvw.at[slot, side]

    for side, w in enumerate((wk, wv)):
        @pl.when((c == side) & (x == 0))
        def _():
            get(w, kv_half(0, side), b.kw_z)

        @pl.when((c == side) & (x > 0))
        def _():
            zx = lax.rem(z // 2 + x // 2, 2) * 2 + lax.rem(z + x, 2)
            put(w, kv_half(0, side), b.kw_s, b.kw_z, dict(z=zx))
    fq.z_first()
    fg.z_send(0)

    for h in range(NC):
        for dz in RING:
            for cc in sides(dz):
                drain(b.F.at[dz * NC + cc, :, wide(h)], b.f_r.at[h, dz * NC + cc])
        tot = sq = jnp.zeros((FEATS, CUT), F32)
        for i in range(NG):
            v = b.F[i, :, pl.ds(LANE + CUT * h, CUT)].astype(F32)
            tot, sq = tot + v, sq + v * v
        b.S[h, me] = jnp.concatenate([jnp.sum(v, axis=0, keepdims=True) for v in (tot, sq)], axis=0)
        for dy, dx in PAIRS:
            put(b.S.at[h, me], b.S.at[h, me], b.s_s.at[h], b.s_r.at[h], dict(y=flip(y, dy), x=flip(x, dx)))
    fq.z_second()
    fo.z_first()

    mine = lambda d: pl.ds(pl.multiple_of(flip(x, d) * SUB, 16), SUB)

    def normalize(h):
        drain(b.S.at[h, first(NJ - 1)], b.s_r.at[h])
        stats = sum(b.S[h, i] for i in range(NJ)) / MODEL
        mean = stats[0:1]
        inv = lax.rsqrt(stats[1:] - mean * mean + LN_EPS)
        lanes = pl.ds(CUT * h, CUT)
        for dz in RING:
            both = []
            for i in (dz * NC, dz * NC + 1):
                both.append((b.F[i, :, pl.ds(LANE + CUT * h, CUT)].astype(F32) - mean) * inv * b.F[i, :, :LANE].astype(F32)[:, :1])
            b.hs[dz, :, lanes] = jnp.concatenate(both, axis=0).astype(BF16)
        get(b.hs.at[:, :, lanes], b.hnT.at[:, 0, mine(0), lanes], b.own_l.at[h])

    part = lambda h: pl.ds(2 * h, 2)

    def rings(k):
        lanes = pl.ds(k * TILE, TILE)
        far = lambda d, h: b.hnT.at[part(h), :, mine(d), lanes]
        near = lambda d, h: b.hnT.at[part(h), d, mine(0), lanes]
        own = lambda h: b.hs.at[part(h), :, lanes]
        sems = [(b.ag_s.at[NC * k + j], b.ag_r.at[NC * k + j]) for j in range(NC)]
        if k in X_FIRST:
            spot = lambda d, h: b.hnT.at[part(h), 0, mine(d), lanes]
            row = lambda d, h: b.hnT.at[part(h), d, :, lanes]
            return Ring('x', x, own, lambda d, h: spot(0, h), spot, sems[0]), Ring('y', y, lambda h: row(0, h), row, row, sems[1])
        return Ring('y', y, own, near, near, sems[0]), Ring('x', x, lambda h: far(0, h), lambda d, h: far(0, h), far, sems[1])

    one, two = zip(*(rings(k) for k in RING))
    normalize(0)
    one[0].start()
    one[1].start()
    one[0].forward()
    one[1].forward()
    normalize(1)
    one[2].start()
    one[3].start()
    for h in range(NC):
        drain(b.hs.at[:, :, pl.ds(CUT * h, CUT)], b.own_l.at[h])
    one[0].finish()
    two[0].start()
    one[2].forward()
    one[3].forward()
    drain(kv_half(0, c), b.kw_z)
    put(kv_half(0, c), kv_half(1, c), b.kw_s, b.kw_y, dict(y=flip(y, 1)))
    put(kv_half(0, c), kv_half(0, c), b.kw_s, b.kw_c.at[0], dict(c=1 - c))
    fg.y_send()
    one[1].finish()
    two[1].start()
    two[0].forward()
    fq.forward()
    fg.forward(0)
    one[2].finish()
    two[2].start()
    one[3].finish()
    fg.z_send(1)
    fq.last()
    drain(kv_half(1, c), b.kw_y)
    put(kv_half(1, c), kv_half(1, c), b.kw_s, b.kw_c.at[1], dict(c=1 - c))

    def load_q(pair):
        for i in range(NC):
            fq.load(NC * pair + i, b.sb.at[pair, part(i), :, first(NB)], b.osem.at[pair])

    def stage(k):
        two[k].finish()
        for dz in RING:
            get(b.hnT.at[dz, :, :, pl.ds(k * TILE, TILE)], b.wt.at[1, :, :, pl.ds(dz * TILE, TILE)], b.wsem.at[1])

    def turn(k):
        drain(b.wt.at[1, :, :, first(ROWS)], b.wsem.at[1])
        for dz in RING:
            for h in range(NC):
                b.hn[dz, pl.ds(k * TILE + h * LANE, LANE), :] = b.wt[1, :, :, pl.ds(dz * TILE + h * LANE, LANE)].reshape(KB, LANE).T

    def query(k):
        at = pl.ds(k * TILE, TILE)
        new = sum(jnp.dot(b.hn[dz, at, :NB], b.sb[dz // 2, part(dz % 2), :, :NB].reshape(NB, NB), preferred_element_type=F32) for dz in RING)
        b.qout[pl.ds(k * NR, NR)] = new.astype(BF16).reshape(NR, MINE, NB)
        kv = jnp.concatenate([b.kvw[:, side].reshape(NB, HD) for side in range(NC)], axis=1)
        new = jnp.dot(b.hn[x, at, :NB], kv, preferred_element_type=F32)
        b.kvout[pl.ds(k * NR, NR)] = new.astype(BF16).reshape(NR, MINE, 2 * HD)

    def project(acc, i, slot, lo=0, hi=ROWS, fresh=False, wait=True):
        if wait:
            drain(b.wt.at[slot], b.wsem.at[slot])

        @pl.loop(lo // TILE, hi // TILE)
        def _(r):
            at = pl.ds(pl.multiple_of(r * TILE, TILE), TILE)
            new = jnp.dot(b.hn[ORDER[i], at, :], b.wt[slot].reshape(KB, KB), preferred_element_type=F32)
            acc[at, :] = new if fresh else new + acc[at, :]

    fetch = lambda f, i, slot: f.load(ORDER[i], b.wt.at[slot], b.wsem.at[slot])

    def roles(i):
        return (0, 3, 2, 1) if i == TURNED else tuple(RING)

    def fetch_d(i, *parts):
        for h in parts:
            for t in (2 * h, 2 * h + 1):
                g = roles(i)[t]
                fd.ready(ORDER[i], g)
                fd.bring(ORDER[i], g, 1, b.wt.at[i % 2, pl.ds(t, 1)], b.wsem.at[2 * h + i % 2])


    fg.z_send(2)
    fu.z_send(0)
    load_q(0)
    load_q(1)
    stage(0)
    two[2].forward()
    two[3].start()
    turn(0)
    for pair in range(NC):
        drain(b.sb.at[pair, :, :, first(NB)], b.osem.at[pair])
    for slot in range(NC):
        drain(kv_half(slot, 1 - c), b.kw_c.at[slot])
    query(0)
    two[1].forward()
    fu.y_send()
    fg.forward(1)
    stage(2)
    turn(2)
    query(2)
    fetch(fg, 0, 0)
    two[3].forward()
    stage(1)
    turn(1)
    query(1)
    fg.forward(2)
    fg.last(0)
    project(b.gacc, 0, 0, 0, 3 * TILE, fresh=True)
    fu.z_send(1)
    fu.forward(0)
    fetch(fg, 1, 0)
    project(b.gacc, 1, 0, 0, 3 * TILE)
    fu.z_send(2)
    stage(3)
    turn(3)
    fetch(fg, 0, 1)
    query(3)
    for dy in (0, 2):
        for dx in AWAY + (0,)[:dy]:
            yy, xx = flip(y, dy), flip(x, dx)
            put(b.kvout.at[yy * NR + xx], b.kv_in.at[2 * dy + x], b.kv_s, b.kv_r, dict(y=yy, x=xx))
    for dy, dx in PAIRS:
        yy, xx = flip(y, dy), flip(x, dx)
        put(b.qout.at[yy * NR + xx], b.q_in.at[me], b.q_s, b.q_r, dict(y=yy, x=xx))
    b.q_in[me] = b.qout[me]
    b.kv_in[x] = b.kvout[me]
    fo.start()
    fd.y_send((2, 1, 3))

    project(b.gacc, 1, 0, 3 * TILE, ROWS, fresh=True, wait=False)
    fetch(fg, 2, 0)
    project(b.gacc, 0, 1, 3 * TILE, ROWS)
    fg.last(1)
    fg.last(2)
    fetch(fg, 3, 1)
    project(b.gacc, 2, 0)
    fu.forward(1)
    fetch(fu, 0, 0)
    project(b.gacc, 3, 1)
    project(b.uacc, 0, 0, fresh=True)
    drain(b.kc, b.ld.at[1])
    drain(b.vc, b.ld.at[2])
    drain(b.q_in.at[first(NJ - 1)], b.q_r)
    drain(b.kv_in.at[first(NG - 1)], b.kv_r)

    @pl.loop(0, MINE)
    def _(r):
        b.lenb[pl.ds(r, 1), :] = jnp.broadcast_to(lens[r], (1, HD)).astype(F32)
    i_half = lax.rem(lax.broadcasted_iota(jnp.int32, (MINE, HD), 1), HALF).astype(F32)
    angle = b.lenb[...] * jnp.power(ROPE_BASE, i_half * (-2.0 / HD))
    low = lax.broadcasted_iota(jnp.int32, (MINE, HD), 1) < HALF
    cos = jnp.cos(angle)
    sin = jnp.where(low, -jnp.sin(angle), jnp.sin(angle))
    rope = lambda v: v * cos + pltpu.roll(v, HALF, 1) * sin
    kv = sum(b.kv_in[i].astype(F32) for i in range(NG)).astype(BF16).astype(F32)
    b.kn[:, :HD] = rope(kv[:, :HD])
    b.kn[:, HD:] = kv[:, HD:]
    for xs in RING:
        for yh in range(NC):
            q = (b.q_in[yh * 4 + xs].astype(F32) + b.q_in[(yh + 2) * 4 + xs].astype(F32)).astype(BF16).astype(F32)
            for h in range(5):
                b.q3[pl.ds(xs * 10 + yh * 5 + h, MINE, stride=HEADS), :] = rope(q[:, h * HD:(h + 1) * HD])
    t_row = lax.broadcasted_iota(jnp.int32, (SEQ, HD), 0)
    t_col = lax.broadcasted_iota(jnp.int32, (HEADS, SEQ), 1)

    def attend(rows):
        ats = [pl.ds(pl.multiple_of(r * HEADS, 8), HEADS) for r in rows]
        here = [t_row == lens[r] for r in rows]
        new = [b.kn[pl.ds(r, 1), :] for r in rows]
        keys = [jnp.where(h, n[:, :HD].astype(BF16).astype(F32), b.kc[r].astype(F32)).astype(BF16) for r, h, n in zip(rows, here, new)]
        vals = [jnp.where(h, n[:, HD:], b.vc[r].astype(F32)).astype(BF16) for r, h, n in zip(rows, here, new)]
        s = [lax.dot_general(b.q3[at, :].astype(BF16), k, NT, preferred_element_type=F32) for at, k in zip(ats, keys)]
        s = [jnp.where(t_col <= lens[r], v * (HD ** -0.5), -1e30) for r, v in zip(rows, s)]
        top = [jnp.max(v, axis=1, keepdims=True) for v in s]
        e = [jnp.exp(v - t) for v, t in zip(s, top)]
        total = [jnp.sum(v, axis=1, keepdims=True) for v in e]
        p = [(v / t).astype(BF16) for v, t in zip(e, total)]
        o = [jnp.dot(v, w, preferred_element_type=F32) for v, w in zip(p, vals)]
        for r, at, k, v, w in zip(rows, ats, keys, vals, o):
            b.kc[r], b.vc[r], b.q3[at, :] = k, v, w

    def attend_some(lo, hi):
        @pl.loop(lo // NG, hi // NG)
        def _(step):
            attend([step * NG + k for k in range(NG)])

    attend_some(0, MINE)
    get(b.kc, kc_o, b.out_l)
    get(b.vc, vc_o, b.out_l)
    for h in range(HEADS):
        b.o_v[:, h * HD:(h + 1) * HD] = b.q3[pl.ds(h, MINE, stride=HEADS), :].astype(BF16)
    block = lambda yy, xx: b.o_v.at[:, pl.ds(pl.multiple_of((xx * 2 + lax.rem(yy, 2)) * NB, LANE), NB)]
    for dy, dx in PAIRS:
        yy, xx = flip(y, dy), flip(x, dx)
        put(block(yy, xx), b.o_in.at[me], b.o_s, b.o_r, dict(y=yy, x=xx))
    b.o_in[me] = block(y, x)[...]

    def start_d(*plan):
        for g, planes in plan:
            fd.wait_y(g)
            for dz in planes:
                fd.z_put(g, dz)

    fu.forward(2)
    fo.z_second()
    fetch(fu, 1, 1)
    fetch(fu, 2, 0)
    project(b.uacc, 1, 1)
    project(b.uacc, 2, 0)
    start_d((2, SIDES))
    fu.last(0)
    fu.last(1)
    fu.last(2)
    fetch(fu, 3, 1)
    load_o = lambda i: fo.load(ORDER[i], b.wo_t.at[i % 2], b.osem.at[i % 2])
    project(b.uacc, 3, 1)
    start_d((1, SIDES[1:]), (3, SIDES[:1]), (0, SIDES))
    fetch_d(0, *BOTH)
    load_o(0)

    @pl.loop(0, ROWS // LANE)
    def _(r):
        at = pl.ds(pl.multiple_of(r * LANE, LANE), LANE)
        g = b.gacc[at, :].astype(BF16).astype(F32)
        b.act[at, :] = (g / (1.0 + jnp.exp(-g)) * b.uacc[at, :].astype(BF16).astype(F32)).astype(BF16)
    drain(b.o_in.at[first(NJ - N1)], b.o_r)
    HA, HBk = first(CUT), pl.ds(CUT, ROWS - CUT)

    rows_of = lambda h: pl.ds(h * HB // N2, HB // N2)

    def sent(i):
        for land, sem in ((b.a1, b.a1s), (b.b1, b.b1s), (b.ta, b.tas), (b.tb, b.tbs)):
            drain(land.at[i], sem.at[i])

    def multiply(i, h):
        slot, k, tall = i % N2, i % N3, part(h)
        drain(b.wt.at[slot, tall], b.wsem.at[N2 * h + slot])
        heads = [t for t in (N2 * h, N2 * h + N1) if roles(i)[t] < N2]
        if heads and i not in loaded_o:
            drain(b.wo_t.at[slot], b.osem.at[slot])
            loaded_o.add(i)

        def some(lo, hi):
            @pl.loop(lo // TILE, hi // TILE)
            def _(r):
                at = pl.ds(pl.multiple_of(r * TILE, TILE), TILE)
                out = lax.dot_general(b.wt[slot, tall].reshape(NB, KB), b.act[at, :], NT, preferred_element_type=F32)
                rows = b.o_in[pl.ds(r * NR, NR)].reshape(TILE, NB)
                if len(heads) == N2:
                    out += lax.dot_general(b.wo_t[slot].reshape(NB, NB), rows, NT, preferred_element_type=F32)
                elif heads:
                    more = lax.dot_general(b.wo_t[slot, roles(i)[heads[N0]]], rows, NT, preferred_element_type=F32)
                    halves = [out[:HB], out[HB:]]
                    halves[heads[N0] - N2 * h] += more
                    out = jnp.concatenate(halves, axis=N0)
                b.sb[k, tall, :, at] = out.astype(BF16).reshape(N2, HB, TILE)

        def first_rows():
            some(N0, CUT)
            if h == FAR:
                for j, d in enumerate(ends(i)):
                    put(b.sb.at[k, N2, rows_of(j), HA], b.ta.at[i, j], b.tas.at[i], b.tar.at[i, j], dict(y=flip(y, d)))
            put(b.sb.at[k, SIDES[h], rows_of(h), HA], b.a1.at[i, h, rows_of(h)], b.a1s.at[i], b.a1r.at[i, h], dict(y=flip(y, ends(i)[h])))
            if h == NEAR and i:
                pass_a(i, h)

        def last_rows():
            some(CUT, ROWS)
            d = ends(i)[h]
            put(b.sb.at[k, tall, mine(N2), HBk], b.tb.at[i, h], b.tbs.at[i], b.tbr.at[i, h], dict(x=flip(x, d)))
            put(b.sb.at[k, tall, mine(d), HBk], b.b1.at[i, h, tall], b.b1s.at[i], b.b1r.at[i, h], dict(x=flip(x, d)))

        for step in (first_rows, last_rows)[::N1 if h else -N1]:
            step()

    loaded_o = set()
    ends = lambda i: SIDES[::-N1] if i == TURNED else SIDES

    def pass_a(i, h):
        k, t, rows = i % N3, SIDES[h], rows_of(N1 - h)
        drain(b.ta.at[i, N1 - h], b.tar.at[i, N1 - h])
        b.sb[k, t, rows, HA] = (b.sb[k, t, rows, HA].astype(F32) + b.ta[i, N1 - h].astype(F32)).astype(BF16)
        put(b.sb.at[k, t, rows, HA], b.a1.at[i, h, rows], b.a1s.at[i], b.a1r.at[i, h], dict(y=flip(y, ends(i)[h])))

    def passed(i, h):
        k, tall = i % N3, part(h)
        if h == FAR or i == N0:
            pass_a(i, h)
        d = ends(i)[N1 - h]
        drain(b.tb.at[i, h], b.tbr.at[i, h])
        b.sb[k, tall, mine(d), HBk] = (b.sb[k, tall, mine(d), HBk].astype(F32) + b.tb[i, h].astype(F32)).astype(BF16)
        put(b.sb.at[k, tall, mine(d), HBk], b.b1.at[i, N1 - h, tall], b.b1s.at[i], b.b1r.at[i, h], dict(x=flip(x, d)))

    def load_a(i):
        for k in range(NC):
            drain(b.a1.at[i, k], b.a1r.at[i, k])
        get(b.a1.at[i], b.va.at[i % N2], b.vsem.at[i % N2])

    def second_a(i):
        dz, va = ORDER[i], b.va.at[i % N2]
        drain(va, b.vsem.at[i % N2])
        b.s2a[dz] = (b.sb[i % N3, N0, :, HA].astype(F32) + (va[N0].astype(F32) + va[N1].astype(F32))).astype(BF16)
        for d in AWAY:
            put(b.s2a.at[dz, mine(d)], b.a2.at[dz, d - N1], b.a2s.at[dz], b.a2r.at[dz], dict(x=flip(x, d)))

    def load_b(i, h):
        drain(b.b1.at[i, :, part(h)], b.b1r.at[i, h])
        get(b.b1.at[i, :, part(h)], b.vb.at[i % N2, :, part(h)], b.vsem.at[N2 + N2 * h + i % N2])

    def second_b(i, h):
        k, tall = i % N3, part(h)
        vb = b.vb.at[i % N2, :, tall]
        drain(vb, b.vsem.at[N2 + N2 * h + i % N2])
        b.s2b[i, tall] = (b.sb[k, tall, mine(N0), HBk].astype(F32) + (vb[N0].astype(F32) + vb[N1].astype(F32))).astype(BF16)
        for t in ((N1,), (N3, N2))[h]:
            put(b.s2b.at[i, t], b.b2.at[i, t - N1], b.b2s.at[i], b.b2r.at[i], dict(y=flip(y, roles(i)[t])))

    def third(i):
        dz = ORDER[i]
        drain(b.a2.at[dz], b.a2r.at[dz])
        drain(b.b2.at[i], b.b2r.at[i])
        for src, own, lanes, at in ((b.a2.at[dz], b.s2a[dz, mine(N0)], HA, LANE), (b.b2.at[i], b.s2b[i, N0], HBk, LANE + CUT)):
            total = own.astype(F32) + sum(src[d].astype(F32) for d in range(NR - N1))
            for cc in range(NC):
                b.fs[dz, cc, :, lanes] = (b.F[dz * NC + cc, :, pl.ds(at, CUT)].astype(F32) + total[cc * FEATS:(cc + N1) * FEATS]).astype(BF16)
        at = z * NC + c
        for cc in sides(dz):
            put(b.fs.at[dz, cc], fin.at[at], b.fin_s, b.fin_r.at[at], dict(z=flip(z, dz), c=cc))
        if dz == N0:
            get(b.fs.at[N0, c], fin.at[at], b.fin_l)

    multiply(N0, FAR)
    multiply(N0, NEAR)
    for dz, g in ((N1, N2), (N3, N2), (N1, N3), (N3, N1)):
        fd.arrive(dz, g)
    fd.pass_on(N2)
    fd.pass_on(N3, N1)
    fd.pass_on(N1, N3)
    fd.z_put(N1, N1)
    fd.z_put(N3, N3)
    fo.forward()
    fetch_d(N1, FAR)
    load_o(N2)
    fetch_d(N2, FAR)
    passed(N0, FAR)
    passed(N0, NEAR)
    multiply(N1, FAR)
    multiply(N2, FAR)
    load_b(N0, FAR)
    load_a(N0)
    load_b(N0, NEAR)
    second_b(N0, FAR)
    second_a(N0)
    second_b(N0, NEAR)
    passed(N1, FAR)
    passed(N2, FAR)
    load_o(N1)
    fd.last(N2)
    fd.last(N3)
    fd.last(N1)
    sent(N0)
    fetch_d(N3, FAR)
    multiply(N3, FAR)
    load_b(N1, FAR)
    load_b(N2, FAR)
    second_b(N1, FAR)
    second_b(N2, FAR)
    fd.arrive(N1, N0)
    fd.arrive(N3, N0)
    fd.pass_on(N0)
    fd.arrive(N1, N1)
    fd.arrive(N3, N3)
    fetch_d(N1, NEAR)
    fetch_d(N2, NEAR)
    multiply(N1, NEAR)
    multiply(N2, NEAR)
    passed(N3, FAR)
    fo.last()
    fd.last(N0)
    fetch_d(N3, NEAR)
    load_o(N3)
    multiply(N3, NEAR)
    passed(N1, NEAR)
    passed(N2, NEAR)
    load_b(N3, FAR)
    load_a(N1)
    load_a(N2)
    second_b(N3, FAR)
    second_a(N1)
    second_a(N2)
    passed(N3, NEAR)
    load_b(N1, NEAR)
    load_b(N2, NEAR)
    second_b(N1, NEAR)
    second_b(N2, NEAR)
    third(N0)
    load_a(N3)
    load_b(N3, NEAR)
    second_a(N3)
    second_b(N3, NEAR)
    third(N1)
    third(N2)
    third(N3)

    for dz in AWAY + (0,):
        for cc in sides(dz):
            at = flip(z, dz) * NC + cc
            drain(fin.at[at], b.fin_r.at[at])
    drain(fin.at[0], b.fin_l)

    some, tile = first(NR - 1), first(TILE)
    for k in RING:
        drain(b.hnT.at[some, 0, :, tile], b.ag_s.at[NC * k])
        drain(b.hnT.at[some, :, :, tile], b.ag_s.at[NC * k + 1])
    for h in range(NC):
        drain(b.S.at[h, first(NJ - 1)], b.s_s.at[h])
    drain(b.F.at[first(NG - 1)], b.f_s)
    drain(b.q_in.at[first(NJ - 1)], b.q_s)
    drain(b.kv_in.at[first(NG - 1)], b.kv_s)
    drain(b.kvw.at[0], b.kw_s)
    drain(kv_half(1, c), b.kw_s)

    @pl.when(x > 0)
    def _():
        drain(kv_half(0, c), b.kw_s)
    drain(b.o_in.at[first(NJ - 1)], b.o_s)
    for dz in ORDER:
        if dz:
            sent(dz)
        drain(b.a2.at[dz], b.a2s.at[dz])
        drain(b.b2.at[dz], b.b2s.at[dz])
    drain(fin.at[first(NG - 1)], b.fin_s)
    for f in (fq, fg, fu, fd, fo):
        f.finish()
    for ref in (b.kc, b.vc):
        drain(ref, b.out_l)


def finish(fin, kc_h, vc_h, out, kc_o, vc_o, fin_v, kc, vc, ov, sem):
    get(fin, fin_v, sem.at[0])
    get(kc_h, kc, sem.at[1])
    get(vc_h, vc, sem.at[2])
    drain(fin_v, sem.at[0])
    row_low = lax.broadcasted_iota(jnp.int32, (FEATS, LANE), 1) < HALF
    for zz in RING:
        for p in range(NG):
            lo, hi = (fin_v[zz * NC + cc, :, pl.ds(p * LANE, LANE)].astype(F32) for cc in range(NC))
            pair = [jnp.where(row_low, lo, pltpu.roll(hi, HALF, 1)), jnp.where(row_low, pltpu.roll(lo, HALF, 1), hi)]
            ov[:, pl.ds(zz * NC * ROWS + p * TILE, TILE)] = jnp.concatenate(pair, axis=1).astype(BF16)
    drain(kc, sem.at[1])
    get(kc, kc_o, sem.at[1])
    drain(vc, sem.at[2])
    get(vc, vc_o, sem.at[2])
    get(ov, out, sem.at[0])
    for i, ref in enumerate((ov, kc, vc)):
        drain(ref, sem.at[i])


def solution(mesh):
    inner = Mesh(mesh.devices.reshape(4, 4, 4, 2), tuple('zyxc'))

    def layer(residual, ln_scale, w_query, w_key, w_value, w_gate, w_up, w_out, w_down, k_cache, v_cache, lengths):
        hbm = pl.BlockSpec(memory_space=pltpu.HBM)
        vmem = pl.BlockSpec(memory_space=pltpu.VMEM)
        smem = pl.BlockSpec(memory_space=pltpu.SMEM)
        shape = lambda a: jax.ShapeDtypeStruct(*a)
        results = [((FEATS, BATCH), BF16), (k_cache.shape, BF16), (v_cache.shape, BF16)]
        fin = ((NG, FEATS, ROWS), BF16)
        outs = [fin] + results[1:] + list(HBM_BUFS.values())
        got = pl.pallas_call(
            kernel,
            out_shape=[shape(a) for a in outs],
            in_specs=[hbm, vmem, smem] + [hbm] * 9,
            out_specs=[hbm] * len(outs),
            scratch_shapes=[pltpu.VMEM(*a) for a in VMEM_BUFS.values()] + [DMA(s) if s else DMA for s in SEMS.values()] + NARROW_SEMS + WIDE_SEMS * 2 + SINGLE_SEMS + NARROW_SEMS,
            name='decode_layer',
            compiler_params=pltpu.CompilerParams(collective_id=0, has_side_effects=True, vmem_limit_bytes=67043328),
        )(residual.T, ln_scale.reshape(1, FEATS), lengths, w_query, w_key, w_value, w_gate, w_up, w_down.T, w_out.T, k_cache, v_cache)
        out, k_new, v_new = pl.pallas_call(
            finish,
            out_shape=[shape(a) for a in results],
            in_specs=[hbm] * 3,
            out_specs=[hbm] * 3,
            scratch_shapes=[pltpu.VMEM(*a) for a in [fin] + results[1:] + results[:1]] + [DMA((3,))],
            name='finish',
        )(*got[:3])
        return out.T, k_new, v_new

    rc, tx, tyz = tuple('zyxc'), tuple('zy'), tuple('xc')
    cache = P(rc, None, None)
    in_specs = (P(None, rc), P(rc), P(tx, tyz), P(tx, None), P(tx, None), P(tx, tyz), P(tx, tyz), P(tyz, tx), P(tyz, tx), cache, cache, P(rc))
    return jax.shard_map(layer, mesh=inner, in_specs=in_specs, out_specs=(P(None, rc), cache, cache), check_vma=False)
```

```python
import jax
import jax.numpy as jnp
from jax import lax
from jax.experimental import pallas as pl
from jax.experimental.pallas import tpu as pltpu
from jax.sharding import Mesh, PartitionSpec as P

LN_EPS = 1e-5
ROPE_BASE = 10000.0
MESH = pl.DeviceIdType.MESH
DMA = pltpu.SemaphoreType.DMA
F32, BF16 = jnp.float32, jnp.bfloat16
ROWS, MODEL, FEATS, BATCH = 1024, 5120, 40, 8192
KB, NB, HB, HD, SUB = 1280, 640, 320, 128, 80
MINE, SEQ, HEADS, LANE, HALF = 64, 64, 40, 128, 64
NR, NC, NJ, NG = 4, 2, 16, 8
X_FIRST = (1,)
CUT = 512
TILE = 256
RING = range(4)
N0, N1, N2, N3 = RING
AWAY = (1, 3, 2)
SIDES = AWAY[:2]
FORTH, BACK = ((1, 0), (3, 1)), ((3, 0), (1, 1))
GROUPS = ((0, 1), (1, 2), (2, 4))
SINGLE = ((0, 1), (1, 2), (2, 3), (3, 4))
ORDER = (0, 1, 3, 2)
BOTH = NEAR, FAR = (0, 1)
TURNED = 2
PAIRS = tuple(sorted(((dy, dx) for dy in RING for dx in RING if dy or dx), key=lambda p: (p.count(2), 0 not in p, abs(p[0] - p[1]))))
NT = (((1,), (1,)), ((), ()))


def flip(i, d):
    return (i, i + 1 - 2 * lax.rem(i, 2), lax.rem(i + 2, 4), 3 - i)[d]


def put(src, dst, ssem, rsem, dev):
    pltpu.make_async_remote_copy(src_ref=src, dst_ref=dst, send_sem=ssem, recv_sem=rsem, device_id=dev, device_id_type=MESH).start()


def added(ref):
    return sum(ref[k].astype(F32) for k in range(NR - 1))


def get(src, dst, sem):
    pltpu.make_async_copy(src, dst, sem).start()


def first(n):
    return pl.ds(0, n)


def drain(ref, sem):
    pltpu.make_async_copy(ref, ref, sem).wait()


class Wide:
    def __init__(self, land, src, sems, pos, groups=GROUPS):
        self.land, self.src = land, src
        self.send, self.yr, self.zr, self.fr, self.dr, self.loc = sems
        self.z, self.y, self.x, self.c = pos
        self.base = self.c * 16
        self.groups = groups
        self.here = set()

    def piece(self, yy):
        return self.src.at[:, pl.ds(pl.multiple_of(yy * NB, LANE), NB)]

    def at(self, dz, g, base=None):
        lo, hi = self.groups[g]
        return self.land.at[pl.ds((self.base if base is None else base) + dz * 4 + lo, hi - lo)]

    def start_local(self):
        get(self.piece(self.y), self.land.at[self.base], self.loc)

    def y_send(self, order=AWAY):
        for dy in order:
            yy = flip(self.y, dy)
            put(self.piece(yy), self.land.at[self.base + dy], self.send, self.yr.at[dy - 1], dict(y=yy))

    def z_send(self, g):
        self.wait_y(g)
        for dz in SIDES:
            self.z_put(g, dz)

    def wait_y(self, g):
        if g:
            for dy in range(*self.groups[g]):
                drain(self.land.at[self.base + dy], self.yr.at[dy - 1])
        self.d2d(0, g)

    def z_put(self, g, dz):
        src = self.at(0, g) if g else self.piece(self.y)
        dst = self.at(dz, g) if g else self.land.at[self.base + dz * 4]
        put(src, dst, self.send, self.zr.at[dz // 2 * len(self.groups) + g], dict(z=flip(self.z, dz)))

    def arrive(self, dz, g):
        drain(self.at(dz, g), self.zr.at[dz // 2 * len(self.groups) + g])
        self.d2d(dz, g)

    def forward(self, g):
        for dz in SIDES:
            self.arrive(dz, g)
        self.pass_on(g)

    def pass_on(self, g, *sides):
        for k, dz in enumerate(SIDES):
            src, dst = (self.at(dz, g), self.at(2, g)) if sides else (self.half(dz, g, k), self.half(2, g, k))
            if dz in (sides or SIDES):
                put(src, dst, self.send, self.fr.at[g], dict(z=flip(self.z, 4 - dz)))

    def half(self, dz, g, k):
        lo, hi = self.groups[g]
        return self.land.at[pl.ds(self.base + dz * 4 + lo, hi - lo), pl.ds(k * HB // 2, HB // 2)]

    def last(self, g):
        drain(self.at(2, g), self.fr.at[g])
        self.d2d(2, g)

    def d2d(self, dz, g):
        to = dict(c=1 - self.c)
        if dz or g:
            put(self.at(dz, g), self.at(dz, g), self.send, self.dr.at[dz * len(self.groups) + g], to)
        else:
            put(self.piece(self.y), self.land.at[self.base], self.send, self.dr.at[0], to)

    def ready(self, dz, g):
        if (dz, g) not in self.here:
            if dz == g == 0:
                drain(self.land.at[self.base], self.loc)
            drain(self.at(dz, g, 16 - self.base), self.dr.at[dz * len(self.groups) + g])
        self.here.add((dz, g))

    def load(self, dz, tile, sem):
        for g in range(len(self.groups)):
            self.ready(dz, g)
        self.bring(dz, 0, NR, tile, sem)

    def bring(self, dz, lo, n, tile, sem):
        for cc in range(NC):
            get(self.land.at[pl.ds(cc * 16 + dz * NR + lo, n)], tile.at[:, :, pl.ds(cc * NB, NB)], sem)

    def finish(self):
        drain(self.land.at[first(31)], self.send)


class Narrow:
    def __init__(self, land, parts, sems, pos):
        self.land, self.parts = land, parts
        self.send, self.yr, self.zr, self.fr, self.dr, self.loc = sems
        self.z, self.y, self.x, self.c = pos
        self.s = lax.rem(self.c + self.y, 2)

    def own(self, slot):
        lo = 0
        for ref in self.parts:
            hi = lo + ref.shape[1]
            yield ref, self.land.at[slot, :, pl.ds(lo, hi - lo)]
            lo = hi

    def start(self):
        @pl.when(self.s == 0)
        def _():
            for src, dst in self.own(0):
                get(src, dst, self.loc)

        @pl.when(self.s == 1)
        def _():
            for src, dst in self.own(1):
                put(src, dst, self.send, self.yr, dict(y=flip(self.y, 1), c=1 - self.c))

    def z_first(self):
        @pl.when(self.s == 0)
        def _():
            for k, dz in enumerate(SIDES):
                for (src, _), (_, dst) in zip(self.own(0), self.own(dz * 2)):
                    put(src, dst, self.send, self.zr.at[k], dict(z=flip(self.z, dz)))
            for src, dst in self.own(0):
                put(src, dst, self.send, self.dr.at[0], dict(c=1 - self.c))

    def z_second(self):
        @pl.when(self.s == 1)
        def _():
            src = self.land.at[1]
            drain(src, self.yr)
            for k, dz in enumerate(SIDES):
                put(src, self.land.at[dz * 2 + 1], self.send, self.zr.at[k], dict(z=flip(self.z, dz)))
            put(src, src, self.send, self.dr.at[0], dict(c=1 - self.c))

    def half(self, slot, k):
        return self.land.at[slot, pl.ds(k * HB // 2, HB // 2)]

    def forward(self):
        for k, dz in enumerate(SIDES):
            slot = dz * 2 + self.s
            piece = self.land.at[slot]
            drain(piece, self.zr.at[k])
            put(self.half(slot, k), self.half(4 + self.s, k), self.send, self.fr.at[k], dict(z=flip(self.z, AWAY[1 - k])))
            put(piece, piece, self.send, self.dr.at[1 + k], dict(c=1 - self.c))

    def last(self):
        for k in range(NC):
            piece = self.half(4 + self.s, k)
            drain(piece, self.fr.at[k])
            put(piece, piece, self.send, self.dr.at[3 + k], dict(c=1 - self.c))

    def load(self, dz, tile, sem):
        o = 1 - self.s
        if dz == 0:
            @pl.when(self.s == 0)
            def _():
                drain(self.land.at[0], self.loc)
        if dz == 2:
            for k in range(NC):
                drain(self.half(4 + o, k), self.dr.at[3 + k])
        else:
            drain(self.land.at[dz * 2 + o], self.dr.at[(dz + 1) // 2])
        get(self.land.at[pl.ds(dz * 2, 2)], tile, sem)

    def finish(self):
        for s in range(NC):
            @pl.when(self.s == s)
            def _():
                drain(self.land.at[first(7 + s)], self.send)


class Ring:
    def __init__(self, axis, at, own, land, moved, sems):
        self.axis, self.at, self.own, self.land, self.moved = axis, at, own, land, moved
        self.send, self.recv = sems

    def to(self, d):
        return {self.axis: flip(self.at, d)}

    def start(self):
        for k in range(NC):
            for d, h in ((1, k), (3, 1 - k)):
                put(self.own(h), self.land(d, h), self.send, self.recv.at[d - 1 + h], self.to(d))

    def forward(self):
        for d, h in FORTH:
            drain(self.moved(d, h), self.recv.at[d - 1 + h])
            put(self.moved(d, h), self.moved(2, h) if self.axis == 'y' else self.moved(d, h), self.send, self.recv.at[4 + h], self.to(4 - d))

    def finish(self):
        for d, h in BACK:
            drain(self.moved(d, h), self.recv.at[d - 1 + h])
        for h in range(NC):
            drain(self.moved(2, h), self.recv.at[4 + h])


WIDE_SEMS, SINGLE_SEMS = ([DMA, DMA((NR - 1,)), DMA((2 * n,)), DMA((n,)), DMA((NR * n,)), DMA] for n in map(len, (GROUPS, SINGLE)))
NARROW_SEMS = [DMA, DMA, DMA((2,)), DMA((2,)), DMA((5,)), DMA]
HBM_BUFS = dict(
    Q=((NG, HB, NB), BF16), G=((NG * NR, HB, NB), BF16), U=((NG * NR, HB, NB), BF16), D=((NG * NR, HB, NB), BF16), O=((NG, HB, NB), BF16),
    hnT=((NR, NR, HB, ROWS), BF16), a1=((NR, NC, HB, CUT), BF16), b1=((NR, NC, NR, SUB, ROWS - CUT), BF16))
VMEM_BUFS = dict(
    rT=((FEATS, BATCH), BF16), xs=((NG, FEATS, ROWS + LANE), BF16), F=((NG, FEATS, ROWS + LANE), BF16), S=((NC, NJ, 2, CUT), F32),
    hs=((NR, SUB, ROWS), BF16), hn=((NR, ROWS, KB), BF16), wt=((NC, NR, HB, KB), BF16), wo_t=((NC, NC, HB, NB), BF16),
    gacc=((ROWS, KB), F32), uacc=((ROWS, KB), F32), qout=((NJ, MINE, NB), BF16), kvout=((NJ, MINE, 2 * HD), BF16), kvw=((NC, NC, HB, HD), BF16), q_in=((NJ, MINE, NB), BF16), kv_in=((NG, MINE, 2 * HD), BF16),
    q3=((MINE * HEADS, HD), F32), lenb=((MINE, HD), F32), kc=((MINE, SEQ, HD), BF16), vc=((MINE, SEQ, HD), BF16), kn=((MINE, 2 * HD), F32),
    o_v=((MINE, MODEL), BF16), o_in=((NJ, MINE, NB), BF16), act=((ROWS, KB), BF16), sb=((NR - 1, NR, HB, ROWS), BF16),
    va=((NC, NC, HB, CUT), BF16), vb=((NC, NC, NR, SUB, ROWS - CUT), BF16),
    ta=((NR, NC, HB // 2, CUT), BF16), tb=((NR, NC, NR // 2, SUB, ROWS - CUT), BF16), s2a=((NR, HB, CUT), BF16), s2b=((NR, NR, SUB, ROWS - CUT), BF16),
    a2=((NR, NR - 1, SUB, CUT), BF16), b2=((NR, NR - 1, SUB, ROWS - CUT), BF16), fs=((NR, NC, FEATS, ROWS), BF16))
ONE, EACH, BY_GROUP = (), (NR,), (NG,)
SEMS = dict(f_s=ONE, fin_l=ONE, s_s=EACH, s_r=EACH, own_l=EACH, q_s=ONE, kw_s=ONE, kw_z=ONE, kw_y=ONE, kw_c=EACH, q_r=ONE, kv_s=ONE, kv_r=ONE, o_s=ONE, o_r=ONE, fin_s=ONE, out_l=ONE,
            a1s=EACH, b1s=EACH, a2s=EACH, a2r=EACH, b2s=EACH, b2r=EACH, ag_s=BY_GROUP, ag_r=(NG, NG), tas=EACH, tbs=EACH, tar=(NR, NC), tbr=(NR, NC), b1r=(NR, NC), a1r=(NR, NC), ld=EACH, wsem=EACH, osem=EACH, vsem=BY_GROUP,
            f_r=(NC, NG), fin_r=BY_GROUP)


def kernel(res, ls, lens, wq, wk, wv, wg, wu, wdT, woT, kc_h, vc_h, fin, kc_o, vc_o, *rest):
    rest = list(rest)

    class b:
        pass
    for name in list(HBM_BUFS) + list(VMEM_BUFS) + list(SEMS):
        setattr(b, name, rest.pop(0))
    pos = z, y, x, c = tuple(lax.axis_index(a) for a in 'zyxc')
    flow = lambda kind, land, src, *more: kind(land, src, [rest.pop(0) for _ in WIDE_SEMS], pos, *more)
    fq = flow(Narrow, b.Q, (wq,))
    fg, fu, fd = flow(Wide, b.G, wg), flow(Wide, b.U, wu), flow(Wide, b.D, wdT, SINGLE)
    fo = flow(Narrow, b.O, (woT,))
    me = y * 4 + x
    row_low = lax.broadcasted_iota(jnp.int32, (FEATS, LANE), 1) < HALF
    sides = lambda dz: (c, 1 - c)[not dz:]

    bar = pltpu.get_barrier_semaphore()
    peers = [dict(z=flip(z, dz), c=cc) for dz in AWAY for cc in (c, 1 - c)] + [dict(c=1 - c), dict(y=flip(y, 1), c=1 - c)]
    peers += [dict(y=flip(y, dy), x=flip(x, dx)) for dy, dx in PAIRS]
    for p in peers:
        pl.semaphore_signal(bar, inc=1, device_id=p, device_id_type=MESH)
    get(res, b.rT, b.ld.at[0])
    get(kc_h, b.kc, b.ld.at[1])
    get(vc_h, b.vc, b.ld.at[2])
    for f in (fg, fu, fd):
        f.start_local()
    pl.semaphore_wait(bar, len(peers))
    fq.start()

    drain(b.rT, b.ld.at[0])
    scale = jnp.broadcast_to(ls[...].astype(F32), (LANE, FEATS)).T.astype(BF16)
    wide = lambda h: pl.ds(LANE * h + CUT * h, CUT + LANE * (1 - h))
    for i in range(NG):
        b.xs[i, :, :LANE] = scale
    for h in range(NC):
        for dz in AWAY + (0,):
            zz = flip(z, dz)
            for p in range(NR * h, NR * h + NR):
                pair = b.rT[:, pl.ds(pl.multiple_of(zz * NC * ROWS + p * TILE, LANE), TILE)].astype(F32)
                t0, t1 = pair[:, :LANE], pair[:, LANE:]
                at = pl.ds(LANE + p * LANE, LANE)
                b.xs[dz * NC, :, at] = jnp.where(row_low, t0, pltpu.roll(t1, HALF, 1)).astype(BF16)
                b.xs[dz * NC + 1, :, at] = jnp.where(row_low, pltpu.roll(t0, HALF, 1), t1).astype(BF16)
            for cc in sides(dz):
                put(b.xs.at[dz * NC + cc, :, wide(h)], b.F.at[dz * NC + c, :, wide(h)], b.f_s, b.f_r.at[h, dz * NC + c], dict(z=flip(z, dz), c=cc))
    b.F[c] = b.xs[c]
    def kv_half(slot, side):
        return b.kvw.at[slot, side]

    for side, w in enumerate((wk, wv)):
        @pl.when((c == side) & (x == 0))
        def _():
            get(w, kv_half(0, side), b.kw_z)

        @pl.when((c == side) & (x > 0))
        def _():
            zx = lax.rem(z // 2 + x // 2, 2) * 2 + lax.rem(z + x, 2)
            put(w, kv_half(0, side), b.kw_s, b.kw_z, dict(z=zx))
    fq.z_first()
    fg.z_send(0)

    for h in range(NC):
        for dz in RING:
            for cc in sides(dz):
                drain(b.F.at[dz * NC + cc, :, wide(h)], b.f_r.at[h, dz * NC + cc])
        tot = sq = jnp.zeros((FEATS, CUT), F32)
        for i in range(NG):
            v = b.F[i, :, pl.ds(LANE + CUT * h, CUT)].astype(F32)
            tot, sq = tot + v, sq + v * v
        b.S[h, me] = jnp.concatenate([jnp.sum(v, axis=0, keepdims=True) for v in (tot, sq)], axis=0)
        for dy, dx in PAIRS:
            put(b.S.at[h, me], b.S.at[h, me], b.s_s.at[h], b.s_r.at[h], dict(y=flip(y, dy), x=flip(x, dx)))
    fq.z_second()
    fo.z_first()

    mine = lambda d: pl.ds(pl.multiple_of(flip(x, d) * SUB, 16), SUB)

    def normalize(h):
        drain(b.S.at[h, first(NJ - 1)], b.s_r.at[h])
        stats = sum(b.S[h, i] for i in range(NJ)) / MODEL
        mean = stats[0:1]
        inv = lax.rsqrt(stats[1:] - mean * mean + LN_EPS)
        lanes = pl.ds(CUT * h, CUT)
        for dz in RING:
            both = []
            for i in (dz * NC, dz * NC + 1):
                both.append((b.F[i, :, pl.ds(LANE + CUT * h, CUT)].astype(F32) - mean) * inv * b.F[i, :, :LANE].astype(F32)[:, :1])
            b.hs[dz, :, lanes] = jnp.concatenate(both, axis=0).astype(BF16)
        get(b.hs.at[:, :, lanes], b.hnT.at[:, 0, mine(0), lanes], b.own_l.at[h])

    part = lambda h: pl.ds(2 * h, 2)

    def rings(k):
        lanes = pl.ds(k * TILE, TILE)
        far = lambda d, h: b.hnT.at[part(h), :, mine(d), lanes]
        near = lambda d, h: b.hnT.at[part(h), d, mine(0), lanes]
        own = lambda h: b.hs.at[part(h), :, lanes]
        sems = [(b.ag_s.at[NC * k + j], b.ag_r.at[NC * k + j]) for j in range(NC)]
        if k in X_FIRST:
            spot = lambda d, h: b.hnT.at[part(h), 0, mine(d), lanes]
            row = lambda d, h: b.hnT.at[part(h), d, :, lanes]
            return Ring('x', x, own, lambda d, h: spot(0, h), spot, sems[0]), Ring('y', y, lambda h: row(0, h), row, row, sems[1])
        return Ring('y', y, own, near, near, sems[0]), Ring('x', x, lambda h: far(0, h), lambda d, h: far(0, h), far, sems[1])

    one, two = zip(*(rings(k) for k in RING))
    normalize(0)
    one[0].start()
    one[1].start()
    one[0].forward()
    one[1].forward()
    normalize(1)
    one[2].start()
    one[3].start()
    for h in range(NC):
        drain(b.hs.at[:, :, pl.ds(CUT * h, CUT)], b.own_l.at[h])
    one[0].finish()
    two[0].start()
    one[2].forward()
    one[3].forward()
    drain(kv_half(0, c), b.kw_z)
    put(kv_half(0, c), kv_half(1, c), b.kw_s, b.kw_y, dict(y=flip(y, 1)))
    put(kv_half(0, c), kv_half(0, c), b.kw_s, b.kw_c.at[0], dict(c=1 - c))
    fg.y_send()
    one[1].finish()
    two[1].start()
    two[0].forward()
    fq.forward()
    fg.forward(0)
    one[2].finish()
    two[2].start()
    one[3].finish()
    fg.z_send(1)
    fq.last()
    drain(kv_half(1, c), b.kw_y)
    put(kv_half(1, c), kv_half(1, c), b.kw_s, b.kw_c.at[1], dict(c=1 - c))

    def load_q(pair):
        for i in range(NC):
            fq.load(NC * pair + i, b.sb.at[pair, part(i), :, first(NB)], b.osem.at[pair])

    def stage(k):
        two[k].finish()
        for dz in RING:
            get(b.hnT.at[dz, :, :, pl.ds(k * TILE, TILE)], b.wt.at[1, :, :, pl.ds(dz * TILE, TILE)], b.wsem.at[1])

    def turn(k):
        drain(b.wt.at[1, :, :, first(ROWS)], b.wsem.at[1])
        for dz in RING:
            for h in range(NC):
                b.hn[dz, pl.ds(k * TILE + h * LANE, LANE), :] = b.wt[1, :, :, pl.ds(dz * TILE + h * LANE, LANE)].reshape(KB, LANE).T

    def query(k):
        at = pl.ds(k * TILE, TILE)
        new = sum(jnp.dot(b.hn[dz, at, :NB], b.sb[dz // 2, part(dz % 2), :, :NB].reshape(NB, NB), preferred_element_type=F32) for dz in RING)
        b.qout[pl.ds(k * NR, NR)] = new.astype(BF16).reshape(NR, MINE, NB)
        kv = jnp.concatenate([b.kvw[:, side].reshape(NB, HD) for side in range(NC)], axis=1)
        new = jnp.dot(b.hn[x, at, :NB], kv, preferred_element_type=F32)
        b.kvout[pl.ds(k * NR, NR)] = new.astype(BF16).reshape(NR, MINE, 2 * HD)

    def project(acc, i, slot, lo=0, hi=ROWS, fresh=False, wait=True):
        if wait:
            drain(b.wt.at[slot], b.wsem.at[slot])

        @pl.loop(lo // TILE, hi // TILE)
        def _(r):
            at = pl.ds(pl.multiple_of(r * TILE, TILE), TILE)
            new = jnp.dot(b.hn[ORDER[i], at, :], b.wt[slot].reshape(KB, KB), preferred_element_type=F32)
            acc[at, :] = new if fresh else new + acc[at, :]

    fetch = lambda f, i, slot: f.load(ORDER[i], b.wt.at[slot], b.wsem.at[slot])

    def roles(i):
        return (0, 3, 2, 1) if i == TURNED else tuple(RING)

    def fetch_d(i, *parts):
        for h in parts:
            for t in (2 * h, 2 * h + 1):
                g = roles(i)[t]
                fd.ready(ORDER[i], g)
                fd.bring(ORDER[i], g, 1, b.wt.at[i % 2, pl.ds(t, 1)], b.wsem.at[2 * h + i % 2])


    fg.z_send(2)
    fu.z_send(0)
    load_q(0)
    load_q(1)
    stage(0)
    two[2].forward()
    two[3].start()
    turn(0)
    for pair in range(NC):
        drain(b.sb.at[pair, :, :, first(NB)], b.osem.at[pair])
    for slot in range(NC):
        drain(kv_half(slot, 1 - c), b.kw_c.at[slot])
    query(0)
    two[1].forward()
    fu.y_send()
    fg.forward(1)
    stage(2)
    turn(2)
    query(2)
    fetch(fg, 0, 0)
    two[3].forward()
    stage(1)
    turn(1)
    query(1)
    fg.forward(2)
    fg.last(0)
    project(b.gacc, 0, 0, 0, 3 * TILE, fresh=True)
    fu.z_send(1)
    fu.forward(0)
    fetch(fg, 1, 0)
    project(b.gacc, 1, 0, 0, 3 * TILE)
    fu.z_send(2)
    stage(3)
    turn(3)
    fetch(fg, 0, 1)
    query(3)
    for dy in (0, 2):
        for dx in AWAY + (0,)[:dy]:
            yy, xx = flip(y, dy), flip(x, dx)
            put(b.kvout.at[yy * NR + xx], b.kv_in.at[2 * dy + x], b.kv_s, b.kv_r, dict(y=yy, x=xx))
    for dy, dx in PAIRS:
        yy, xx = flip(y, dy), flip(x, dx)
        put(b.qout.at[yy * NR + xx], b.q_in.at[me], b.q_s, b.q_r, dict(y=yy, x=xx))
    b.q_in[me] = b.qout[me]
    b.kv_in[x] = b.kvout[me]
    fo.start()
    fd.y_send((2, 1, 3))

    project(b.gacc, 1, 0, 3 * TILE, ROWS, fresh=True, wait=False)
    fetch(fg, 2, 0)
    project(b.gacc, 0, 1, 3 * TILE, ROWS)
    fg.last(1)
    fg.last(2)
    fetch(fg, 3, 1)
    project(b.gacc, 2, 0)
    fu.forward(1)
    fetch(fu, 0, 0)
    project(b.gacc, 3, 1)
    project(b.uacc, 0, 0, fresh=True)
    drain(b.kc, b.ld.at[1])
    drain(b.vc, b.ld.at[2])
    drain(b.q_in.at[first(NJ - 1)], b.q_r)
    drain(b.kv_in.at[first(NG - 1)], b.kv_r)

    @pl.loop(0, MINE)
    def _(r):
        b.lenb[pl.ds(r, 1), :] = jnp.broadcast_to(lens[r], (1, HD)).astype(F32)
    i_half = lax.rem(lax.broadcasted_iota(jnp.int32, (MINE, HD), 1), HALF).astype(F32)
    angle = b.lenb[...] * jnp.power(ROPE_BASE, i_half * (-2.0 / HD))
    low = lax.broadcasted_iota(jnp.int32, (MINE, HD), 1) < HALF
    cos = jnp.cos(angle)
    sin = jnp.where(low, -jnp.sin(angle), jnp.sin(angle))
    rope = lambda v: v * cos + pltpu.roll(v, HALF, 1) * sin
    kv = sum(b.kv_in[i].astype(F32) for i in range(NG)).astype(BF16).astype(F32)
    b.kn[:, :HD] = rope(kv[:, :HD])
    b.kn[:, HD:] = kv[:, HD:]
    for xs in RING:
        for yh in range(NC):
            q = (b.q_in[yh * 4 + xs].astype(F32) + b.q_in[(yh + 2) * 4 + xs].astype(F32)).astype(BF16).astype(F32)
            for h in range(5):
                b.q3[pl.ds(xs * 10 + yh * 5 + h, MINE, stride=HEADS), :] = rope(q[:, h * HD:(h + 1) * HD])
    t_row = lax.broadcasted_iota(jnp.int32, (SEQ, HD), 0)
    t_col = lax.broadcasted_iota(jnp.int32, (HEADS, SEQ), 1)

    def attend(rows):
        ats = [pl.ds(pl.multiple_of(r * HEADS, 8), HEADS) for r in rows]
        here = [t_row == lens[r] for r in rows]
        new = [b.kn[pl.ds(r, 1), :] for r in rows]
        keys = [jnp.where(h, n[:, :HD].astype(BF16).astype(F32), b.kc[r].astype(F32)).astype(BF16) for r, h, n in zip(rows, here, new)]
        vals = [jnp.where(h, n[:, HD:], b.vc[r].astype(F32)).astype(BF16) for r, h, n in zip(rows, here, new)]
        s = [lax.dot_general(b.q3[at, :].astype(BF16), k, NT, preferred_element_type=F32) for at, k in zip(ats, keys)]
        s = [jnp.where(t_col <= lens[r], v * (HD ** -0.5), -1e30) for r, v in zip(rows, s)]
        top = [jnp.max(v, axis=1, keepdims=True) for v in s]
        e = [jnp.exp(v - t) for v, t in zip(s, top)]
        total = [jnp.sum(v, axis=1, keepdims=True) for v in e]
        p = [(v / t).astype(BF16) for v, t in zip(e, total)]
        o = [jnp.dot(v, w, preferred_element_type=F32) for v, w in zip(p, vals)]
        for r, at, k, v, w in zip(rows, ats, keys, vals, o):
            b.kc[r], b.vc[r], b.q3[at, :] = k, v, w

    def attend_some(lo, hi):
        @pl.loop(lo // NG, hi // NG)
        def _(step):
            attend([step * NG + k for k in range(NG)])

    attend_some(0, MINE)
    get(b.kc, kc_o, b.out_l)
    get(b.vc, vc_o, b.out_l)
    for h in range(HEADS):
        b.o_v[:, h * HD:(h + 1) * HD] = b.q3[pl.ds(h, MINE, stride=HEADS), :].astype(BF16)
    block = lambda yy, xx: b.o_v.at[:, pl.ds(pl.multiple_of((xx * 2 + lax.rem(yy, 2)) * NB, LANE), NB)]
    for dy, dx in PAIRS:
        yy, xx = flip(y, dy), flip(x, dx)
        put(block(yy, xx), b.o_in.at[me], b.o_s, b.o_r, dict(y=yy, x=xx))
    b.o_in[me] = block(y, x)[...]

    def start_d(*plan):
        for g, planes in plan:
            fd.wait_y(g)
            for dz in planes:
                fd.z_put(g, dz)

    fu.forward(2)
    fo.z_second()
    fetch(fu, 1, 1)
    fetch(fu, 2, 0)
    project(b.uacc, 1, 1)
    project(b.uacc, 2, 0)
    start_d((2, SIDES))
    fu.last(0)
    fu.last(1)
    fu.last(2)
    fetch(fu, 3, 1)
    load_o = lambda i: fo.load(ORDER[i], b.wo_t.at[i % 2], b.osem.at[i % 2])
    project(b.uacc, 3, 1)
    start_d((1, SIDES[1:]), (3, SIDES[:1]), (0, SIDES))
    fetch_d(0, *BOTH)
    load_o(0)

    @pl.loop(0, ROWS // LANE)
    def _(r):
        at = pl.ds(pl.multiple_of(r * LANE, LANE), LANE)
        g = b.gacc[at, :].astype(BF16).astype(F32)
        b.act[at, :] = (g / (1.0 + jnp.exp(-g)) * b.uacc[at, :].astype(BF16).astype(F32)).astype(BF16)
    drain(b.o_in.at[first(NJ - N1)], b.o_r)
    HA, HBk = first(CUT), pl.ds(CUT, ROWS - CUT)

    rows_of = lambda h: pl.ds(h * HB // N2, HB // N2)

    def sent(i):
        for land, sem in ((b.a1, b.a1s), (b.b1, b.b1s), (b.ta, b.tas), (b.tb, b.tbs)):
            drain(land.at[i], sem.at[i])

    def multiply(i, h):
        slot, k, tall = i % N2, i % N3, part(h)
        drain(b.wt.at[slot, tall], b.wsem.at[N2 * h + slot])
        heads = [t for t in (N2 * h, N2 * h + N1) if roles(i)[t] < N2]
        if heads and i not in loaded_o:
            drain(b.wo_t.at[slot], b.osem.at[slot])
            loaded_o.add(i)

        def some(lo, hi):
            @pl.loop(lo // TILE, hi // TILE)
            def _(r):
                at = pl.ds(pl.multiple_of(r * TILE, TILE), TILE)
                out = lax.dot_general(b.wt[slot, tall].reshape(NB, KB), b.act[at, :], NT, preferred_element_type=F32)
                rows = b.o_in[pl.ds(r * NR, NR)].reshape(TILE, NB)
                if len(heads) == N2:
                    out += lax.dot_general(b.wo_t[slot].reshape(NB, NB), rows, NT, preferred_element_type=F32)
                elif heads:
                    more = lax.dot_general(b.wo_t[slot, roles(i)[heads[N0]]], rows, NT, preferred_element_type=F32)
                    halves = [out[:HB], out[HB:]]
                    halves[heads[N0] - N2 * h] += more
                    out = jnp.concatenate(halves, axis=N0)
                b.sb[k, tall, :, at] = out.astype(BF16).reshape(N2, HB, TILE)

        def first_rows():
            some(N0, CUT)
            if h == FAR:
                for j, d in enumerate(ends(i)):
                    put(b.sb.at[k, N2, rows_of(j), HA], b.ta.at[i, j], b.tas.at[i], b.tar.at[i, j], dict(y=flip(y, d)))
            put(b.sb.at[k, SIDES[h], rows_of(h), HA], b.a1.at[i, h, rows_of(h)], b.a1s.at[i], b.a1r.at[i, h], dict(y=flip(y, ends(i)[h])))
            if h == NEAR and i:
                pass_a(i, h)

        def last_rows():
            some(CUT, ROWS)
            d = ends(i)[h]
            put(b.sb.at[k, tall, mine(N2), HBk], b.tb.at[i, h], b.tbs.at[i], b.tbr.at[i, h], dict(x=flip(x, d)))
            put(b.sb.at[k, tall, mine(d), HBk], b.b1.at[i, h, tall], b.b1s.at[i], b.b1r.at[i, h], dict(x=flip(x, d)))

        for step in (first_rows, last_rows)[::N1 if h else -N1]:
            step()

    loaded_o = set()
    ends = lambda i: SIDES[::-N1] if i == TURNED else SIDES

    def pass_a(i, h):
        k, t, rows = i % N3, SIDES[h], rows_of(N1 - h)
        drain(b.ta.at[i, N1 - h], b.tar.at[i, N1 - h])
        b.sb[k, t, rows, HA] = (b.sb[k, t, rows, HA].astype(F32) + b.ta[i, N1 - h].astype(F32)).astype(BF16)
        put(b.sb.at[k, t, rows, HA], b.a1.at[i, h, rows], b.a1s.at[i], b.a1r.at[i, h], dict(y=flip(y, ends(i)[h])))

    def passed(i, h):
        k, tall = i % N3, part(h)
        if h == FAR or i == N0:
            pass_a(i, h)
        d = ends(i)[N1 - h]
        drain(b.tb.at[i, h], b.tbr.at[i, h])
        b.sb[k, tall, mine(d), HBk] = (b.sb[k, tall, mine(d), HBk].astype(F32) + b.tb[i, h].astype(F32)).astype(BF16)
        put(b.sb.at[k, tall, mine(d), HBk], b.b1.at[i, N1 - h, tall], b.b1s.at[i], b.b1r.at[i, h], dict(x=flip(x, d)))

    def load_a(i):
        for k in range(NC):
            drain(b.a1.at[i, k], b.a1r.at[i, k])
        get(b.a1.at[i], b.va.at[i % N2], b.vsem.at[i % N2])

    def second_a(i):
        dz, va = ORDER[i], b.va.at[i % N2]
        drain(va, b.vsem.at[i % N2])
        b.s2a[dz] = (b.sb[i % N3, N0, :, HA].astype(F32) + (va[N0].astype(F32) + va[N1].astype(F32))).astype(BF16)
        for d in AWAY:
            put(b.s2a.at[dz, mine(d)], b.a2.at[dz, d - N1], b.a2s.at[dz], b.a2r.at[dz], dict(x=flip(x, d)))

    def load_b(i, h):
        drain(b.b1.at[i, :, part(h)], b.b1r.at[i, h])
        get(b.b1.at[i, :, part(h)], b.vb.at[i % N2, :, part(h)], b.vsem.at[N2 + N2 * h + i % N2])

    def second_b(i, h):
        k, tall = i % N3, part(h)
        vb = b.vb.at[i % N2, :, tall]
        drain(vb, b.vsem.at[N2 + N2 * h + i % N2])
        b.s2b[i, tall] = (b.sb[k, tall, mine(N0), HBk].astype(F32) + (vb[N0].astype(F32) + vb[N1].astype(F32))).astype(BF16)
        for t in ((N1,), (N3, N2))[h]:
            put(b.s2b.at[i, t], b.b2.at[i, t - N1], b.b2s.at[i], b.b2r.at[i], dict(y=flip(y, roles(i)[t])))

    def third(i):
        dz = ORDER[i]
        drain(b.a2.at[dz], b.a2r.at[dz])
        drain(b.b2.at[i], b.b2r.at[i])
        for src, own, lanes, at in ((b.a2.at[dz], b.s2a[dz, mine(N0)], HA, LANE), (b.b2.at[i], b.s2b[i, N0], HBk, LANE + CUT)):
            total = own.astype(F32) + sum(src[d].astype(F32) for d in range(NR - N1))
            for cc in range(NC):
                b.fs[dz, cc, :, lanes] = (b.F[dz * NC + cc, :, pl.ds(at, CUT)].astype(F32) + total[cc * FEATS:(cc + N1) * FEATS]).astype(BF16)
        at = z * NC + c
        for cc in sides(dz):
            put(b.fs.at[dz, cc], fin.at[at], b.fin_s, b.fin_r.at[at], dict(z=flip(z, dz), c=cc))
        if dz == N0:
            get(b.fs.at[N0, c], fin.at[at], b.fin_l)

    multiply(N0, FAR)
    multiply(N0, NEAR)
    for dz, g in ((N1, N2), (N3, N2), (N1, N3), (N3, N1)):
        fd.arrive(dz, g)
    fd.z_put(N1, N1)
    fd.z_put(N3, N3)
    fd.pass_on(N2)
    fd.pass_on(N3, N1)
    fd.pass_on(N1, N3)
    fo.forward()
    fetch_d(N1, FAR)
    load_o(N2)
    fetch_d(N2, FAR)
    passed(N0, FAR)
    passed(N0, NEAR)
    multiply(N1, FAR)
    multiply(N2, FAR)
    load_b(N0, FAR)
    load_a(N0)
    load_b(N0, NEAR)
    second_b(N0, FAR)
    second_a(N0)
    second_b(N0, NEAR)
    passed(N1, FAR)
    load_o(N1)
    fd.arrive(N1, N0)
    fd.arrive(N3, N0)
    fd.pass_on(N0)
    fd.arrive(N1, N1)
    fd.arrive(N3, N3)
    fetch_d(N1, NEAR)
    fetch_d(N2, NEAR)
    multiply(N1, NEAR)
    passed(N2, FAR)
    multiply(N2, NEAR)
    fd.last(N2)
    fd.last(N3)
    fd.last(N1)
    sent(N0)
    fetch_d(N3, FAR)
    multiply(N3, FAR)
    passed(N1, NEAR)
    passed(N2, NEAR)
    load_b(N1, FAR)
    load_b(N2, FAR)
    second_b(N1, FAR)
    second_b(N2, FAR)
    fo.last()
    fd.last(N0)
    fetch_d(N3, NEAR)
    load_o(N3)
    passed(N3, FAR)
    multiply(N3, NEAR)
    load_a(N1)
    load_a(N2)
    second_a(N1)
    second_a(N2)
    load_b(N1, NEAR)
    load_b(N2, NEAR)
    second_b(N1, NEAR)
    second_b(N2, NEAR)
    passed(N3, NEAR)
    third(N0)
    load_b(N3, FAR)
    second_b(N3, FAR)
    load_a(N3)
    second_a(N3)
    load_b(N3, NEAR)
    second_b(N3, NEAR)
    third(N1)
    third(N2)
    third(N3)

    for dz in AWAY + (0,):
        for cc in sides(dz):
            at = flip(z, dz) * NC + cc
            drain(fin.at[at], b.fin_r.at[at])
    drain(fin.at[0], b.fin_l)

    some, tile = first(NR - 1), first(TILE)
    for k in RING:
        drain(b.hnT.at[some, 0, :, tile], b.ag_s.at[NC * k])
        drain(b.hnT.at[some, :, :, tile], b.ag_s.at[NC * k + 1])
    for h in range(NC):
        drain(b.S.at[h, first(NJ - 1)], b.s_s.at[h])
    drain(b.F.at[first(NG - 1)], b.f_s)
    drain(b.q_in.at[first(NJ - 1)], b.q_s)
    drain(b.kv_in.at[first(NG - 1)], b.kv_s)
    drain(b.kvw.at[0], b.kw_s)
    drain(kv_half(1, c), b.kw_s)

    @pl.when(x > 0)
    def _():
        drain(kv_half(0, c), b.kw_s)
    drain(b.o_in.at[first(NJ - 1)], b.o_s)
    for dz in ORDER:
        if dz:
            sent(dz)
        drain(b.a2.at[dz], b.a2s.at[dz])
        drain(b.b2.at[dz], b.b2s.at[dz])
    drain(fin.at[first(NG - 1)], b.fin_s)
    for f in (fq, fg, fu, fd, fo):
        f.finish()
    for ref in (b.kc, b.vc):
        drain(ref, b.out_l)


def finish(fin, kc_h, vc_h, out, kc_o, vc_o, fin_v, kc, vc, ov, sem):
    get(fin, fin_v, sem.at[0])
    get(kc_h, kc, sem.at[1])
    get(vc_h, vc, sem.at[2])
    drain(fin_v, sem.at[0])
    row_low = lax.broadcasted_iota(jnp.int32, (FEATS, LANE), 1) < HALF
    for zz in RING:
        for p in range(NG):
            lo, hi = (fin_v[zz * NC + cc, :, pl.ds(p * LANE, LANE)].astype(F32) for cc in range(NC))
            pair = [jnp.where(row_low, lo, pltpu.roll(hi, HALF, 1)), jnp.where(row_low, pltpu.roll(lo, HALF, 1), hi)]
            ov[:, pl.ds(zz * NC * ROWS + p * TILE, TILE)] = jnp.concatenate(pair, axis=1).astype(BF16)
    drain(kc, sem.at[1])
    get(kc, kc_o, sem.at[1])
    drain(vc, sem.at[2])
    get(vc, vc_o, sem.at[2])
    get(ov, out, sem.at[0])
    for i, ref in enumerate((ov, kc, vc)):
        drain(ref, sem.at[i])


def solution(mesh):
    inner = Mesh(mesh.devices.reshape(4, 4, 4, 2), tuple('zyxc'))

    def layer(residual, ln_scale, w_query, w_key, w_value, w_gate, w_up, w_out, w_down, k_cache, v_cache, lengths):
        hbm = pl.BlockSpec(memory_space=pltpu.HBM)
        vmem = pl.BlockSpec(memory_space=pltpu.VMEM)
        smem = pl.BlockSpec(memory_space=pltpu.SMEM)
        shape = lambda a: jax.ShapeDtypeStruct(*a)
        results = [((FEATS, BATCH), BF16), (k_cache.shape, BF16), (v_cache.shape, BF16)]
        fin = ((NG, FEATS, ROWS), BF16)
        outs = [fin] + results[1:] + list(HBM_BUFS.values())
        got = pl.pallas_call(
            kernel,
            out_shape=[shape(a) for a in outs],
            in_specs=[hbm, vmem, smem] + [hbm] * 9,
            out_specs=[hbm] * len(outs),
            scratch_shapes=[pltpu.VMEM(*a) for a in VMEM_BUFS.values()] + [DMA(s) if s else DMA for s in SEMS.values()] + NARROW_SEMS + WIDE_SEMS * 2 + SINGLE_SEMS + NARROW_SEMS,
            name='decode_layer',
            compiler_params=pltpu.CompilerParams(collective_id=0, has_side_effects=True, vmem_limit_bytes=67043328),
        )(residual.T, ln_scale.reshape(1, FEATS), lengths, w_query, w_key, w_value, w_gate, w_up, w_down.T, w_out.T, k_cache, v_cache)
        out, k_new, v_new = pl.pallas_call(
            finish,
            out_shape=[shape(a) for a in results],
            in_specs=[hbm] * 3,
            out_specs=[hbm] * 3,
            scratch_shapes=[pltpu.VMEM(*a) for a in [fin] + results[1:] + results[:1]] + [DMA((3,))],
            name='finish',
        )(*got[:3])
        return out.T, k_new, v_new

    rc, tx, tyz = tuple('zyxc'), tuple('zy'), tuple('xc')
    cache = P(rc, None, None)
    in_specs = (P(None, rc), P(rc), P(tx, tyz), P(tx, None), P(tx, None), P(tx, tyz), P(tx, tyz), P(tyz, tx), P(tyz, tx), cache, cache, P(rc))
    return jax.shard_map(layer, mesh=inner, in_specs=in_specs, out_specs=(P(None, rc), cache, cache), check_vma=False)
```

```python
import jax
import jax.numpy as jnp
from jax import lax
from jax.experimental import pallas as pl
from jax.experimental.pallas import tpu as pltpu
from jax.sharding import Mesh, PartitionSpec as P

LN_EPS = 1e-5
ROPE_BASE = 10000.0
MESH = pl.DeviceIdType.MESH
DMA = pltpu.SemaphoreType.DMA
F32, BF16 = jnp.float32, jnp.bfloat16
ROWS, MODEL, FEATS, BATCH = 1024, 5120, 40, 8192
KB, NB, HB, HD, SUB = 1280, 640, 320, 128, 80
MINE, SEQ, HEADS, LANE, HALF = 64, 64, 40, 128, 64
NR, NC, NJ, NG = 4, 2, 16, 8
X_FIRST = (1,)
CUT = 512
TILE = 256
RING = range(4)
N0, N1, N2, N3 = RING
AWAY = (1, 3, 2)
SIDES = AWAY[:2]
FORTH, BACK = ((1, 0), (3, 1)), ((3, 0), (1, 1))
GROUPS = ((0, 1), (1, 2), (2, 4))
SINGLE = ((0, 1), (1, 2), (2, 3), (3, 4))
ORDER = (0, 1, 3, 2)
BOTH = NEAR, FAR = (0, 1)
TURNED = 2
PAIRS = tuple(sorted(((dy, dx) for dy in RING for dx in RING if dy or dx), key=lambda p: (p.count(2), 0 not in p, abs(p[0] - p[1]))))
NT = (((1,), (1,)), ((), ()))


def flip(i, d):
    return (i, i + 1 - 2 * lax.rem(i, 2), lax.rem(i + 2, 4), 3 - i)[d]


def put(src, dst, ssem, rsem, dev):
    pltpu.make_async_remote_copy(src_ref=src, dst_ref=dst, send_sem=ssem, recv_sem=rsem, device_id=dev, device_id_type=MESH).start()


def added(ref):
    return sum(ref[k].astype(F32) for k in range(NR - 1))


def get(src, dst, sem):
    pltpu.make_async_copy(src, dst, sem).start()


def first(n):
    return pl.ds(0, n)


def drain(ref, sem):
    pltpu.make_async_copy(ref, ref, sem).wait()


class Wide:
    def __init__(self, land, src, sems, pos, groups=GROUPS):
        self.land, self.src = land, src
        self.send, self.yr, self.zr, self.fr, self.dr, self.loc = sems
        self.z, self.y, self.x, self.c = pos
        self.base = self.c * 16
        self.groups = groups
        self.here = set()

    def piece(self, yy):
        return self.src.at[:, pl.ds(pl.multiple_of(yy * NB, LANE), NB)]

    def at(self, dz, g, base=None):
        lo, hi = self.groups[g]
        return self.land.at[pl.ds((self.base if base is None else base) + dz * 4 + lo, hi - lo)]

    def start_local(self):
        get(self.piece(self.y), self.land.at[self.base], self.loc)

    def y_send(self, order=AWAY):
        for dy in order:
            yy = flip(self.y, dy)
            put(self.piece(yy), self.land.at[self.base + dy], self.send, self.yr.at[dy - 1], dict(y=yy))

    def z_send(self, g):
        self.wait_y(g)
        for dz in SIDES:
            self.z_put(g, dz)

    def wait_y(self, g):
        if g:
            for dy in range(*self.groups[g]):
                drain(self.land.at[self.base + dy], self.yr.at[dy - 1])
        self.d2d(0, g)

    def z_put(self, g, dz):
        src = self.at(0, g) if g else self.piece(self.y)
        dst = self.at(dz, g) if g else self.land.at[self.base + dz * 4]
        put(src, dst, self.send, self.zr.at[dz // 2 * len(self.groups) + g], dict(z=flip(self.z, dz)))

    def arrive(self, dz, g):
        drain(self.at(dz, g), self.zr.at[dz // 2 * len(self.groups) + g])
        self.d2d(dz, g)

    def forward(self, g):
        for dz in SIDES:
            self.arrive(dz, g)
        self.pass_on(g)

    def pass_on(self, g, *sides):
        for k, dz in enumerate(SIDES):
            src, dst = (self.at(dz, g), self.at(2, g)) if sides else (self.half(dz, g, k), self.half(2, g, k))
            if dz in (sides or SIDES):
                put(src, dst, self.send, self.fr.at[g], dict(z=flip(self.z, 4 - dz)))

    def half(self, dz, g, k):
        lo, hi = self.groups[g]
        return self.land.at[pl.ds(self.base + dz * 4 + lo, hi - lo), pl.ds(k * HB // 2, HB // 2)]

    def last(self, g):
        drain(self.at(2, g), self.fr.at[g])
        self.d2d(2, g)

    def d2d(self, dz, g):
        to = dict(c=1 - self.c)
        if dz or g:
            put(self.at(dz, g), self.at(dz, g), self.send, self.dr.at[dz * len(self.groups) + g], to)
        else:
            put(self.piece(self.y), self.land.at[self.base], self.send, self.dr.at[0], to)

    def ready(self, dz, g):
        if (dz, g) not in self.here:
            if dz == g == 0:
                drain(self.land.at[self.base], self.loc)
            drain(self.at(dz, g, 16 - self.base), self.dr.at[dz * len(self.groups) + g])
        self.here.add((dz, g))

    def load(self, dz, tile, sem):
        for g, (lo, hi) in enumerate(self.groups):
            self.ready(dz, g)
            self.bring(dz, lo, hi - lo, tile.at[pl.ds(lo, hi - lo)], sem)

    def bring(self, dz, lo, n, tile, sem):
        for cc in range(NC):
            get(self.land.at[pl.ds(cc * 16 + dz * NR + lo, n)], tile.at[:, :, pl.ds(cc * NB, NB)], sem)

    def finish(self):
        drain(self.land.at[first(31)], self.send)


class Narrow:
    def __init__(self, land, parts, sems, pos):
        self.land, self.parts = land, parts
        self.send, self.yr, self.zr, self.fr, self.dr, self.loc = sems
        self.z, self.y, self.x, self.c = pos
        self.s = lax.rem(self.c + self.y, 2)

    def own(self, slot):
        lo = 0
        for ref in self.parts:
            hi = lo + ref.shape[1]
            yield ref, self.land.at[slot, :, pl.ds(lo, hi - lo)]
            lo = hi

    def start(self):
        @pl.when(self.s == 0)
        def _():
            for src, dst in self.own(0):
                get(src, dst, self.loc)

        @pl.when(self.s == 1)
        def _():
            for src, dst in self.own(1):
                put(src, dst, self.send, self.yr, dict(y=flip(self.y, 1), c=1 - self.c))

    def z_first(self):
        @pl.when(self.s == 0)
        def _():
            for k, dz in enumerate(SIDES):
                for (src, _), (_, dst) in zip(self.own(0), self.own(dz * 2)):
                    put(src, dst, self.send, self.zr.at[k], dict(z=flip(self.z, dz)))
            for src, dst in self.own(0):
                put(src, dst, self.send, self.dr.at[0], dict(c=1 - self.c))

    def z_second(self):
        @pl.when(self.s == 1)
        def _():
            src = self.land.at[1]
            drain(src, self.yr)
            for k, dz in enumerate(SIDES):
                put(src, self.land.at[dz * 2 + 1], self.send, self.zr.at[k], dict(z=flip(self.z, dz)))
            put(src, src, self.send, self.dr.at[0], dict(c=1 - self.c))

    def half(self, slot, k):
        return self.land.at[slot, pl.ds(k * HB // 2, HB // 2)]

    def forward(self):
        for k, dz in enumerate(SIDES):
            slot = dz * 2 + self.s
            piece = self.land.at[slot]
            drain(piece, self.zr.at[k])
            put(self.half(slot, k), self.half(4 + self.s, k), self.send, self.fr.at[k], dict(z=flip(self.z, AWAY[1 - k])))
            put(piece, piece, self.send, self.dr.at[1 + k], dict(c=1 - self.c))

    def last(self):
        for k in range(NC):
            piece = self.half(4 + self.s, k)
            drain(piece, self.fr.at[k])
            put(piece, piece, self.send, self.dr.at[3 + k], dict(c=1 - self.c))

    def load(self, dz, tile, sem):
        o = 1 - self.s
        if dz == 0:
            @pl.when(self.s == 0)
            def _():
                drain(self.land.at[0], self.loc)
        if dz == 2:
            for k in range(NC):
                drain(self.half(4 + o, k), self.dr.at[3 + k])
        else:
            drain(self.land.at[dz * 2 + o], self.dr.at[(dz + 1) // 2])
        get(self.land.at[pl.ds(dz * 2, 2)], tile, sem)

    def finish(self):
        for s in range(NC):
            @pl.when(self.s == s)
            def _():
                drain(self.land.at[first(7 + s)], self.send)


class Ring:
    def __init__(self, axis, at, own, land, moved, sems):
        self.axis, self.at, self.own, self.land, self.moved = axis, at, own, land, moved
        self.send, self.recv = sems

    def to(self, d):
        return {self.axis: flip(self.at, d)}

    def start(self):
        for k in range(NC):
            for d, h in ((1, k), (3, 1 - k)):
                put(self.own(h), self.land(d, h), self.send, self.recv.at[d - 1 + h], self.to(d))

    def forward(self):
        for d, h in FORTH:
            drain(self.moved(d, h), self.recv.at[d - 1 + h])
            put(self.moved(d, h), self.moved(2, h) if self.axis == 'y' else self.moved(d, h), self.send, self.recv.at[4 + h], self.to(4 - d))

    def finish(self):
        for d, h in BACK:
            drain(self.moved(d, h), self.recv.at[d - 1 + h])
        for h in range(NC):
            drain(self.moved(2, h), self.recv.at[4 + h])


WIDE_SEMS, SINGLE_SEMS = ([DMA, DMA((NR - 1,)), DMA((2 * n,)), DMA((n,)), DMA((NR * n,)), DMA] for n in map(len, (GROUPS, SINGLE)))
NARROW_SEMS = [DMA, DMA, DMA((2,)), DMA((2,)), DMA((5,)), DMA]
HBM_BUFS = dict(
    Q=((NG, HB, NB), BF16), G=((NG * NR, HB, NB), BF16), U=((NG * NR, HB, NB), BF16), D=((NG * NR, HB, NB), BF16), O=((NG, HB, NB), BF16),
    hnT=((NR, NR, HB, ROWS), BF16), a1=((NR, NC, HB, CUT), BF16), b1=((NR, NC, NR, SUB, ROWS - CUT), BF16))
VMEM_BUFS = dict(
    rT=((FEATS, BATCH), BF16), xs=((NG, FEATS, ROWS + LANE), BF16), F=((NG, FEATS, ROWS + LANE), BF16), S=((NC, NJ, 2, CUT), F32),
    hs=((NR, SUB, ROWS), BF16), hn=((NR, ROWS, KB), BF16), wt=((NC, NR, HB, KB), BF16), wo_t=((NC, NC, HB, NB), BF16),
    gacc=((ROWS, KB), F32), uacc=((ROWS, KB), F32), qout=((NJ, MINE, NB), BF16), kvout=((NJ, MINE, 2 * HD), BF16), kvw=((NC, NC, HB, HD), BF16), q_in=((NJ, MINE, NB), BF16), kv_in=((NG, MINE, 2 * HD), BF16),
    q3=((MINE * HEADS, HD), F32), lenb=((MINE, HD), F32), kc=((MINE, SEQ, HD), BF16), vc=((MINE, SEQ, HD), BF16), kn=((MINE, 2 * HD), F32),
    o_v=((MINE, MODEL), BF16), o_in=((NJ, MINE, NB), BF16), act=((ROWS, KB), BF16), sb=((NR - 1, NR, HB, ROWS), BF16),
    va=((NC, NC, HB, CUT), BF16), vb=((NC, NC, NR, SUB, ROWS - CUT), BF16),
    ta=((NR, NC, HB // 2, CUT), BF16), tb=((NR, NC, NR // 2, SUB, ROWS - CUT), BF16), s2a=((NR, HB, CUT), BF16), s2b=((NR, NR, SUB, ROWS - CUT), BF16),
    a2=((NR, NR - 1, SUB, CUT), BF16), b2=((NR, NR - 1, SUB, ROWS - CUT), BF16), fs=((NR, NC, FEATS, ROWS), BF16))
ONE, EACH, BY_GROUP = (), (NR,), (NG,)
SEMS = dict(f_s=ONE, fin_l=ONE, s_s=(NC,), s_r=(NC,), own_l=(NC,), q_s=ONE, kw_s=ONE, kw_z=ONE, kw_y=ONE, kw_c=(NC,), q_r=ONE, kv_s=ONE, kv_r=ONE, o_s=ONE, o_r=ONE, fin_s=ONE, out_l=ONE,
            a1s=EACH, b1s=EACH, a2s=EACH, a2r=EACH, b2s=EACH, b2r=EACH, ag_s=BY_GROUP, ag_r=(NG, 6), tas=EACH, tbs=EACH, tar=(NR, NC), tbr=(NR, NC), b1r=(NR, NC), a1r=(NR, NC), ld=EACH, wsem=EACH, osem=(NC,), vsem=BY_GROUP,
            f_r=(NC, NG), fin_r=BY_GROUP)


def kernel(res, ls, lens, wq, wk, wv, wg, wu, wdT, woT, kc_h, vc_h, fin, kc_o, vc_o, *rest):
    rest = list(rest)

    class b:
        pass
    for name in list(HBM_BUFS) + list(VMEM_BUFS) + list(SEMS):
        setattr(b, name, rest.pop(0))
    pos = z, y, x, c = tuple(lax.axis_index(a) for a in 'zyxc')
    flow = lambda kind, land, src, *more: kind(land, src, [rest.pop(0) for _ in WIDE_SEMS], pos, *more)
    fq = flow(Narrow, b.Q, (wq,))
    fg, fu, fd = flow(Wide, b.G, wg), flow(Wide, b.U, wu, SINGLE), flow(Wide, b.D, wdT, SINGLE)
    fo = flow(Narrow, b.O, (woT,))
    me = y * 4 + x
    row_low = lax.broadcasted_iota(jnp.int32, (FEATS, LANE), 1) < HALF
    sides = lambda dz: (c, 1 - c)[not dz:]

    bar = pltpu.get_barrier_semaphore()
    peers = [dict(z=flip(z, dz), c=cc) for dz in AWAY for cc in (c, 1 - c)] + [dict(c=1 - c), dict(y=flip(y, 1), c=1 - c)]
    peers += [dict(y=flip(y, dy), x=flip(x, dx)) for dy, dx in PAIRS]
    for p in peers:
        pl.semaphore_signal(bar, inc=1, device_id=p, device_id_type=MESH)
    get(res, b.rT, b.ld.at[0])
    get(kc_h, b.kc, b.ld.at[1])
    get(vc_h, b.vc, b.ld.at[2])
    for f in (fg, fu, fd):
        f.start_local()
    pl.semaphore_wait(bar, len(peers))
    fq.start()

    drain(b.rT, b.ld.at[0])
    scale = jnp.broadcast_to(ls[...].astype(F32), (LANE, FEATS)).T.astype(BF16)
    wide = lambda h: pl.ds(LANE * h + CUT * h, CUT + LANE * (1 - h))
    for i in range(NG):
        b.xs[i, :, :LANE] = scale
    for h in range(NC):
        for dz in AWAY + (0,):
            zz = flip(z, dz)
            for p in range(NR * h, NR * h + NR):
                pair = b.rT[:, pl.ds(pl.multiple_of(zz * NC * ROWS + p * TILE, LANE), TILE)].astype(F32)
                t0, t1 = pair[:, :LANE], pair[:, LANE:]
                at = pl.ds(LANE + p * LANE, LANE)
                b.xs[dz * NC, :, at] = jnp.where(row_low, t0, pltpu.roll(t1, HALF, 1)).astype(BF16)
                b.xs[dz * NC + 1, :, at] = jnp.where(row_low, pltpu.roll(t0, HALF, 1), t1).astype(BF16)
            for cc in sides(dz):
                put(b.xs.at[dz * NC + cc, :, wide(h)], b.F.at[dz * NC + c, :, wide(h)], b.f_s, b.f_r.at[h, dz * NC + c], dict(z=flip(z, dz), c=cc))
    b.F[c] = b.xs[c]
    def kv_half(slot, side):
        return b.kvw.at[slot, side]

    for side, w in enumerate((wk, wv)):
        @pl.when((c == side) & (x == 0))
        def _():
            get(w, kv_half(0, side), b.kw_z)

        @pl.when((c == side) & (x > 0))
        def _():
            zx = lax.rem(z // 2 + x // 2, 2) * 2 + lax.rem(z + x, 2)
            put(w, kv_half(0, side), b.kw_s, b.kw_z, dict(z=zx))
    fq.z_first()
    fg.z_send(0)

    for h in range(NC):
        for dz in RING:
            for cc in sides(dz):
                drain(b.F.at[dz * NC + cc, :, wide(h)], b.f_r.at[h, dz * NC + cc])
        tot = sq = jnp.zeros((FEATS, CUT), F32)
        for i in range(NG):
            v = b.F[i, :, pl.ds(LANE + CUT * h, CUT)].astype(F32)
            tot, sq = tot + v, sq + v * v
        b.S[h, me] = jnp.concatenate([jnp.sum(v, axis=0, keepdims=True) for v in (tot, sq)], axis=0)
        for dy, dx in PAIRS:
            put(b.S.at[h, me], b.S.at[h, me], b.s_s.at[h], b.s_r.at[h], dict(y=flip(y, dy), x=flip(x, dx)))
    fq.z_second()
    fo.z_first()

    mine = lambda d: pl.ds(pl.multiple_of(flip(x, d) * SUB, 16), SUB)

    def normalize(h):
        drain(b.S.at[h, first(NJ - 1)], b.s_r.at[h])
        stats = sum(b.S[h, i] for i in range(NJ)) / MODEL
        mean = stats[0:1]
        inv = lax.rsqrt(stats[1:] - mean * mean + LN_EPS)
        lanes = pl.ds(CUT * h, CUT)
        for dz in RING:
            both = []
            for i in (dz * NC, dz * NC + 1):
                both.append((b.F[i, :, pl.ds(LANE + CUT * h, CUT)].astype(F32) - mean) * inv * b.F[i, :, :LANE].astype(F32)[:, :1])
            b.hs[dz, :, lanes] = jnp.concatenate(both, axis=0).astype(BF16)
        get(b.hs.at[:, :, lanes], b.hnT.at[:, 0, mine(0), lanes], b.own_l.at[h])

    part = lambda h: pl.ds(2 * h, 2)

    def rings(k):
        lanes = pl.ds(k * TILE, TILE)
        far = lambda d, h: b.hnT.at[part(h), :, mine(d), lanes]
        near = lambda d, h: b.hnT.at[part(h), d, mine(0), lanes]
        own = lambda h: b.hs.at[part(h), :, lanes]
        sems = [(b.ag_s.at[NC * k + j], b.ag_r.at[NC * k + j]) for j in range(NC)]
        if k in X_FIRST:
            spot = lambda d, h: b.hnT.at[part(h), 0, mine(d), lanes]
            row = lambda d, h: b.hnT.at[part(h), d, :, lanes]
            return Ring('x', x, own, lambda d, h: spot(0, h), spot, sems[0]), Ring('y', y, lambda h: row(0, h), row, row, sems[1])
        return Ring('y', y, own, near, near, sems[0]), Ring('x', x, lambda h: far(0, h), lambda d, h: far(0, h), far, sems[1])

    one, two = zip(*(rings(k) for k in RING))
    normalize(0)
    one[0].start()
    one[1].start()
    one[0].forward()
    one[1].forward()
    normalize(1)
    one[2].start()
    one[3].start()
    for h in range(NC):
        drain(b.hs.at[:, :, pl.ds(CUT * h, CUT)], b.own_l.at[h])
    one[0].finish()
    two[0].start()
    one[2].forward()
    one[3].forward()
    drain(kv_half(0, c), b.kw_z)
    put(kv_half(0, c), kv_half(1, c), b.kw_s, b.kw_y, dict(y=flip(y, 1)))
    put(kv_half(0, c), kv_half(0, c), b.kw_s, b.kw_c.at[0], dict(c=1 - c))
    fg.y_send()
    one[1].finish()
    two[1].start()
    two[0].forward()
    fq.forward()
    fg.forward(0)
    one[2].finish()
    two[2].start()
    one[3].finish()
    fg.z_send(1)
    fq.last()
    drain(kv_half(1, c), b.kw_y)
    put(kv_half(1, c), kv_half(1, c), b.kw_s, b.kw_c.at[1], dict(c=1 - c))

    def load_q(pair):
        for i in range(NC):
            fq.load(NC * pair + i, b.sb.at[pair, part(i), :, first(NB)], b.osem.at[pair])

    def stage(k):
        two[k].finish()
        for dz in RING:
            get(b.hnT.at[dz, :, :, pl.ds(k * TILE, TILE)], b.wt.at[1, :, :, pl.ds(dz * TILE, TILE)], b.wsem.at[1])

    def turn(k):
        drain(b.wt.at[1, :, :, first(ROWS)], b.wsem.at[1])
        for dz in RING:
            for h in range(NC):
                b.hn[dz, pl.ds(k * TILE + h * LANE, LANE), :] = b.wt[1, :, :, pl.ds(dz * TILE + h * LANE, LANE)].reshape(KB, LANE).T

    def query(k):
        at = pl.ds(k * TILE, TILE)
        new = sum(jnp.dot(b.hn[dz, at, :NB], b.sb[dz // 2, part(dz % 2), :, :NB].reshape(NB, NB), preferred_element_type=F32) for dz in RING)
        b.qout[pl.ds(k * NR, NR)] = new.astype(BF16).reshape(NR, MINE, NB)
        kv = jnp.concatenate([b.kvw[:, side].reshape(NB, HD) for side in range(NC)], axis=1)
        new = jnp.dot(b.hn[x, at, :NB], kv, preferred_element_type=F32)
        b.kvout[pl.ds(k * NR, NR)] = new.astype(BF16).reshape(NR, MINE, 2 * HD)

    def project(acc, i, slot, lo=0, hi=ROWS, fresh=False, wait=True):
        if wait:
            drain(b.wt.at[slot], b.wsem.at[slot])

        @pl.loop(lo // TILE, hi // TILE)
        def _(r):
            at = pl.ds(pl.multiple_of(r * TILE, TILE), TILE)
            new = jnp.dot(b.hn[ORDER[i], at, :], b.wt[slot].reshape(KB, KB), preferred_element_type=F32)
            acc[at, :] = new if fresh else new + acc[at, :]

    fetch = lambda f, i, slot: f.load(ORDER[i], b.wt.at[slot], b.wsem.at[slot])

    def roles(i):
        return (0, 3, 2, 1) if i == TURNED else tuple(RING)

    def fetch_d(i, *parts):
        for h in parts:
            for t in (2 * h, 2 * h + 1):
                g = roles(i)[t]
                fd.ready(ORDER[i], g)
                fd.bring(ORDER[i], g, 1, b.wt.at[i % 2, pl.ds(t, 1)], b.wsem.at[2 * h + i % 2])


    fg.z_send(2)
    fu.z_send(0)
    load_q(0)
    load_q(1)
    stage(0)
    two[2].forward()
    two[3].start()
    turn(0)
    for pair in range(NC):
        drain(b.sb.at[pair, :, :, first(NB)], b.osem.at[pair])
    for slot in range(NC):
        drain(kv_half(slot, 1 - c), b.kw_c.at[slot])
    query(0)
    two[1].forward()
    fu.y_send()
    fg.forward(1)
    stage(2)
    turn(2)
    query(2)
    fetch(fg, 0, 0)
    two[3].forward()
    stage(1)
    turn(1)
    query(1)
    fg.forward(2)
    fg.last(0)
    project(b.gacc, 0, 0, 0, 3 * TILE, fresh=True)
    fu.z_send(1)
    fu.forward(0)
    fetch(fg, 1, 0)
    project(b.gacc, 1, 0, 0, 3 * TILE)
    fu.z_send(3)
    fu.z_send(2)
    stage(3)
    turn(3)
    fetch(fg, 0, 1)
    query(3)
    for dy in (0, 2):
        for dx in AWAY + (0,)[:dy]:
            yy, xx = flip(y, dy), flip(x, dx)
            put(b.kvout.at[yy * NR + xx], b.kv_in.at[2 * dy + x], b.kv_s, b.kv_r, dict(y=yy, x=xx))
    for dy, dx in PAIRS:
        yy, xx = flip(y, dy), flip(x, dx)
        put(b.qout.at[yy * NR + xx], b.q_in.at[me], b.q_s, b.q_r, dict(y=yy, x=xx))
    b.q_in[me] = b.qout[me]
    b.kv_in[x] = b.kvout[me]
    fo.start()
    fd.y_send((2, 1, 3))

    project(b.gacc, 1, 0, 3 * TILE, ROWS, fresh=True, wait=False)
    fetch(fg, 2, 0)
    project(b.gacc, 0, 1, 3 * TILE, ROWS)
    fg.last(1)
    fg.last(2)
    fetch(fg, 3, 1)
    project(b.gacc, 2, 0)
    fu.forward(1)
    fetch(fu, 0, 0)
    project(b.gacc, 3, 1)
    project(b.uacc, 0, 0, fresh=True)
    drain(b.kc, b.ld.at[1])
    drain(b.vc, b.ld.at[2])
    drain(b.q_in.at[first(NJ - 1)], b.q_r)
    drain(b.kv_in.at[first(NG - 1)], b.kv_r)

    @pl.loop(0, MINE)
    def _(r):
        b.lenb[pl.ds(r, 1), :] = jnp.broadcast_to(lens[r], (1, HD)).astype(F32)
    i_half = lax.rem(lax.broadcasted_iota(jnp.int32, (MINE, HD), 1), HALF).astype(F32)
    angle = b.lenb[...] * jnp.power(ROPE_BASE, i_half * (-2.0 / HD))
    low = lax.broadcasted_iota(jnp.int32, (MINE, HD), 1) < HALF
    cos = jnp.cos(angle)
    sin = jnp.where(low, -jnp.sin(angle), jnp.sin(angle))
    rope = lambda v: v * cos + pltpu.roll(v, HALF, 1) * sin
    kv = sum(b.kv_in[i].astype(F32) for i in range(NG)).astype(BF16).astype(F32)
    b.kn[:, :HD] = rope(kv[:, :HD])
    b.kn[:, HD:] = kv[:, HD:]
    for xs in RING:
        for yh in range(NC):
            q = (b.q_in[yh * 4 + xs].astype(F32) + b.q_in[(yh + 2) * 4 + xs].astype(F32)).astype(BF16).astype(F32)
            for h in range(5):
                b.q3[pl.ds(xs * 10 + yh * 5 + h, MINE, stride=HEADS), :] = rope(q[:, h * HD:(h + 1) * HD])
    t_row = lax.broadcasted_iota(jnp.int32, (SEQ, HD), 0)
    t_col = lax.broadcasted_iota(jnp.int32, (HEADS, SEQ), 1)

    def attend(rows):
        ats = [pl.ds(pl.multiple_of(r * HEADS, 8), HEADS) for r in rows]
        here = [t_row == lens[r] for r in rows]
        new = [b.kn[pl.ds(r, 1), :] for r in rows]
        keys = [jnp.where(h, n[:, :HD].astype(BF16).astype(F32), b.kc[r].astype(F32)).astype(BF16) for r, h, n in zip(rows, here, new)]
        vals = [jnp.where(h, n[:, HD:], b.vc[r].astype(F32)).astype(BF16) for r, h, n in zip(rows, here, new)]
        s = [lax.dot_general(b.q3[at, :].astype(BF16), k, NT, preferred_element_type=F32) for at, k in zip(ats, keys)]
        s = [jnp.where(t_col <= lens[r], v * (HD ** -0.5), -1e30) for r, v in zip(rows, s)]
        top = [jnp.max(v, axis=1, keepdims=True) for v in s]
        e = [jnp.exp(v - t) for v, t in zip(s, top)]
        total = [jnp.sum(v, axis=1, keepdims=True) for v in e]
        p = [(v / t).astype(BF16) for v, t in zip(e, total)]
        o = [jnp.dot(v, w, preferred_element_type=F32) for v, w in zip(p, vals)]
        for r, at, k, v, w in zip(rows, ats, keys, vals, o):
            b.kc[r], b.vc[r], b.q3[at, :] = k, v, w

    def attend_some(lo, hi):
        @pl.loop(lo // NG, hi // NG)
        def _(step):
            attend([step * NG + k for k in range(NG)])

    attend_some(0, MINE)
    get(b.kc, kc_o, b.out_l)
    get(b.vc, vc_o, b.out_l)
    for h in range(HEADS):
        b.o_v[:, h * HD:(h + 1) * HD] = b.q3[pl.ds(h, MINE, stride=HEADS), :].astype(BF16)
    block = lambda yy, xx: b.o_v.at[:, pl.ds(pl.multiple_of((xx * 2 + lax.rem(yy, 2)) * NB, LANE), NB)]
    for dy, dx in PAIRS:
        yy, xx = flip(y, dy), flip(x, dx)
        put(block(yy, xx), b.o_in.at[me], b.o_s, b.o_r, dict(y=yy, x=xx))
    b.o_in[me] = block(y, x)[...]

    def start_d(*plan):
        for g, planes in plan:
            fd.wait_y(g)
            for dz in planes:
                fd.z_put(g, dz)

    fu.forward(3)
    fu.forward(2)
    fo.z_second()
    fetch(fu, 1, 1)
    fetch(fu, 2, 0)
    project(b.uacc, 1, 1)
    project(b.uacc, 2, 0)
    start_d((2, SIDES))
    fu.last(0)
    fu.last(1)
    fu.last(3)
    fu.last(2)
    fetch(fu, 3, 1)
    load_o = lambda i: fo.load(ORDER[i], b.wo_t.at[i % 2], b.osem.at[i % 2])
    project(b.uacc, 3, 1)
    start_d((1, SIDES[1:]), (3, SIDES[:1]), (0, SIDES))
    fetch_d(0, *BOTH)
    load_o(0)

    @pl.loop(0, ROWS // LANE)
    def _(r):
        at = pl.ds(pl.multiple_of(r * LANE, LANE), LANE)
        g = b.gacc[at, :].astype(BF16).astype(F32)
        b.act[at, :] = (g / (1.0 + jnp.exp(-g)) * b.uacc[at, :].astype(BF16).astype(F32)).astype(BF16)
    drain(b.o_in.at[first(NJ - N1)], b.o_r)
    HA, HBk = first(CUT), pl.ds(CUT, ROWS - CUT)

    rows_of = lambda h: pl.ds(h * HB // N2, HB // N2)

    def sent(i):
        for land, sem in ((b.a1, b.a1s), (b.b1, b.b1s), (b.ta, b.tas), (b.tb, b.tbs)):
            drain(land.at[i], sem.at[i])

    def multiply(i, h):
        slot, k, tall = i % N2, i % N3, part(h)
        drain(b.wt.at[slot, tall], b.wsem.at[N2 * h + slot])
        heads = [t for t in (N2 * h, N2 * h + N1) if roles(i)[t] < N2]
        if heads and i not in loaded_o:
            drain(b.wo_t.at[slot], b.osem.at[slot])
            loaded_o.add(i)

        def some(lo, hi):
            @pl.loop(lo // TILE, hi // TILE)
            def _(r):
                at = pl.ds(pl.multiple_of(r * TILE, TILE), TILE)
                out = lax.dot_general(b.wt[slot, tall].reshape(NB, KB), b.act[at, :], NT, preferred_element_type=F32)
                rows = b.o_in[pl.ds(r * NR, NR)].reshape(TILE, NB)
                if len(heads) == N2:
                    out += lax.dot_general(b.wo_t[slot].reshape(NB, NB), rows, NT, preferred_element_type=F32)
                elif heads:
                    more = lax.dot_general(b.wo_t[slot, roles(i)[heads[N0]]], rows, NT, preferred_element_type=F32)
                    halves = [out[:HB], out[HB:]]
                    halves[heads[N0] - N2 * h] += more
                    out = jnp.concatenate(halves, axis=N0)
                b.sb[k, tall, :, at] = out.astype(BF16).reshape(N2, HB, TILE)

        def first_rows():
            some(N0, CUT)
            if h == FAR:
                for j, d in enumerate(ends(i)):
                    put(b.sb.at[k, N2, rows_of(j), HA], b.ta.at[i, j], b.tas.at[i], b.tar.at[i, j], dict(y=flip(y, d)))
            put(b.sb.at[k, SIDES[h], rows_of(h), HA], b.a1.at[i, h, rows_of(h)], b.a1s.at[i], b.a1r.at[i, h], dict(y=flip(y, ends(i)[h])))
            if h == NEAR and i:
                pass_a(i, h)

        def last_rows():
            some(CUT, ROWS)
            d = ends(i)[h]
            put(b.sb.at[k, tall, mine(N2), HBk], b.tb.at[i, h], b.tbs.at[i], b.tbr.at[i, h], dict(x=flip(x, d)))
            put(b.sb.at[k, tall, mine(d), HBk], b.b1.at[i, h, tall], b.b1s.at[i], b.b1r.at[i, h], dict(x=flip(x, d)))

        for step in (first_rows, last_rows)[::N1 if h else -N1]:
            step()

    loaded_o = set()
    ends = lambda i: SIDES[::-N1] if i == TURNED else SIDES

    def pass_a(i, h):
        k, t, rows = i % N3, SIDES[h], rows_of(N1 - h)
        drain(b.ta.at[i, N1 - h], b.tar.at[i, N1 - h])
        b.sb[k, t, rows, HA] = (b.sb[k, t, rows, HA].astype(F32) + b.ta[i, N1 - h].astype(F32)).astype(BF16)
        put(b.sb.at[k, t, rows, HA], b.a1.at[i, h, rows], b.a1s.at[i], b.a1r.at[i, h], dict(y=flip(y, ends(i)[h])))

    def passed(i, h):
        k, tall = i % N3, part(h)
        if h == FAR or i == N0:
            pass_a(i, h)
        d = ends(i)[N1 - h]
        drain(b.tb.at[i, h], b.tbr.at[i, h])
        b.sb[k, tall, mine(d), HBk] = (b.sb[k, tall, mine(d), HBk].astype(F32) + b.tb[i, h].astype(F32)).astype(BF16)
        put(b.sb.at[k, tall, mine(d), HBk], b.b1.at[i, N1 - h, tall], b.b1s.at[i], b.b1r.at[i, h], dict(x=flip(x, d)))

    def load_a(i):
        for k in range(NC):
            drain(b.a1.at[i, k], b.a1r.at[i, k])
        get(b.a1.at[i], b.va.at[i % N2], b.vsem.at[i % N2])

    def second_a(i):
        dz, va = ORDER[i], b.va.at[i % N2]
        drain(va, b.vsem.at[i % N2])
        b.s2a[dz] = (b.sb[i % N3, N0, :, HA].astype(F32) + (va[N0].astype(F32) + va[N1].astype(F32))).astype(BF16)
        for d in AWAY:
            put(b.s2a.at[dz, mine(d)], b.a2.at[dz, d - N1], b.a2s.at[dz], b.a2r.at[dz], dict(x=flip(x, d)))

    def load_b(i, h):
        drain(b.b1.at[i, :, part(h)], b.b1r.at[i, h])
        get(b.b1.at[i, :, part(h)], b.vb.at[i % N2, :, part(h)], b.vsem.at[N2 + N2 * h + i % N2])

    def second_b(i, h):
        k, tall = i % N3, part(h)
        vb = b.vb.at[i % N2, :, tall]
        drain(vb, b.vsem.at[N2 + N2 * h + i % N2])
        b.s2b[i, tall] = (b.sb[k, tall, mine(N0), HBk].astype(F32) + (vb[N0].astype(F32) + vb[N1].astype(F32))).astype(BF16)
        for t in ((N1,), (N3, N2))[h]:
            put(b.s2b.at[i, t], b.b2.at[i, t - N1], b.b2s.at[i], b.b2r.at[i], dict(y=flip(y, roles(i)[t])))

    def third(i):
        dz = ORDER[i]
        drain(b.a2.at[dz], b.a2r.at[dz])
        drain(b.b2.at[i], b.b2r.at[i])
        for src, own, lanes, at in ((b.a2.at[dz], b.s2a[dz, mine(N0)], HA, LANE), (b.b2.at[i], b.s2b[i, N0], HBk, LANE + CUT)):
            total = own.astype(F32) + sum(src[d].astype(F32) for d in range(NR - N1))
            for cc in range(NC):
                b.fs[dz, cc, :, lanes] = (b.F[dz * NC + cc, :, pl.ds(at, CUT)].astype(F32) + total[cc * FEATS:(cc + N1) * FEATS]).astype(BF16)
        at = z * NC + c
        for cc in sides(dz):
            put(b.fs.at[dz, cc], fin.at[at], b.fin_s, b.fin_r.at[at], dict(z=flip(z, dz), c=cc))
        if dz == N0:
            get(b.fs.at[N0, c], fin.at[at], b.fin_l)

    multiply(N0, FAR)
    multiply(N0, NEAR)
    for dz, g in ((N1, N2), (N3, N2), (N1, N3), (N3, N1)):
        fd.arrive(dz, g)
    fd.z_put(N1, N1)
    fd.z_put(N3, N3)
    fd.pass_on(N2)
    fd.pass_on(N3, N1)
    fd.pass_on(N1, N3)
    fo.forward()
    fetch_d(N1, FAR)
    load_o(N2)
    fetch_d(N2, FAR)
    passed(N0, FAR)
    passed(N0, NEAR)
    multiply(N1, FAR)
    multiply(N2, FAR)
    load_b(N0, FAR)
    load_a(N0)
    load_b(N0, NEAR)
    second_b(N0, FAR)
    second_a(N0)
    second_b(N0, NEAR)
    passed(N1, FAR)
    load_o(N1)
    fd.arrive(N1, N0)
    fd.arrive(N3, N0)
    fd.pass_on(N0)
    fd.arrive(N1, N1)
    fd.arrive(N3, N3)
    fetch_d(N1, NEAR)
    fetch_d(N2, NEAR)
    multiply(N1, NEAR)
    passed(N2, FAR)
    multiply(N2, NEAR)
    fd.last(N2)
    fd.last(N3)
    fd.last(N1)
    sent(N0)
    fetch_d(N3, FAR)
    multiply(N3, FAR)
    passed(N1, NEAR)
    passed(N2, NEAR)
    load_b(N1, FAR)
    load_b(N2, FAR)
    second_b(N1, FAR)
    second_b(N2, FAR)
    fo.last()
    fd.last(N0)
    fetch_d(N3, NEAR)
    load_o(N3)
    passed(N3, FAR)
    multiply(N3, NEAR)
    load_a(N1)
    load_a(N2)
    second_a(N1)
    second_a(N2)
    load_b(N1, NEAR)
    load_b(N2, NEAR)
    second_b(N1, NEAR)
    second_b(N2, NEAR)
    passed(N3, NEAR)
    third(N0)
    load_b(N3, FAR)
    second_b(N3, FAR)
    load_a(N3)
    second_a(N3)
    load_b(N3, NEAR)
    second_b(N3, NEAR)
    third(N1)
    third(N2)
    third(N3)

    for dz in AWAY + (0,):
        for cc in sides(dz):
            at = flip(z, dz) * NC + cc
            drain(fin.at[at], b.fin_r.at[at])
    drain(fin.at[0], b.fin_l)

    some, tile = first(NR - 1), first(TILE)
    for k in RING:
        drain(b.hnT.at[some, 0, :, tile], b.ag_s.at[NC * k])
        drain(b.hnT.at[some, :, :, tile], b.ag_s.at[NC * k + 1])
    for h in range(NC):
        drain(b.S.at[h, first(NJ - 1)], b.s_s.at[h])
    drain(b.F.at[first(NG - 1)], b.f_s)
    drain(b.q_in.at[first(NJ - 1)], b.q_s)
    drain(b.kv_in.at[first(NG - 1)], b.kv_s)
    drain(b.kvw.at[0], b.kw_s)
    drain(kv_half(1, c), b.kw_s)

    @pl.when(x > 0)
    def _():
        drain(kv_half(0, c), b.kw_s)
    drain(b.o_in.at[first(NJ - 1)], b.o_s)
    for dz in ORDER:
        if dz:
            sent(dz)
        drain(b.a2.at[dz], b.a2s.at[dz])
        drain(b.b2.at[dz], b.b2s.at[dz])
    drain(fin.at[first(NG - 1)], b.fin_s)
    for f in (fq, fg, fu, fd, fo):
        f.finish()
    for ref in (b.kc, b.vc):
        drain(ref, b.out_l)


def finish(fin, kc_h, vc_h, out, kc_o, vc_o, fin_v, kc, vc, ov, sem):
    get(fin, fin_v, sem.at[0])
    get(kc_h, kc, sem.at[1])
    get(vc_h, vc, sem.at[2])
    drain(fin_v, sem.at[0])
    row_low = lax.broadcasted_iota(jnp.int32, (FEATS, LANE), 1) < HALF
    for zz in RING:
        for p in range(NG):
            lo, hi = (fin_v[zz * NC + cc, :, pl.ds(p * LANE, LANE)].astype(F32) for cc in range(NC))
            pair = [jnp.where(row_low, lo, pltpu.roll(hi, HALF, 1)), jnp.where(row_low, pltpu.roll(lo, HALF, 1), hi)]
            ov[:, pl.ds(zz * NC * ROWS + p * TILE, TILE)] = jnp.concatenate(pair, axis=1).astype(BF16)
    drain(kc, sem.at[1])
    get(kc, kc_o, sem.at[1])
    drain(vc, sem.at[2])
    get(vc, vc_o, sem.at[2])
    get(ov, out, sem.at[0])
    for i, ref in enumerate((ov, kc, vc)):
        drain(ref, sem.at[i])


def solution(mesh):
    inner = Mesh(mesh.devices.reshape(4, 4, 4, 2), tuple('zyxc'))

    def layer(residual, ln_scale, w_query, w_key, w_value, w_gate, w_up, w_out, w_down, k_cache, v_cache, lengths):
        hbm = pl.BlockSpec(memory_space=pltpu.HBM)
        vmem = pl.BlockSpec(memory_space=pltpu.VMEM)
        smem = pl.BlockSpec(memory_space=pltpu.SMEM)
        shape = lambda a: jax.ShapeDtypeStruct(*a)
        results = [((FEATS, BATCH), BF16), (k_cache.shape, BF16), (v_cache.shape, BF16)]
        fin = ((NG, FEATS, ROWS), BF16)
        outs = [fin] + results[1:] + list(HBM_BUFS.values())
        got = pl.pallas_call(
            kernel,
            out_shape=[shape(a) for a in outs],
            in_specs=[hbm, vmem, smem] + [hbm] * 9,
            out_specs=[hbm] * len(outs),
            scratch_shapes=[pltpu.VMEM(*a) for a in VMEM_BUFS.values()] + [DMA(s) if s else DMA for s in SEMS.values()] + NARROW_SEMS + WIDE_SEMS + SINGLE_SEMS * 2 + NARROW_SEMS,
            name='decode_layer',
            compiler_params=pltpu.CompilerParams(collective_id=0, has_side_effects=True, vmem_limit_bytes=67043328),
        )(residual.T, ln_scale.reshape(1, FEATS), lengths, w_query, w_key, w_value, w_gate, w_up, w_down.T, w_out.T, k_cache, v_cache)
        out, k_new, v_new = pl.pallas_call(
            finish,
            out_shape=[shape(a) for a in results],
            in_specs=[hbm] * 3,
            out_specs=[hbm] * 3,
            scratch_shapes=[pltpu.VMEM(*a) for a in [fin] + results[1:] + results[:1]] + [DMA((3,))],
            name='finish',
        )(*got[:3])
        return out.T, k_new, v_new

    rc, tx, tyz = tuple('zyxc'), tuple('zy'), tuple('xc')
    cache = P(rc, None, None)
    in_specs = (P(None, rc), P(rc), P(tx, tyz), P(tx, None), P(tx, None), P(tx, tyz), P(tx, tyz), P(tyz, tx), P(tyz, tx), cache, cache, P(rc))
    return jax.shard_map(layer, mesh=inner, in_specs=in_specs, out_specs=(P(None, rc), cache, cache), check_vma=False)
```
